32 devices in a mesh: section: 2 (over core), shard: 4 (over z), rep: 4 (over y, x).
Axes of the slice: x: 2, y: 2, z: 4, core: 2. Of those that a mesh axis runs over, the one named last changes fastest.
Arguments:
- boundary: bfloat16 [2, 2, 16, 256, 1536], P('section', None, ('shard', 'rep')), may hold values from -6 to 6
- lengths: int32 [2, 16], P(None, ('shard', 'rep')), may hold values from 1 to 256, 2457 in all within a row
- in_proj: bfloat16 [2, 1536, 6400], P('section', 'shard'), may hold values from -0.15625 to 0.15625
- dt_proj: bfloat16 [2, 1536, 48], P('section', 'shard'), may hold values from -0.15625 to 0.15625
- out_proj: bfloat16 [2, 3072, 1536], P('section', 'shard'), may hold values from -0.109375 to 0.109375
- conv_weight: bfloat16 [2, 4, 3328], P('section', None, 'shard'), may hold values from -3 to 3
- conv_bias: bfloat16 [2, 3328], P('section', 'shard'), may hold values from -3 to 3
- dt_bias: bfloat16 [2, 48], P('section', 'shard'), may hold values from -6 to -2
- a_log: bfloat16 [2, 48], P('section', 'shard'), may hold values from 0 to 2.765625
- d_skip: bfloat16 [2, 48], P('section', 'shard'), may hold values from 0.5 to 1.5
- pre_gain: bfloat16 [2, 1536], P('section', 'shard'), may hold values from 0.5 to 1.5
- out_gain: bfloat16 [2, 3072], P('section', 'shard'), may hold values from 0.5 to 1.5
Outputs:
- activations: bfloat16 [2, 2, 16, 256, 1536], P('section', None, ('shard', 'rep'))
- input_grads: bfloat16 [2, 2, 16, 256, 1536], P('section', None, ('shard', 'rep'))
- grad_in_proj: float32 [2, 1536, 6400], P('section', 'shard')
- grad_dt_proj: float32 [2, 1536, 48], P('section', 'shard')
- grad_out_proj: float32 [2, 3072, 1536], P('section', 'shard')
- grad_conv_weight: float32 [2, 4, 3328], P('section', None, 'shard')
- grad_conv_bias: float32 [2, 3328], P('section', 'shard')
- grad_dt_bias: float32 [2, 48], P('section', 'shard')
- grad_a_log: float32 [2, 48], P('section', 'shard')
- grad_d_skip: float32 [2, 48], P('section', 'shard')
- grad_pre_gain: float32 [2, 1536], P('section', 'shard')
- grad_out_gain: float32 [2, 3072], P('section', 'shard')
The draws below stay inside these ranges and needn't reach their ends.
Inputs may be any that keep to these rules, and one draw needn't show every extreme that they name: `lengths`: in each micro-batch some sequence has exactly 256 tokens.
All inputs are finite; a program needn't handle non-finite values. No bound on the sum of `lengths` on one device may be relied on, other than what follows from the above.
Results may differ from the reference program's by a relative error of at most 0.02.
Values may be sent and summed in bfloat16 or wider, within the bound.
A program may use at most 768 MiB of HBM per device.

```python
import math
import jax
import jax.numpy as jnp
import numpy as np
from jax import lax

D = 1536
HEADS = 48
TAPS = 4
SCAN_BLOCK = 128
MICRO = 2
SEQ_LEN = 256
INNER = 3072
PROJ = 6400
CONV = 3328
SEQS = 16


def levels(own_key, dims, shards, low, largest):
    def one(axis_at, blocks):
        heights = jax.random.uniform(jax.random.fold_in(jax.random.fold_in(own_key, 6), axis_at), (blocks,), jnp.float32, low / len(shards), largest / len(shards))
        return jnp.repeat(jnp.exp(heights), dims[axis_at] // blocks).reshape((-1,) + (1,) * (len(dims) - axis_at - 1))

    level = one(*shards[0])
    for cut in shards[1:]:
        level = level * one(*cut)
    return level


def profile(amount, total, limit, lean):
    loads = [(1 << 20) // math.isqrt(grade ** lean) + 1 for grade in range(2, amount + 1)]
    spare, holding = total - limit - (amount - 1), [1] * (amount - 1)
    while spare > 0:
        movable = [i for i in range(amount - 1) if holding[i] < limit]
        pool, left = sum([loads[i] for i in movable]), spare
        for i in movable:
            more = min(limit - holding[i], max(1, left * loads[i] // pool), spare)
            holding[i] = holding[i] + more
            spare = spare - more
    return np.array([limit] + holding)


def uneven(key, amount, total, bound, lean):
    if amount == 2:
        one = jax.random.randint(key, (), max(1, total - bound), min(bound, total - 1) + 1)
        return jnp.stack([one, total - one])
    sizes = jnp.asarray(profile(amount, total, bound, lean), jnp.int32)
    pairs = (amount - 1) // 2
    source_of, taker = sizes[1:1 + 2 * pairs:2], sizes[2:2 + 2 * pairs:2]
    slack = jnp.minimum(source_of - 1, bound - taker)
    passed = jax.random.randint(jax.random.fold_in(key, 1), (pairs,), 0, 1 << 20) % (slack + 1)
    sizes = sizes.at[1:1 + 2 * pairs:2].set(source_of - passed).at[2:2 + 2 * pairs:2].set(taker + passed)
    return sizes[jax.random.permutation(jax.random.fold_in(key, 2), amount)]


def noise(rng, shape, scale, most, split=(), kind=jnp.bfloat16):
    values = scale * jax.random.normal(rng, shape, jnp.float32)
    if split:
        values = values * levels(rng, shape, split, -0.22, 0.18)
    return jnp.clip(values, -most, most).astype(kind)


def setup_inputs(seed: int = 0) -> dict:
    seeds = jax.random.split(jax.random.key(seed), 13)
    return {
        "boundary": noise(seeds[0], (2, MICRO, SEQS, SEQ_LEN, D), 1.0, 6.0, ((0, 2), (2, 16))),
        "lengths": jax.vmap(lambda own: uneven(own, SEQS, SEQS * SEQ_LEN * 3 // 5, SEQ_LEN, 2))(jax.random.split(seeds[1], MICRO)).reshape((MICRO, SEQS)).astype(jnp.int32),
        "in_proj": noise(seeds[2], (2, D, PROJ), D ** -0.5, 0.15625, ((0, 2), (1, 4))),
        "dt_proj": noise(seeds[3], (2, D, HEADS), D ** -0.5, 0.15625, ((0, 2), (1, 4))),
        "out_proj": noise(seeds[4], (2, INNER, D), INNER ** -0.5, 0.109375, ((0, 2), (1, 4))),
        "conv_weight": noise(seeds[5], (2, TAPS, CONV), TAPS ** -0.5, 3.0, ((0, 2), (2, 4))),
        "conv_bias": noise(seeds[6], (2, CONV), 0.5, 3.0, ((0, 2), (1, 4))),
        "dt_bias": jnp.clip(-6.0 + 4.0 * jax.random.uniform(seeds[7], (2, HEADS), jnp.float32) ** levels(seeds[7], (2, HEADS), ((0, 2), (1, 4)), -0.2, 0.2), -6.0, -2.0).astype(jnp.bfloat16),
        "a_log": jnp.clip(2.765625 * jax.random.uniform(seeds[8], (2, HEADS), jnp.float32) ** levels(seeds[8], (2, HEADS), ((0, 2), (1, 4)), -0.2, 0.2), 0.0, 2.765625).astype(jnp.bfloat16),
        "d_skip": jnp.clip(0.5 + 1.0 * jax.random.uniform(seeds[9], (2, HEADS), jnp.float32) ** levels(seeds[9], (2, HEADS), ((0, 2), (1, 4)), -0.2, 0.2), 0.5, 1.5).astype(jnp.bfloat16),
        "pre_gain": jnp.clip(1.0 + 0.1 * jax.random.normal(seeds[10], (2, D), jnp.float32), 0.5, 1.5).astype(jnp.bfloat16),
        "out_gain": jnp.clip(1.0 + 0.1 * jax.random.normal(seeds[11], (2, INNER), jnp.float32), 0.5, 1.5).astype(jnp.bfloat16),
    }


HIGH = lax.Precision.HIGHEST
EPSILON = 1e-05

def pre_norm(rows, gain_row):
    return rows * lax.rsqrt(lax.optimization_barrier(jnp.mean(rows * rows, axis=-1, keepdims=True)) + EPSILON) * gain_row

def state_space(inputs, decay, b_rows, c_rows):
    seq_len, heads, head_dim = inputs.shape
    state_dim = b_rows.shape[1]
    blocks = seq_len // SCAN_BLOCK
    x_blocks = inputs.reshape(blocks, SCAN_BLOCK, heads, head_dim)
    d_blocks = decay.reshape(blocks, SCAN_BLOCK, heads)
    b_blocks = b_rows.reshape(blocks, SCAN_BLOCK, state_dim)
    c_blocks = c_rows.reshape(blocks, SCAN_BLOCK, state_dim)
    places = jnp.arange(SCAN_BLOCK, dtype=jnp.int32)
    lower = (places[:, None] >= places[None, :])[None, :, :]

    def advance(carried, pieces):
        x_piece, d_piece, b_piece, c_piece = pieces
        cumul = jnp.cumsum(d_piece, axis=0).T
        spread = cumul[:, :, None] - cumul[:, None, :]
        weights = jnp.where(lower, jnp.exp(jnp.where(lower, spread, 0.0)), 0.0)
        scores = jnp.dot(c_piece, b_piece.T, precision=HIGH)
        inside = jnp.einsum('hij,jhp->ihp', weights * scores[None], x_piece, precision=HIGH)
        from_state = jnp.einsum('in,hpn->ihp', c_piece, carried, precision=HIGH) * jnp.exp(cumul).T[:, :, None]
        tail = jnp.exp(cumul[:, -1:] - cumul).T
        fresh = jnp.einsum('jhp,jn->hpn', x_piece * tail[:, :, None], b_piece, precision=HIGH)
        updated = jnp.exp(cumul[:, -1])[:, None, None] * carried + fresh
        return (updated, inside + from_state)
    start = jnp.zeros((heads, head_dim, state_dim), jnp.float32)
    _, outputs = lax.scan(advance, start, (x_blocks, d_blocks, b_blocks, c_blocks))
    return outputs.reshape(seq_len, heads, head_dim)

def mixer_core(projected, dt_raw, floats):
    conv_weight, conv_bias, dt_bias, a_log, d_skip, out_gain = floats
    inner = out_gain.shape[0]
    heads = dt_bias.shape[0]
    state_dim = (conv_weight.shape[1] - inner) // 2
    taps = conv_weight.shape[0]
    seq_len = projected.shape[0]
    gate_part = projected[:, :inner]
    conv_in = projected[:, inner:]
    padded = jnp.pad(conv_in, ((taps - 1, 0), (0, 0)))
    summed = conv_bias + conv_weight[0] * padded[0:seq_len]
    for offset in range(1, taps):
        summed = summed + conv_weight[offset] * padded[offset:offset + seq_len]
    conv_act = jax.nn.silu(summed)
    x_part = conv_act[:, :inner].reshape(seq_len, heads, inner // heads)
    b_rows = conv_act[:, inner:inner + state_dim]
    c_rows = conv_act[:, inner + state_dim:]
    step_size = jax.nn.softplus(dt_raw + dt_bias)
    decay = -jnp.exp(a_log) * step_size
    output = state_space(x_part * step_size[:, :, None], decay, b_rows, c_rows) + d_skip[None, :, None] * x_part
    gated = output.reshape(seq_len, inner) * jax.nn.silu(gate_part)
    return pre_norm(gated, out_gain)

def core_floats(params):
    return tuple((params[place].astype(jnp.float32) for place in (3, 4, 5, 6, 7, 9)))

def live_mask(seq_len, count):
    return (jnp.arange(seq_len, dtype=jnp.int32) < count).astype(jnp.float32)[:, None]

def block_forward(rows, count, params):
    rows32 = rows.astype(jnp.float32)
    normed = pre_norm(rows32, params[8].astype(jnp.float32)).astype(jnp.bfloat16)
    projected = jnp.dot(normed, params[0], preferred_element_type=jnp.float32)
    dt_raw = jnp.dot(normed, params[1], preferred_element_type=jnp.float32)
    mixed = mixer_core(projected, dt_raw, core_floats(params)).astype(jnp.bfloat16)
    out_rows = jnp.dot(mixed, params[2], preferred_element_type=jnp.float32)
    result = (rows32 + live_mask(rows.shape[0], count) * out_rows).astype(jnp.bfloat16)
    return (result, (normed, projected, dt_raw, mixed))

def block_backward(cotangent, rows, stored, count, params):
    normed, projected, dt_raw, mixed = stored
    cot32 = cotangent.astype(jnp.float32)
    g_out = (cot32 * live_mask(rows.shape[0], count)).astype(jnp.bfloat16)
    d_out_proj = jnp.dot(mixed.T, g_out, preferred_element_type=jnp.float32)
    d_mixed = jnp.dot(g_out, params[2].T, preferred_element_type=jnp.float32)
    _, core_back = jax.vjp(mixer_core, projected, dt_raw, core_floats(params))
    d_projected, d_dt_raw, d_floats = core_back(d_mixed)
    d_proj_low = d_projected.astype(jnp.bfloat16)
    d_dt_low = d_dt_raw.astype(jnp.bfloat16)
    d_in_proj = jnp.dot(normed.T, d_proj_low, preferred_element_type=jnp.float32)
    d_dt_proj = jnp.dot(normed.T, d_dt_low, preferred_element_type=jnp.float32)
    d_normed = jnp.dot(d_proj_low, params[0].T, preferred_element_type=jnp.float32) + jnp.dot(d_dt_low, params[1].T, preferred_element_type=jnp.float32)
    _, norm_back = jax.vjp(pre_norm, rows.astype(jnp.float32), params[8].astype(jnp.float32))
    d_rows, d_pre_gain = norm_back(d_normed)
    d_input = (cot32 + d_rows).astype(jnp.bfloat16)
    grads = (d_in_proj, d_dt_proj, d_out_proj, d_floats[0], d_floats[1], d_floats[2], d_floats[3], d_floats[4], d_pre_gain, d_floats[5])
    return (d_input, grads)

def reference(boundary, lengths, in_proj, dt_proj, out_proj, conv_weight, conv_bias, dt_bias, a_log, d_skip, pre_gain, out_gain):
    stacks = (in_proj, dt_proj, out_proj, conv_weight, conv_bias, dt_bias, a_log, d_skip, pre_gain, out_gain)
    first = tuple((item[0] for item in stacks))
    second = tuple((item[1] for item in stacks))
    inputs = boundary[0].reshape(MICRO * SEQS, SEQ_LEN, D)
    cotangents = boundary[1].reshape(MICRO * SEQS, SEQ_LEN, D)
    counts = lengths.reshape(MICRO * SEQS)
    zeros_first = tuple((jnp.zeros(item.shape, jnp.float32) for item in first))
    zeros_second = tuple((jnp.zeros(item.shape, jnp.float32) for item in second))

    def per_sequence(carry, pieces):
        rows, cotangent, count = pieces
        hidden, stored_first = block_forward(rows, count, first)
        final, stored_second = block_forward(hidden, count, second)
        d_hidden, grads_second = block_backward(cotangent, hidden, stored_second, count, second)
        d_rows, grads_first = block_backward(d_hidden, rows, stored_first, count, first)
        acc_first = tuple((a + b for a, b in zip(carry[0], grads_first)))
        acc_second = tuple((a + b for a, b in zip(carry[1], grads_second)))
        return ((acc_first, acc_second), (hidden, final, d_rows, d_hidden))
    totals, outputs = lax.scan(per_sequence, (zeros_first, zeros_second), (inputs, cotangents, counts))
    hidden, final, d_rows, d_hidden = outputs
    activations = jnp.stack([hidden, final]).reshape(2, MICRO, SEQS, SEQ_LEN, D)
    input_grads = jnp.stack([d_rows, d_hidden]).reshape(2, MICRO, SEQS, SEQ_LEN, D)
    grads = tuple((jnp.stack([a, b]) for a, b in zip(totals[0], totals[1])))
    return (activations, input_grads, grads[0], grads[1], grads[2], grads[3], grads[4], grads[5], grads[6], grads[7], grads[8], grads[9])
```

```python
import functools

import jax
import jax.numpy as jnp
from jax import lax
from jax.experimental import pallas as pl
from jax.experimental.pallas import tpu as pltpu
from jax.sharding import PartitionSpec as P

BF = jnp.bfloat16
F32 = jnp.float32
HIGH = lax.Precision.HIGHEST
EPSILON = 1e-05
CHUNK = 128
LANES = 128
PAIR = 2


def mm(a, b):
    return jnp.dot(a.astype(BF), b.astype(BF), preferred_element_type=F32)


def mm_t(a, b):
    return lax.dot_general(a.astype(BF), b.astype(BF), (((1,), (1,)), ((), ())), preferred_element_type=F32)


def t_mm(a, b):
    return lax.dot_general(a.astype(BF), b.astype(BF), (((0,), (0,)), ((), ())), preferred_element_type=F32)


def rows_of(shape):
    return lax.broadcasted_iota(jnp.int32, shape, 0)


def lanes_of(shape):
    return lax.broadcasted_iota(jnp.int32, shape, 1)


def shift_down(v, steps):
    return jnp.where(rows_of(v.shape) >= steps, pltpu.roll(v, steps, 0), 0.0)


def shift_up(v, steps):
    size = v.shape[0]
    return jnp.where(rows_of(v.shape) < size - steps, pltpu.roll(v, size - steps, 0), 0.0)


def conv(v, taps_ref, taps):
    total = taps_ref[taps : taps + 1, :] + taps_ref[taps - 1 : taps, :] * v
    for k in range(taps - 1):
        total = total + taps_ref[k : k + 1, :] * shift_down(v, taps - 1 - k)
    return total


def conv_back(d_sum, v, taps_ref, taps):
    d_v = taps_ref[taps - 1 : taps, :] * d_sum
    d_taps = []
    for k in range(taps - 1):
        d_v = d_v + taps_ref[k : k + 1, :] * shift_up(d_sum, taps - 1 - k)
        d_taps.append(jnp.sum(d_sum * shift_down(v, taps - 1 - k), axis=0, keepdims=True))
    d_taps.append(jnp.sum(d_sum * v, axis=0, keepdims=True))
    d_taps.append(jnp.sum(d_sum, axis=0, keepdims=True))
    return d_v, d_taps


def head_map(width, head_dim):
    shape = (LANES, width)
    return (rows_of(shape) == lanes_of(shape) // head_dim).astype(BF)


def expand(v, spread):
    high = v.astype(BF)
    low = (v - high.astype(F32)).astype(BF)
    return mm(high, spread) + mm(low, spread)


def step_of(dt, ph_ref):
    pre = dt + ph_ref[0:1, :]
    step = jnp.maximum(pre, 0.0) + jnp.log1p(jnp.exp(-jnp.abs(pre)))
    rate = -jnp.exp(ph_ref[1:2, :])
    return pre, step, rate


def lower_mask():
    shape = (CHUNK, CHUNK)
    return rows_of(shape) >= lanes_of(shape)


def pair_rows(v, first):
    return jnp.concatenate([jnp.where(first, v, 0.0), jnp.where(first, 0.0, v)], axis=0)


def as_row(column):
    return jnp.broadcast_to(column, (CHUNK, LANES)).T[0:1, :]


def as_column(row):
    return jnp.broadcast_to(row, (CHUNK, LANES)).T[:, 0:1]


def forward_kernel(px_ref, pbc_ref, ph_ref, gate_ref, x_ref, bcdt_ref, *refs, taps, heads, with_dots):
    if with_dots:
        dmix_ref, gg_ref, y_ref, st_ref, ss_ref, dot_ref = refs
    else:
        gg_ref, y_ref, st_ref, ss_ref = refs
    width = x_ref.shape[1]
    head_dim = width // heads
    states = pbc_ref.shape[1] // 2
    spread = head_map(width, head_dim)
    bcdt = bcdt_ref[...].astype(F32)
    sums = conv(bcdt[:, : 2 * states], pbc_ref, taps)
    bc = sums * jax.nn.sigmoid(sums)
    _, step, rate = step_of(bcdt[:, 2 * states :], ph_ref)
    decay = rate * step
    sums = conv(x_ref[...].astype(F32), px_ref, taps)
    act = sums * jax.nn.sigmoid(sums)
    xs = act * expand(step, spread)
    lower = lower_mask()
    tri = lower.astype(F32)
    first = lanes_of((CHUNK, 2 * head_dim)) < head_dim
    state = None
    chunks = x_ref.shape[0] // CHUNK
    for c in range(chunks):
        span = slice(c * CHUNK, (c + 1) * CHUNK)
        cum = jnp.dot(tri, decay[span], precision=HIGH, preferred_element_type=F32)
        cum_t = cum.T
        b_c = bc[span, :states].astype(BF)
        c_c = bc[span, states:].astype(BF)
        scores = mm_t(c_c, b_c)
        xs_c = xs[span]
        pieces = []
        for p in range(heads // 2):
            two = slice(p * 2 * head_dim, (p + 1) * 2 * head_dim)
            mixes = []
            for h in (2 * p, 2 * p + 1):
                gap = jnp.minimum(cum[:, h : h + 1] - cum_t[h : h + 1, :], 0.0)
                mixes.append(jnp.where(lower, jnp.exp(gap) * scores, 0.0).astype(BF))
            pieces.append(mm(jnp.concatenate(mixes, axis=1), pair_rows(xs_c[:, two], first)))
        y = jnp.concatenate(pieces, axis=1)
        if c > 0:
            y = y + mm(c_c, state) * expand(jnp.exp(cum), spread)
        if c + 1 < chunks:
            last = cum[CHUNK - 1 : CHUNK, :]
            fresh = t_mm(b_c, xs_c * expand(jnp.exp(last - cum), spread))
            state = fresh if c == 0 else fresh + state * expand(jnp.exp(jnp.broadcast_to(last, (states, LANES))), spread)
            st_ref[c] = state
        y = y + px_ref[taps + 1 : taps + 2, :] * act[span]
        y_low = y.astype(BF)
        y_ref[span, :] = y_low
        y = y_low.astype(F32)
        gate = gate_ref[span, :].astype(F32)
        gated = y * (gate * jax.nn.sigmoid(gate))
        ss_ref[c : c + 1, :] = as_row(jnp.sum(gated * gated, axis=1, keepdims=True))
        gg = gated * px_ref[taps + 2 : taps + 3, :]
        gg_ref[span, :] = gg.astype(BF)
        if with_dots:
            dot_ref[c : c + 1, :] = as_row(jnp.sum(gg * dmix_ref[span, :].astype(F32), axis=1, keepdims=True))


def backward_kernel(
    px_ref, pbc_ref, ph_ref, gate_ref, x_ref, bcdt_ref, y_ref, st_ref, dmix_ref, sc_ref,
    dgate_ref, dx_ref, dbcdt_ref, small_ref, *, taps, heads,
):
    length, width = x_ref.shape
    head_dim = width // heads
    states = pbc_ref.shape[1] // 2
    spread = head_map(width, head_dim)

    @pl.when(pl.program_id(0) == 0)
    def _():
        small_ref[...] = jnp.zeros_like(small_ref)

    gx_ref = small_ref.at[:, :width]
    gbc_ref = small_ref.at[:, width : width + 2 * states]
    gh_ref = small_ref.at[:, width + 2 * states :]

    gate = gate_ref[...].astype(F32)
    y = y_ref[...].astype(F32)
    dmix = dmix_ref[...].astype(F32)
    chunks = length // CHUNK
    r = jnp.concatenate([as_column(sc_ref[c : c + 1, :]) for c in range(chunks)], axis=0)
    coef = jnp.concatenate([as_column(sc_ref[chunks + c : chunks + c + 1, :]) for c in range(chunks)], axis=0)
    sig = jax.nn.sigmoid(gate)
    gated = y * gate * sig
    gx_ref[taps + 2 : taps + 3, :] += jnp.sum(dmix * gated * r, axis=0, keepdims=True)
    dgated = r * px_ref[taps + 2 : taps + 3, :] * dmix - coef * gated
    dgate_ref[...] = (dgated * y * (sig * (1.0 + gate * (1.0 - sig)))).astype(BF)
    dy = dgated * gate * sig

    bcdt = bcdt_ref[...].astype(F32)
    bc_in = bcdt[:, : 2 * states]
    bc_sum = conv(bc_in, pbc_ref, taps)
    bc_sig = jax.nn.sigmoid(bc_sum)
    bc = bc_sum * bc_sig
    pre, step, rate = step_of(bcdt[:, 2 * states :], ph_ref)
    decay = rate * step
    x_in = x_ref[...].astype(F32)
    x_sum = conv(x_in, px_ref, taps)
    x_sig = jax.nn.sigmoid(x_sum)
    act = x_sum * x_sig
    step_wide = expand(step, spread)
    xs = act * step_wide
    gx_ref[taps + 1 : taps + 2, :] += jnp.sum(dy * act, axis=0, keepdims=True)

    lower = lower_mask()
    tri = lower.astype(F32)
    upper = (rows_of((CHUNK, CHUNK)) <= lanes_of((CHUNK, CHUNK))).astype(F32)
    last_row = rows_of((CHUNK, LANES)) == CHUNK - 1
    head_lane = lanes_of((CHUNK, LANES))
    head_row = rows_of((LANES, CHUNK))
    first = lanes_of((CHUNK, 2 * head_dim)) < head_dim
    d_state = None
    d_xs, d_bc, d_decay = [None] * chunks, [None] * chunks, [None] * chunks
    for c in reversed(range(chunks)):
        span = slice(c * CHUNK, (c + 1) * CHUNK)
        cum = jnp.dot(tri, decay[span], precision=HIGH, preferred_element_type=F32)
        cum_t = cum.T
        b_c = bc[span, :states].astype(BF)
        c_c = bc[span, states:].astype(BF)
        xs_c = xs[span]
        dy_c = dy[span]
        scores = mm_t(c_c, b_c)
        d_scores = jnp.zeros((CHUNK, CHUNK), F32)
        by_row = jnp.zeros((CHUNK, LANES), F32)
        by_col = jnp.zeros((LANES, CHUNK), F32)
        pieces = []
        for p in range(heads // 2):
            two = slice(p * 2 * head_dim, (p + 1) * 2 * head_dim)
            dy_two = pair_rows(dy_c[:, two], first).astype(BF)
            d_mix = mm_t(dy_two, xs_c[:, two])
            mixes = []
            for i, h in enumerate((2 * p, 2 * p + 1)):
                gap = jnp.minimum(cum[:, h : h + 1] - cum_t[h : h + 1, :], 0.0)
                fall = jnp.where(lower, jnp.exp(gap), 0.0)
                mixes.append((fall * scores).astype(BF))
                d_fall = d_mix[i * CHUNK : (i + 1) * CHUNK] * fall
                d_scores = d_scores + d_fall
                both = d_fall * scores
                by_row = jnp.where(head_lane == h, jnp.sum(both, axis=1, keepdims=True), by_row)
                by_col = jnp.where(head_row == h, jnp.sum(both, axis=0, keepdims=True), by_col)
            pieces.append(t_mm(jnp.concatenate(mixes, axis=0), dy_two))
        d_xs_c = jnp.concatenate(pieces, axis=1)
        d_c = mm(d_scores, b_c)
        d_b = t_mm(d_scores, c_c)
        d_cum = by_row - by_col.T
        new_state = None
        if c > 0:
            before = st_ref[c - 1]
            grow = expand(jnp.exp(cum), spread)
            d_off = dy_c * grow
            new_state = t_mm(c_c, d_off)
            d_c = d_c + mm_t(d_off, before)
            d_cum = d_cum + mm_t(d_off * mm(c_c, before), spread)
        if c + 1 < chunks:
            last = cum[CHUNK - 1 : CHUNK, :]
            tail = expand(jnp.exp(last - cum), spread)
            tailed = xs_c * tail
            d_tailed = mm(b_c, d_state)
            d_b = d_b + mm_t(tailed, d_state)
            d_xs_c = d_xs_c + d_tailed * tail
            lost = mm_t(d_tailed * tailed, spread)
            d_last = jnp.sum(lost, axis=0, keepdims=True)
            if c > 0:
                whole = expand(jnp.exp(jnp.broadcast_to(last, (states, LANES))), spread)
                d_last = d_last + jnp.sum(mm_t(d_state * before * whole, spread), axis=0, keepdims=True)
                new_state = new_state + d_state * whole
            d_cum = d_cum - lost + jnp.where(last_row, d_last, 0.0)
        d_state = new_state
        d_xs[c] = d_xs_c
        d_bc[c] = jnp.concatenate([d_b, d_c], axis=1)
        d_decay[c] = jnp.dot(upper, d_cum, precision=HIGH, preferred_element_type=F32)
    d_xs = jnp.concatenate(d_xs, axis=0)
    d_bc = jnp.concatenate(d_bc, axis=0)
    d_decay = jnp.concatenate(d_decay, axis=0)

    d_step = mm_t(act * d_xs, spread) + d_decay * rate
    gh_ref[1:2, :] += jnp.sum(d_decay * decay, axis=0, keepdims=True)
    d_dt = d_step * jax.nn.sigmoid(pre)
    gh_ref[0:1, :] += jnp.sum(d_dt, axis=0, keepdims=True)

    d_act = dy * px_ref[taps + 1 : taps + 2, :] + d_xs * step_wide
    d_sum = d_act * (x_sig * (1.0 + x_sum * (1.0 - x_sig)))
    d_x, d_taps = conv_back(d_sum, x_in, px_ref, taps)
    dx_ref[...] = d_x.astype(BF)
    for k, value in enumerate(d_taps):
        gx_ref[k : k + 1, :] += value
    d_sum = d_bc * (bc_sig * (1.0 + bc_sum * (1.0 - bc_sig)))
    d_bc_in, d_taps = conv_back(d_sum, bc_in, pbc_ref, taps)
    for k, value in enumerate(d_taps):
        gbc_ref[k : k + 1, :] += value
    dbcdt_ref[:, : 2 * states] = d_bc_in.astype(BF)
    dbcdt_ref[:, 2 * states :] = d_dt.astype(BF)


def per_seq(*dims):
    return pl.BlockSpec((None,) + dims, lambda i: (i,) + (0,) * len(dims))


def fixed(*dims):
    return pl.BlockSpec(dims, lambda i: (0,) * len(dims))


PARAMS = pltpu.CompilerParams(dimension_semantics=("arbitrary",), vmem_limit_bytes=60 << 20)


def run_forward(small, gate, x, bcdt, dmix, taps, heads):
    px, pbc, ph = small
    seqs, length, width = x.shape
    states = pbc.shape[1] // 2
    chunks = length // CHUNK
    more = [] if dmix is None else [dmix]
    sums = [jax.ShapeDtypeStruct((seqs, chunks, LANES), F32)] * (1 + len(more))
    return pl.pallas_call(
        functools.partial(forward_kernel, taps=taps, heads=heads, with_dots=bool(more)),
        grid=(seqs,),
        in_specs=[fixed(*px.shape), fixed(*pbc.shape), fixed(*ph.shape), per_seq(length, width), per_seq(length, width), per_seq(length, bcdt.shape[2])]
        + [per_seq(length, width)] * len(more),
        out_specs=[per_seq(length, width), per_seq(length, width), per_seq(chunks - 1, states, width)] + [per_seq(chunks, LANES)] * len(sums),
        out_shape=[
            jax.ShapeDtypeStruct((seqs, length, width), BF),
            jax.ShapeDtypeStruct((seqs, length, width), BF),
            jax.ShapeDtypeStruct((seqs, chunks - 1, states, width), F32),
        ]
        + sums,
        compiler_params=PARAMS,
        cost_estimate=pl.CostEstimate(flops=seqs * 400_000_000, bytes_accessed=seqs * 4_000_000, transcendentals=seqs * 2_000_000),
        name="mix_forward",
    )(px, pbc, ph, gate, x, bcdt, *more)


def run_backward(small, gate, x, bcdt, y, state, dmix, scalars, taps, heads):
    px, pbc, ph = small
    seqs, length, width = x.shape
    smalls = px.shape[1] + pbc.shape[1] + ph.shape[1]
    return pl.pallas_call(
        functools.partial(backward_kernel, taps=taps, heads=heads),
        grid=(seqs,),
        in_specs=[
            fixed(*px.shape), fixed(*pbc.shape), fixed(*ph.shape), per_seq(length, width), per_seq(length, width),
            per_seq(length, bcdt.shape[2]), per_seq(length, width), per_seq(*state.shape[1:]), per_seq(length, width), per_seq(*scalars.shape[1:]),
        ],
        out_specs=[per_seq(length, width), per_seq(length, width), per_seq(length, bcdt.shape[2]), fixed(8, smalls)],
        out_shape=[
            jax.ShapeDtypeStruct((seqs, length, width), BF),
            jax.ShapeDtypeStruct((seqs, length, width), BF),
            jax.ShapeDtypeStruct((seqs, length, bcdt.shape[2]), BF),
            jax.ShapeDtypeStruct((8, smalls), F32),
        ],
        compiler_params=PARAMS,
        cost_estimate=pl.CostEstimate(flops=seqs * 1_200_000_000, bytes_accessed=seqs * 6_000_000, transcendentals=seqs * 4_000_000),
        name="mix_backward",
    )(px, pbc, ph, gate, x, bcdt, y, state, dmix, scalars)


MESH = pl.DeviceIdType.MESH
VM = pl.BlockSpec(memory_space=pltpu.VMEM)


def partners():
    section = lax.axis_index("section")
    rep = lax.axis_index("rep")
    xb = rep % PAIR
    return section, xb, {"section": 1 - section}, {"rep": rep + 1 - 2 * xb}


def greet(*devices):
    barrier = pltpu.get_barrier_semaphore()
    for device in devices:
        pl.semaphore_signal(barrier, inc=1, device_id=device, device_id_type=MESH)
    pl.semaphore_wait(barrier, len(devices))


def remote(src, dst, send, recv, device):
    return pltpu.make_async_remote_copy(src_ref=src, dst_ref=dst, send_sem=send, recv_sem=recv, device_id=device, device_id_type=MESH)


def sums_kernel(v_ref, out_ref, got_ref, half_ref, send, recv):
    _, _, peer, beside = partners()
    greet(peer, beside)
    first = remote(v_ref, got_ref.at[0], send.at[0], recv.at[0], peer)
    first.start()
    first.wait()
    half_ref[...] = v_ref[...] + got_ref[0]
    second = remote(half_ref, got_ref.at[1], send.at[1], recv.at[1], beside)
    second.start()
    second.wait()
    out_ref[...] = half_ref[...] + got_ref[1]


def run_sums(v, collective_id):
    return pl.pallas_call(
        sums_kernel,
        in_specs=[VM],
        out_specs=VM,
        out_shape=jax.ShapeDtypeStruct(v.shape, F32),
        scratch_shapes=[pltpu.VMEM((2,) + v.shape, F32), pltpu.VMEM(v.shape, F32), pltpu.SemaphoreType.DMA((2,)), pltpu.SemaphoreType.DMA((2,))],
        compiler_params=pltpu.CompilerParams(collective_id=collective_id, has_side_effects=True),
        cost_estimate=pl.CostEstimate(flops=10_000_000, bytes_accessed=20_000_000, transcendentals=0),
        name="token_sums",
    )(v)


def exchange(part_ref, got_a, held, got_x, send, recv, use):
    section, _, peer, beside = partners()
    per = part_ref.shape[1] // CHUNK
    steps = PAIR * per

    def at(i):
        return i // per, pl.ds(pl.multiple_of(i % per * CHUNK, CHUNK), CHUNK)

    def to_peer(i):
        x, span = at(i)
        return remote(part_ref.at[x * 2 + 1 - section, span], got_a.at[i], send.at[0, i], recv.at[0, i], peer)

    def to_beside(i):
        return remote(held.at[i], got_x.at[i], send.at[1, i], recv.at[1, i], beside)

    def start_peer(i, _):
        to_peer(i).start()
        return 0

    def add(i, _):
        to_peer(i).wait_recv()
        x, span = at(i)
        held[i] = (part_ref[x * 2 + section, span].astype(F32) + got_a[i].astype(F32)).astype(BF)

        @pl.when(i > 0)
        def _():
            to_beside(i - 1).start()

        return 0

    def finish(i):
        to_beside(i).wait_recv()
        x, span = at(i)
        use(i, x, span, held[i].astype(F32) + got_x[i].astype(F32))

    def drain(i, _):
        to_peer(i).wait_send()
        to_beside(i).wait_send()
        return 0

    lax.fori_loop(0, steps, start_peer, 0)
    yield
    lax.fori_loop(0, steps, add, 0)
    yield
    to_beside(steps - 1).start()
    yield
    for i in range(steps):
        finish(i)
        yield
    lax.fori_loop(0, steps, drain, 0)


def weights_flow(b, q_ref, o_ref, w_in, w_out, qs, qr, os_, or_, *, ns, ny, split=False):
    section, xb, peer, _ = partners()
    z = lax.axis_index("shard")
    yb = lax.axis_index("rep") // PAIR
    half = ns // 2
    part = q_ref.shape[2] // PARTS
    home = z // half

    def y_peer(k):
        return {"rep": (yb + k) % ny * PAIR + xb}

    def rows_at(h):
        return pl.ds(h * part, part)

    def there(way):
        return z < ns - 1 if way > 0 else z > 0

    def first(t, way, h):
        return remote(q_ref.at[t, yb, rows_at(h)], w_in.at[yb, z, rows_at(h)], qs.at[0, t * 2 + (way + 1) // 2, h], qr.at[yb, z, h],
                      {"section": t, "shard": z + way})

    def chip(j, h):
        return remote(q_ref.at[1 - b, j, rows_at(h)], w_in.at[j, z, rows_at(h)], qs.at[1, j, h], qr.at[j, z, h], peer)

    def stay(j, h):
        return pltpu.make_async_copy(q_ref.at[b, j, rows_at(h)], w_in.at[j, z, rows_at(h)], qs.at[2 + ny, j, h])

    def onward(place, way, h):
        block = w_in.at[yb, place, rows_at(h)]
        return remote(block, block, qs.at[2, place, h], qr.at[yb, place, h], {"shard": z + way})

    def across(place, k, h):
        block = w_in.at[yb, place, rows_at(h)]
        return remote(block, block, qs.at[2 + k, place, h], qr.at[yb, place, h], y_peer(k))

    def arrival(j, place, h):
        block = w_in.at[j, place, rows_at(h)]
        return remote(block, block, qs.at[2, place, h], qr.at[j, place, h], peer)

    def o_first(way):
        return remote(o_ref.at[yb], w_out.at[z % half, yb], os_.at[0, (way + 1) // 2], or_.at[z % half, yb], {"section": home, "shard": z + way})

    def o_chip(j):
        return remote(o_ref.at[j], w_out.at[z % half, j], os_.at[1, j], or_.at[z % half, j], peer)

    def o_stay(j):
        return pltpu.make_async_copy(o_ref.at[j], w_out.at[z % half, j], os_.at[1, j])

    def o_onward(k, way):
        block = w_out.at[k, yb]
        return remote(block, block, os_.at[2, k], or_.at[k, yb], {"shard": z + way})

    def o_across(k, i):
        block = w_out.at[k, yb]
        return remote(block, block, os_.at[2 + i, k], or_.at[k, yb], y_peer(i))

    def o_arrival(k, j):
        block = w_out.at[k, j]
        return remote(block, block, os_.at[2, k], or_.at[k, j], peer)

    def start_in():
        @pl.when(section == b)
        def _():
            for h in range(PARTS):
                for way in (1, -1):
                    @pl.when(there(way))
                    def _():
                        for t in range(2):
                            first(t, way, h).start()

    def start_out():
        @pl.when(section == b)
        def _():
            for way in (1, -1):
                @pl.when(there(way))
                def _():
                    o_first(way).start()
            for j in range(ny):
                @pl.when(home == b)
                def _():
                    o_stay(j).start()

                @pl.when(home != b)
                def _():
                    o_chip(j).start()

    def start_chip():
        @pl.when(section == b)
        def _():
            for j in range(ny):
                for h in range(PARTS):
                    chip(j, h).start()
                    stay(j, h).start()

    def relay_in(d, h=None):
        for h in range(PARTS) if h is None else (h,):
            for way in (1, -1):
                place = z - way * d

                @pl.when((place >= 0) & (place < ns))
                def _():
                    arrival(yb, place, h).wait_recv()

                    @pl.when(there(way))
                    def _():
                        onward(place, way, h).start()

                    for k in range(1, ny):
                        across(place, k, h).start()

    def relay_out(d):
        for way in (1, -1):
            place = z - way * d
            k = place - section * half

            @pl.when((place >= 0) & (place < ns) & (k >= 0) & (k < half))
            def _():
                o_arrival(k, yb).wait_recv()

                @pl.when(there(way))
                def _():
                    o_onward(k, way).start()

                for i in range(1, ny):
                    o_across(k, i).start()

    def finish_in():
        for place in range(ns):
            @pl.when(place != z)
            def _():
                for h in range(PARTS):
                    for k in range(1, ny):
                        arrival((yb + k) % ny, place, h).wait_recv()
                        across(place, k, h).wait_send()

                    @pl.when(jnp.where(place < z, z < ns - 1, z > 0))
                    def _():
                        onward(place, 1, h).wait_send()

        @pl.when(section != b)
        def _():
            for j in range(ny):
                for h in range(PARTS):
                    arrival(j, z, h).wait_recv()

        @pl.when(section == b)
        def _():
            for way in (1, -1):
                @pl.when(there(way))
                def _():
                    for h in range(PARTS):
                        for t in range(2):
                            first(t, way, h).wait_send()
            for j in range(ny):
                for h in range(PARTS):
                    chip(j, h).wait_send()
                    stay(j, h).wait()

    def finish_out():
        @pl.when((section != b) & (home != b))
        def _():
            for j in range(ny):
                o_arrival(z % half, j).wait_recv()

        for k in range(half):
            place = section * half + k

            @pl.when(place != z)
            def _():
                for i in range(1, ny):
                    o_arrival(k, (yb + i) % ny).wait_recv()
                    o_across(k, i).wait_send()

                @pl.when(jnp.where(place < z, z < ns - 1, z > 0))
                def _():
                    o_onward(k, 1).wait_send()

        @pl.when(section == b)
        def _():
            for way in (1, -1):
                @pl.when(there(way))
                def _():
                    o_first(way).wait_send()
            for j in range(ny):
                @pl.when(home == b)
                def _():
                    o_stay(j).wait()

                @pl.when(home != b)
                def _():
                    o_chip(j).wait_send()

    def start():
        start_in()
        start_out()
        start_chip()

    def relay(d):
        relay_in(d)
        relay_out(d)

    def finish():
        finish_in()
        finish_out()

    if split:
        return start, relay_in, relay_out, finish
    return start, relay, finish


def weights_shapes(q, o, ns):
    ny = q.shape[1]
    outs = [
        jax.ShapeDtypeStruct((ny, ns) + q.shape[2:], BF),
        jax.ShapeDtypeStruct((ns // 2,) + o.shape, BF),
    ]
    dma = pltpu.SemaphoreType.DMA
    sems = [dma((3 + ny, max(ns, 4), PARTS)), dma((ny, ns, PARTS)), dma((2 + ny, max(ns, 2))), dma((ns // 2, ny))]
    return outs, sems


def greet_line(ns, ny):
    section, xb, peer, beside = partners()
    z = lax.axis_index("shard")
    yb = lax.axis_index("rep") // PAIR
    found = [peer, beside] + [{"rep": (yb + k) % ny * PAIR + xb} for k in range(1, ny)]
    for k in (1, ns - 1):
        found += [{"shard": (z + k) % ns}, {"section": 1 - section, "shard": (z + k) % ns}]
    greet(*found)


def start_kernel(tokens_ref, counts_ref, cw_ref, cb_ref, dtb_ref, alg_ref, dsk_ref, pgn_ref, ogn_ref, bc_ref, dt_ref, q_ref, o_ref,
                 all_tokens, normed_ref, live_out_ref, live_ref, px_ref, pbc_ref, ph_ref, gain_ref, wbc_ref, w_in, w_out,
                 small, all_small, mine, packs, full, row8, all_counts,
                 qs, qr, os_, or_, ts, tr, ss, sr, ps, pr, cs, cr, *, ns, ny, taps, heads):
    section, xb, peer, beside = partners()
    z = lax.axis_index("shard")
    yb = lax.axis_index("rep") // PAIR
    half = ns // 2
    greet_all(ns, ny)
    start, relay, finish = weights_flow(0, q_ref, o_ref, w_in, w_out, qs, qr, os_, or_, ns=ns, ny=ny)

    part = cw_ref.shape[1]
    mine[...] = jnp.zeros_like(mine)
    mine[0:taps, :part] = cw_ref[...].astype(F32)
    mine[taps : taps + 1, :part] = cb_ref[...].astype(F32)
    for i, ref in enumerate((pgn_ref, ogn_ref, dtb_ref, alg_ref, dsk_ref)):
        mine[taps + 1 + i : taps + 2 + i, : ref.shape[1]] = ref[...].astype(F32)

    def pack_to(t, k):
        return remote(mine, packs.at[section, z], ps.at[t, k], pr.at[section, z], {"section": t, "shard": (z + k) % ns})

    def pack_from(t, place):
        return remote(mine, packs.at[t, place], ps.at[0, 0], pr.at[t, place], peer)

    counts = remote(counts_ref, all_counts.at[xb], cs, cr, beside)
    counts.start()
    for k in range(1, ns):
        for t in range(2):
            pack_to(t, k).start()
    remote(mine, packs.at[section, z], ps.at[0, 0], pr.at[section, z], peer).start()
    packs[section, z] = mine[...]
    all_counts[xb] = counts_ref[...]

    def there(way):
        return z < ns - 1 if way > 0 else z > 0

    lanes = bc_ref.shape[1]
    rows = bc_ref.shape[0] // ny
    for j in range(ny):
        small[j] = jnp.zeros_like(small[j])
        small[j, :, :lanes] = bc_ref[j * rows : (j + 1) * rows]
        small[j, :, lanes : lanes + heads] = dt_ref[j * rows : (j + 1) * rows]

    def first(way):
        return remote(small.at[yb], all_small.at[section, z, yb], ss.at[0, (way + 1) // 2, 0], sr.at[section, z, yb], {"shard": z + way})

    def held(place, j):
        return all_small.at[section, place, j]

    def onward(place, way):
        return remote(held(place, yb), held(place, yb), ss.at[1, place, 0], sr.at[section, place, yb], {"shard": z + way})

    def across(place, k):
        return remote(held(place, yb), held(place, yb), ss.at[1 + k, place, 0], sr.at[section, place, yb], {"rep": (yb + k) % ny * PAIR + xb})

    def chip(place, j):
        return remote(held(place, j), held(place, j), ss.at[1 + ny, place, j], sr.at[section, place, j], peer)

    def arrival(b, place, j):
        return remote(all_small.at[b, place, j], all_small.at[b, place, j], ss.at[1, place, 0], sr.at[b, place, j], peer)

    for way in (1, -1):
        @pl.when(there(way))
        def _():
            first(way).start()

    def tokens_beside(m):
        return remote(tokens_ref.at[m], all_tokens.at[section, xb, m], ts.at[0, m], tr.at[section, xb, m], beside)

    def tokens_chip(x, m):
        if x is None:
            return remote(tokens_ref.at[m], all_tokens.at[section, xb, m], ts.at[1, m], tr.at[section, xb, m], peer)
        place = all_tokens.at[section, x, m]
        return remote(place, place, ts.at[2, m], tr.at[section, x, m], peer)

    def tokens_arrival(b, x, m):
        place = all_tokens.at[b, x, m]
        return remote(place, place, ts.at[0, m], tr.at[b, x, m], peer)

    micro, seq_len, width = tokens_ref.shape
    start()
    for m in range(micro):
        tokens_beside(m).start()
        tokens_chip(None, m).start()
        all_tokens[section, xb, m] = tokens_ref[m]
    for j in range(ny):
        all_small[section, z, j] = small[j]

    def relay_small(d):
        for way in (1, -1):
            place = z - way * d

            @pl.when((place >= 0) & (place < ns))
            def _():
                arrival(section, place, yb).wait_recv()

                @pl.when(there(way))
                def _():
                    onward(place, way).start()

                for k in range(1, ny):
                    across(place, k).start()
                chip(place, yb).start()

    def unpack():
        channels = part * ns
        inner = ogn_ref.shape[1] * ns
        cw = inner // ns // PAIR
        unit = dtb_ref.shape[1] // PAIR
        mine_w = half * cw
        for k in range(1, ns):
            for t in range(2):
                pack_from(t, (z + k) % ns).wait_recv()
        pack_from(1 - section, z).wait_recv()
        ph_ref[...] = jnp.zeros_like(ph_ref)
        px_ref[...] = jnp.zeros_like(px_ref)
        pbc_ref[...] = jnp.zeros_like(pbc_ref)
        spread = head_map(mine_w, 2 * PAIR * mine_w // heads)
        for b in range(2):
            for at in range(ns):
                full[0 : taps + 1, at * part : (at + 1) * part] = packs[b, at, 0 : taps + 1, :part]
                size = pgn_ref.shape[1]
                gain_ref[b, :, at * size : (at + 1) * size] = packs[b, at, taps + 1 : taps + 2, :size]
            pbc_ref[b, 0 : taps + 1, :] = full[0 : taps + 1, inner:channels]
            row8[...] = jnp.zeros_like(row8)
            for t in range(2):
                for q in range(PAIR):
                    @pl.when((section == t) & (xb == q))
                    def _():
                        for k in range(half):
                            at = t * half + k
                            col = (at * PAIR + q) * cw
                            put = slice(k * cw, (k + 1) * cw)
                            lane = slice(k * unit, (k + 1) * unit)
                            take = slice(q * unit, (q + 1) * unit)
                            px_ref[b, 0 : taps + 1, put] = full[0 : taps + 1, col : col + cw]
                            px_ref[b, taps + 2 : taps + 3, put] = packs[b, at, taps + 2 : taps + 3, q * cw : (q + 1) * cw]
                            ph_ref[b, 0:1, lane] = packs[b, at, taps + 3 : taps + 4, take]
                            ph_ref[b, 1:2, lane] = packs[b, at, taps + 4 : taps + 5, take]
                            row8[0:1, lane] = packs[b, at, taps + 5 : taps + 6, take]
            px_ref[b, taps + 1 : taps + 2, :] = mm(row8[...], spread)[0:1]

    def shared_columns():
        unit = dtb_ref.shape[1] // PAIR
        shape = (wbc_ref.shape[2] - lanes, LANES)
        source, head = rows_of(shape), lanes_of(shape)
        wanted = ((section * half + head // unit) * PAIR + xb) * unit + head % unit
        chosen = ((source == wanted) & (head < half * unit)).astype(BF)
        for b in range(2):
            for at in range(ns):
                for j in range(ny):
                    low = (at * ny + j) * rows
                    wbc_ref[b, low : low + rows, :lanes] = all_small[b, at, j, :, :lanes]
                    wbc_ref[b, low : low + rows, lanes:] = mm(all_small[b, at, j, :, lanes:], chosen).astype(BF)

    def prepare():
        per = seq_len // CHUNK
        for x in range(PAIR):
            for m in range(micro):
                for c in range(per):
                    row = (x * micro + m) * per + c
                    at = lanes_of((1, LANES)).astype(F32) + float(c * CHUNK)
                    live_ref[row : row + 1, :] = (at < all_counts[x, m : m + 1, :]).astype(F32)

        def step(i, _):
            x, m, c = i // (micro * per), i // per % micro, i % per
            span = pl.ds(pl.multiple_of(c * CHUNK, CHUNK), CHUNK)
            wide = all_tokens[0, x, m, span].astype(F32)
            normed_ref[x * micro + m, span] = (wide * rms(wide) * gain_ref[0]).astype(BF)
            live = as_column(live_ref[pl.ds(i, 1), :])
            live_out_ref[x * micro + m, span] = (all_tokens[1, x, m, span].astype(F32) * live).astype(BF)
            return 0

        lax.fori_loop(0, PAIR * micro * per, step, 0)

    relay_small(1)
    for j in range(ny):
        chip(z, j).start()
    for d in range(1, ns):
        if d == ns - 1:
            unpack()
            for m in range(micro):
                tokens_arrival(section, 1 - xb, m).wait_recv()
                tokens_chip(1 - xb, m).start()
            counts.wait_send()
            remote(counts_ref, all_counts.at[1 - xb], cs, cr, beside).wait_recv()
            for m in range(micro):
                for x in range(PAIR):
                    tokens_arrival(1 - section, x, m).wait_recv()
            prepare()
        relay(d)
        if d + 1 < ns:
            relay_small(d + 1)
    for place in range(ns):
        @pl.when(place != z)
        def _():
            for k in range(1, ny):
                j = (yb + k) % ny
                arrival(section, place, j).wait_recv()
                chip(place, j).start()
    for place in range(ns):
        for j in range(ny):
            arrival(1 - section, place, j).wait_recv()
    shared_columns()
    finish()
    for m in range(micro):
        tokens_beside(m).wait_send()
        tokens_chip(None, m).wait_send()
        tokens_chip(1 - xb, m).wait_send()
    for k in range(1, ns):
        for t in range(2):
            pack_to(t, k).wait_send()
    pack_from(section, z).wait_send()
    for way in (1, -1):
        @pl.when(there(way))
        def _():
            first(way).wait_send()
    for place in range(ns):
        for j in range(ny):
            chip(place, j).wait_send()

        @pl.when(place != z)
        def _():
            for k in range(1, ny):
                across(place, k).wait_send()

            @pl.when(jnp.where(place < z, z < ns - 1, z > 0))
            def _():
                onward(place, 1).wait_send()


def greet_all(ns, ny):
    section, xb, peer, beside = partners()
    z = lax.axis_index("shard")
    yb = lax.axis_index("rep") // PAIR
    found = [peer, beside] + [{"rep": (yb + k) % ny * PAIR + xb} for k in range(1, ny)]
    for k in range(1, ns):
        found += [{"shard": (z + k) % ns}, {"section": 1 - section, "shard": (z + k) % ns}]
    greet(*found)


def run_start(tokens, counts, smalls, bc, dt, q, o, heads):
    conv_weight, conv_bias, dt_bias, a_log, d_skip, pre_gain, out_gain = smalls
    ny = q.shape[1]
    ns = heads // dt_bias.shape[1]
    micro, seq_len, width = tokens.shape
    taps = conv_weight.shape[0]
    inner = out_gain.shape[1] * ns
    mine_w = inner // (2 * PAIR)
    states2 = bc.shape[1]
    seqs = PAIR * micro
    outs, sems = weights_shapes(q, o, ns)
    dma = pltpu.SemaphoreType.DMA
    hbm = pl.BlockSpec(memory_space=pl.ANY)
    shape = jax.ShapeDtypeStruct
    rows = bc.shape[0] // ny
    pack = (16, -(-max(conv_weight.shape[1], out_gain.shape[1]) // LANES) * LANES)
    return pl.pallas_call(
        functools.partial(start_kernel, ns=ns, ny=ny, taps=taps, heads=heads),
        in_specs=[VM] * 13,
        out_specs=[VM] * 9 + [hbm, hbm],
        out_shape=[
            shape((2, PAIR) + tokens.shape, BF),
            shape((seqs, seq_len, width), BF),
            shape((seqs, seq_len, width), BF),
            shape((seqs * seq_len // CHUNK, LANES), F32),
            shape((2, 8, mine_w), F32),
            shape((2, 8, states2), F32),
            shape((2, 8, LANES), F32),
            shape((2, 1, width), F32),
            shape((2, width, states2 + LANES), BF),
        ]
        + outs,
        scratch_shapes=[
            pltpu.VMEM((ny, rows, states2 + LANES), BF),
            pltpu.VMEM((2, ns, ny, rows, states2 + LANES), BF),
            pltpu.VMEM(pack, F32),
            pltpu.VMEM((2, ns) + pack, F32),
            pltpu.VMEM((8, conv_weight.shape[1] * ns), F32),
            pltpu.VMEM((8, LANES), F32),
            pltpu.VMEM((PAIR,) + counts.shape, F32),
        ]
        + sems
        + [
            dma((3, 2)), dma((2, PAIR, 2)), dma((2 + ny, max(ns, 2), ny)), dma((2, ns, ny)),
            dma((2, ns)), dma((2, ns)), dma(()), dma(()),
        ],
        compiler_params=comm_params(5),
        cost_estimate=pl.CostEstimate(flops=50_000_000, bytes_accessed=200_000_000, transcendentals=0),
        name="start",
    )(tokens, counts, *smalls, bc, dt, q, o)


def rms(v):
    return lax.rsqrt(jnp.mean(v * v, axis=-1, keepdims=True) + EPSILON)


def spread_out(out_ref, send, recv, peer, section, per):
    def copy(i, owner):
        span = pl.ds(pl.multiple_of(i % per * CHUNK, CHUNK), CHUNK)
        place = out_ref.at[i // per * 2 + owner, span]
        return remote(place, place, send.at[2, i], recv.at[2, i], peer)

    return copy


def onward_kernel(part_ref, rows_ref, sums_ref, live_ref, gain_ref, q_ref, o_ref, hidden_ref, normed_ref, rate_ref, gain_out_ref, w_in, w_out,
                  got_a, held, got_x, got_s, half_s, send, recv, send_s, recv_s, qs, qr, os_, or_, *, inner, ns, ny):
    section, _, peer, beside = partners()
    per = part_ref.shape[1] // CHUNK
    steps = PAIR * per
    greet_line(ns, ny)
    start, relay_in, relay_out, finish = weights_flow(1, q_ref, o_ref, w_in, w_out, qs, qr, os_, or_, ns=ns, ny=ny, split=True)
    first = remote(sums_ref, got_s.at[0], send_s.at[0], recv_s.at[0], peer)
    second = remote(half_s, got_s.at[1], send_s.at[1], recv_s.at[1], beside)
    first.start()
    copy = spread_out(hidden_ref, send, recv, peer, section, per)

    def use(i, x, span, total):
        seq = x * 2 + section
        scale = as_column(rate_ref[pl.ds(seq * per + i % per, 1), :] * live_ref[pl.ds(seq * per + i % per, 1), :])
        gained = scale * total
        gain_out_ref[i] = gained.astype(BF)
        low = (rows_ref[seq, span].astype(F32) + gained).astype(BF)
        hidden_ref[seq, span] = low

        @pl.when(i > 0)
        def _():
            copy(i - 1, section).start()

        wide = low.astype(F32)
        normed_ref[seq, span] = (wide * rms(wide) * gain_ref[...]).astype(BF)

    def other(i, _):
        copy(i, section).wait_recv()
        seq = i // per * 2 + 1 - section
        span = pl.ds(pl.multiple_of(i % per * CHUNK, CHUNK), CHUNK)
        wide = hidden_ref[seq, span].astype(F32)
        normed_ref[seq, span] = (wide * rms(wide) * gain_ref[...]).astype(BF)
        return 0

    def drain(i, _):
        copy(i, section).wait_send()
        return 0

    stages = exchange(part_ref, got_a, held, got_x, send, recv, use)
    start()
    next(stages)
    next(stages)
    first.wait()
    half_s[...] = sums_ref[...] + got_s[0]
    next(stages)
    second.start()
    second.wait()
    rate_ref[...] = lax.rsqrt((half_s[...] + got_s[1]) / inner + EPSILON)
    work = [lambda d=d, h=h: relay_in(d, h) if h < PARTS else relay_out(d) for d in range(1, ns) for h in range(PARTS + 1)]
    for i in range(steps):
        for _ in range(2 if i == 0 else 1):
            work.pop(0)()
        next(stages)
    copy(steps - 1, section).start()
    lax.fori_loop(0, steps, other, 0)
    for step in work:
        step()
    finish()
    for _ in stages:
        pass
    lax.fori_loop(0, steps, drain, 0)


def back_kernel(part_ref, rows_ref, cot_ref, gained_ref, live_ref, gain_ref, ga_ref, gb_ref, out_ref, live_out_ref, dots_ref, all_a, all_b,
                got_a, held, got_x, dots_own, dots_got, send, recv, send_s, recv_s, *flow, ns, ny):
    section, xb, peer, beside = partners()
    per = part_ref.shape[1] // CHUNK
    steps = PAIR * per
    greet_line(ns, ny)
    grads = reduce_flow(1, ga_ref, gb_ref, (all_a, all_b), *flow, ns=ns, ny=ny)
    dots_own[...] = jnp.zeros_like(dots_own)
    copy = spread_out(out_ref, send, recv, peer, section, per)

    def live_of(seq, i):
        return as_column(live_ref[pl.ds(seq * per + i % per, 1), :])

    def use(i, x, span, total):
        seq = x * 2 + section
        rows = rows_ref[seq, span].astype(F32)
        inv = rms(rows)
        hat = rows * inv
        d_hat = total * gain_ref[...]
        d_rows = inv * (d_hat - hat * jnp.mean(d_hat * hat, axis=-1, keepdims=True))
        low = (cot_ref[seq, span].astype(F32) + d_rows).astype(BF)
        out_ref[seq, span] = low

        @pl.when(i > 0)
        def _():
            copy(i - 1, section).start()

        live = low.astype(F32) * live_of(seq, i)
        live_out_ref[seq, span] = live.astype(BF)
        dots_own[pl.ds(i, 1), :] = as_row(jnp.sum(live * gained_ref[i].astype(F32), axis=1, keepdims=True))

    def other(i, _):
        copy(i, section).wait_recv()
        seq = i // per * 2 + 1 - section
        span = pl.ds(pl.multiple_of(i % per * CHUNK, CHUNK), CHUNK)
        live_out_ref[seq, span] = (out_ref[seq, span].astype(F32) * live_of(seq, i)).astype(BF)
        return 0

    def drain(i, _):
        copy(i, section).wait_send()
        return 0

    stages = exchange(part_ref, got_a, held, got_x, send, recv, use)
    next(stages)
    next(grads)
    next(stages)
    next(stages)
    for i in range(steps):
        next(stages)
        if i < 3:
            next(grads)
    copy(steps - 1, section).start()
    dots = remote(dots_own, dots_got, send_s.at[0], recv_s.at[0], peer)
    lax.fori_loop(0, steps, other, 0)
    dots.start()
    for _ in stages:
        pass
    for _ in grads:
        pass
    lax.fori_loop(0, steps, drain, 0)
    dots.wait()
    for x in range(PAIR):
        for c in range(per):
            i = x * per + c
            dots_ref[pl.ds((x * 2 + section) * per + c, 1), :] = dots_own[i : i + 1, :]
            dots_ref[pl.ds((x * 2 + 1 - section) * per + c, 1), :] = dots_got[i : i + 1, :]


def exchange_scratch(part):
    steps = PAIR * part.shape[1] // CHUNK
    block = (steps, CHUNK, part.shape[2])
    return [pltpu.VMEM(block, BF)] * 3, [pltpu.SemaphoreType.DMA((3, steps)), pltpu.SemaphoreType.DMA((3, steps))]


def comm_params(collective_id):
    return pltpu.CompilerParams(collective_id=collective_id, has_side_effects=True, vmem_limit_bytes=60 << 20)


def run_onward(part, rows, sums, live, gain, q, o, inner, ns):
    wide, sems = exchange_scratch(part)
    steps = PAIR * part.shape[1] // CHUNK
    small = pltpu.VMEM(sums.shape, F32)
    ny = q.shape[1]
    outs, more = weights_shapes(q, o, ns)
    return pl.pallas_call(
        functools.partial(onward_kernel, inner=inner, ns=ns, ny=ny),
        in_specs=[VM] * 7,
        out_specs=[VM] * 4 + [pl.BlockSpec(memory_space=pl.ANY)] * 2,
        out_shape=[
            jax.ShapeDtypeStruct(part.shape, BF),
            jax.ShapeDtypeStruct(part.shape, BF),
            jax.ShapeDtypeStruct(sums.shape, F32),
            jax.ShapeDtypeStruct((steps, CHUNK, part.shape[2]), BF),
        ]
        + outs,
        scratch_shapes=wide + [pltpu.VMEM((2,) + sums.shape, F32), small] + sems + [pltpu.SemaphoreType.DMA((2,))] * 2 + more,
        compiler_params=comm_params(1),
        cost_estimate=pl.CostEstimate(flops=50_000_000, bytes_accessed=150_000_000, transcendentals=0),
        name="onward",
    )(part, rows, sums, live, gain, q, o)


def run_back(part, rows, cot, gained, live, gain, ga, gb):
    wide, sems = exchange_scratch(part)
    outs, flow = reduce_shapes(ga, gb)
    small = pltpu.VMEM((8, LANES), F32)
    return pl.pallas_call(
        functools.partial(back_kernel, ns=ga.shape[1], ny=ga.shape[0]),
        in_specs=[VM] * 8,
        out_specs=[VM] * 5,
        out_shape=[
            jax.ShapeDtypeStruct(part.shape, BF),
            jax.ShapeDtypeStruct(part.shape, BF),
            jax.ShapeDtypeStruct(live.shape, F32),
        ]
        + outs,
        scratch_shapes=wide + [small, small] + sems + [pltpu.SemaphoreType.DMA((2,))] * 2 + flow,
        compiler_params=comm_params(2),
        cost_estimate=pl.CostEstimate(flops=50_000_000, bytes_accessed=150_000_000, transcendentals=0),
        name="back",
    )(part, rows, cot, gained, live, gain, ga, gb)


PARTS = 2


def line_steps(n):
    return [step for i in range(n - 1) for step in ((1, n - 1 - i), (-1, i))]


def reduce_flow(b, ga_ref, gb_ref, boards, got_ya, acc_a, got_za, own_a, acc_b, got_zb, own_b, ya_s, ya_r, za_s, za_r, zb_s, zb_r, pc_s, pc_r, *, ns, ny):
    section, xb, peer, beside = partners()
    z = lax.axis_index("shard")
    yb = lax.axis_index("rep") // PAIR
    part = ga_ref.shape[2] // PARTS
    owns = (own_a, own_b)
    steps = line_steps(ns)
    order = []
    for _, target in steps:
        if target not in order:
            order.append(target)

    def y_peer(k):
        return {"rep": (yb + k) % ny * PAIR + xb}

    def y_from(k):
        return (yb + ny - k) % ny

    def rows_at(h):
        return pl.ds(h * part, part)

    def ya(k, target, h):
        return remote(ga_ref.at[(yb + k) % ny, target, rows_at(h)], got_ya.at[k - 1, target, rows_at(h)],
                      ya_s.at[k - 1, target, h], ya_r.at[k - 1, target, h], y_peer(k))

    def start():
        for h in range(PARTS):
            for target in order:
                @pl.when(target != z)
                def _():
                    for k in range(1, ny):
                        ya(k, target, h).start()
            for k in range(1, ny):
                ya(k, z, h).start()

    def piece(i, x, y, t, h, kind, device):
        rows = boards[i].shape[3] // PARTS
        place = boards[i].at[x, y, t, pl.ds(h * rows, rows)]
        return remote(place, place, pc_s.at[i, kind, x, y, t, h], pc_r.at[i, x, y, t, h], device)

    def offer(i, h):
        rows = boards[i].shape[3] // PARTS
        return remote(owns[i].at[pl.ds(h * rows, rows)], boards[i].at[xb, yb, 1 - b, pl.ds(h * rows, rows)],
                      pc_s.at[i, 0, xb, yb, 1 - b, h], pc_r.at[i, xb, yb, 1 - b, h], peer)

    def gather_chip(i, h):
        rows = boards[i].shape[3] // PARTS

        @pl.when(section == b)
        def _():
            boards[i][xb, yb, b, pl.ds(h * rows, rows)] = owns[i][pl.ds(h * rows, rows)]

        @pl.when(section != b)
        def _():
            offer(i, h).start()

    def gather_y(i, h):
        @pl.when(section == b)
        def _():
            piece(i, xb, yb, 1 - b, h, 0, peer).wait_recv()
            for k in range(1, ny):
                for t in range(2):
                    piece(i, xb, yb, t, h, k, y_peer(k)).start()
            for t in range(2):
                piece(i, xb, yb, t, h, ny, beside).start()

    def gather_x(i, h):
        @pl.when(section == b)
        def _():
            for k in range(1, ny):
                for t in range(2):
                    piece(i, xb, y_from(k), t, h, k, peer).wait_recv()
                    piece(i, xb, y_from(k), t, h, ny, beside).start()

    def gather_end(i, h):
        @pl.when(section == b)
        def _():
            for y in range(ny):
                for t in range(2):
                    piece(i, 1 - xb, y, t, h, ny, beside).wait_recv()
            for t in range(2):
                for k in range(1, ny):
                    piece(i, xb, yb, t, h, k, peer).wait_send()
                for y in range(ny):
                    piece(i, xb, y, t, h, ny, peer).wait_send()

        @pl.when(section != b)
        def _():
            offer(i, h).wait_send()

    def line(way, acc, got, target, place, span, send, recv):
        return remote(acc.at[target, span], got.at[place, span], send, recv, {"shard": z + way})

    def place_of(way, target):
        return jnp.where(target == z - 1, ns, target) if way < 0 else target

    def line_a(way, target, h):
        place = place_of(way, target)
        return line(way, acc_a, got_za, target, place, rows_at(h), za_s.at[target, h], za_r.at[place, h])

    def line_b(way, target):
        place = place_of(way, target)
        return line(way, acc_b, got_zb, target, place, pl.ds(0, gb_ref.shape[1]), zb_s.at[target], zb_r.at[place])

    def wait_a(place, h):
        remote(acc_a.at[0, rows_at(h)], got_za.at[place, rows_at(h)], za_s.at[0, h], za_r.at[place, h], peer).wait_recv()

    def wait_b(place):
        remote(acc_b.at[0], got_zb.at[place], zb_s.at[0], zb_r.at[place], peer).wait_recv()

    def base_a(target, h):
        total = ga_ref[yb, target, rows_at(h)].astype(F32)
        for k in range(1, ny):
            remote(ga_ref.at[0, target, rows_at(h)], got_ya.at[k - 1, target, rows_at(h)], ya_s.at[k - 1, target, h],
                   ya_r.at[k - 1, target, h], peer).wait_recv()
            total = total + got_ya[k - 1, target, rows_at(h)].astype(F32)
        return total

    def active(way, target):
        return target > z if way > 0 else target < z

    def far(way):
        return z > 0 if way > 0 else z < ns - 1

    def step_a(way, target, h):
        @pl.when(active(way, target))
        def _():
            total = base_a(target, h)

            @pl.when(jnp.logical_not(far(way)))
            def _():
                acc_a[target, rows_at(h)] = total.astype(BF)

            @pl.when(far(way))
            def _():
                wait_a(target, h)
                acc_a[target, rows_at(h)] = (total + got_za[target, rows_at(h)].astype(F32)).astype(BF)

            line_a(way, target, h).start()

    def step_b(way, target):
        @pl.when(active(way, target))
        def _():
            @pl.when(jnp.logical_not(far(way)))
            def _():
                acc_b[target] = gb_ref[target]

            @pl.when(far(way))
            def _():
                wait_b(target)
                acc_b[target] = (gb_ref[target].astype(F32) + got_zb[target].astype(F32)).astype(BF)

            line_b(way, target).start()

    def last(total, got, own, span, wait):
        @pl.when(z == 0)
        def _():
            wait(ns)
            own[span] = (total + got[ns, span].astype(F32)).astype(BF)

        @pl.when(z == ns - 1)
        def _():
            wait(z)
            own[span] = (total + got[z, span].astype(F32)).astype(BF)

        @pl.when((z > 0) & (z < ns - 1))
        def _():
            wait(z)
            wait(ns)
            own[span] = (total + got[z, span].astype(F32) + got[ns, span].astype(F32)).astype(BF)

    def last_a(h):
        last(base_a(z, h), got_za, own_a, rows_at(h), lambda place: wait_a(place, h))

    def last_b():
        last(gb_ref[z].astype(F32), got_zb, own_b, pl.ds(0, gb_ref.shape[1]), wait_b)

    def finish():
        for i in (1, 0):
            for h in range(PARTS):
                gather_end(i, h)
        for h in range(PARTS):
            for target in range(ns):
                for k in range(1, ny):
                    ya(k, target, h).wait_send()
        for way, target in steps:
            @pl.when(active(way, target))
            def _():
                line_b(way, target).wait_send()
                for h in range(PARTS):
                    line_a(way, target, h).wait_send()

    def stages():
        start()
        yield
        for way, target in steps[:2]:
            step_b(way, target)
            step_a(way, target, 0)
        yield
        for way, target in steps[2:4]:
            step_b(way, target)
            step_a(way, target, 0)
        yield
        for way, target in steps[4:]:
            step_b(way, target)
            step_a(way, target, 0)
        yield
        last_b()
        for h in range(PARTS):
            gather_chip(1, h)
        last_a(0)
        gather_chip(0, 0)
        yield
        for h in range(PARTS):
            gather_y(1, h)
        for way, target in steps[:2]:
            step_a(way, target, 1)
        gather_y(0, 0)
        for h in range(PARTS):
            gather_x(1, h)
        yield
        for way, target in steps[2:4]:
            step_a(way, target, 1)
        gather_x(0, 0)
        yield
        for way, target in steps[4:]:
            step_a(way, target, 1)
        last_a(1)
        gather_chip(0, 1)
        yield
        gather_y(0, 1)
        yield
        gather_x(0, 1)
        finish()

    return stages()


def reduce_shapes(ga, gb):
    ny, ns, ra, ca = ga.shape
    rb, cb = gb.shape[1:]
    dma = pltpu.SemaphoreType.DMA
    outs = [jax.ShapeDtypeStruct((PAIR, ny, 2, ra, ca), BF), jax.ShapeDtypeStruct((PAIR, ny, 2, rb, cb), BF)]
    scratch = [
        pltpu.VMEM((ny - 1, ns, ra, ca), BF),
        pltpu.VMEM((ns, ra, ca), BF),
        pltpu.VMEM((ns + 1, ra, ca), BF),
        pltpu.VMEM((ra, ca), BF),
        pltpu.VMEM((ns, rb, cb), BF),
        pltpu.VMEM((ns + 1, rb, cb), BF),
        pltpu.VMEM((rb, cb), BF),
        dma((ny - 1, ns, PARTS)), dma((ny - 1, ns, PARTS)),
        dma((ns, PARTS)), dma((ns + 1, PARTS)),
        dma((ns,)), dma((ns + 1,)),
        dma((2, ny + 1, PAIR, ny, 2, PARTS)), dma((2, PAIR, ny, 2, PARTS)),
    ]
    return outs, scratch


def tail_kernel(ga_ref, gb_ref, vec_ref, p0_ref, p1_ref, rows_ref, cot_ref, hidden_ref, scale_ref, gain_ref,
                all_a, all_b, vec_out, res_ref, *refs, ns, ny):
    flow, (got_p, held, got_x, give, vec_y, vec_h, vec_z, vec_t, ra_s, ra_r, v_s, v_r) = refs[:15], refs[15:]
    section, xb, peer, beside = partners()
    z = lax.axis_index("shard")
    yb = lax.axis_index("rep") // PAIR

    def y_peer(k):
        return {"rep": (yb + k) % ny * PAIR + xb}

    def z_peer(k):
        return {"shard": (z + k) % ns}

    greet(peer, beside, *(y_peer(k) for k in range(1, ny)), *(z_peer(k) for k in range(1, ns)))

    def over_y(k):
        return remote(vec_ref, vec_y.at[k - 1], v_s.at[k], v_r.at[k], y_peer(k))

    def over_z(k):
        return remote(vec_h, vec_z.at[k - 1], v_s.at[ny + k], v_r.at[ny + k], z_peer(k))

    to_chip = remote(vec_t.at[1 - section], vec_out.at[section, xb], v_s.at[0], v_r.at[0], peer)

    def to_side(t):
        return remote(vec_out.at[t, xb], vec_out.at[t, xb], v_s.at[ny + ns + t], v_r.at[ny + ns + t], beside)

    for k in range(1, ny):
        over_y(k).start()

    per = p0_ref.shape[1] // CHUNK
    flows = (p0_ref, p1_ref)

    def p_peer(f, x, c):
        span = pl.ds(c * CHUNK, CHUNK)
        return remote(flows[f].at[x * 2 + 1 - section, span], got_p.at[f, x, c], ra_s.at[0, f, x, c], ra_r.at[0, f, x, c], peer)

    def p_beside(f, c):
        return remote(held.at[f, 1 - xb, c], got_x.at[f, c], ra_s.at[1, f, 0, c], ra_r.at[1, f, 0, c], beside)

    def p_give(c):
        return remote(give.at[c], res_ref.at[section, pl.ds(c * CHUNK, CHUNK)], ra_s.at[1, 0, 1, c], ra_r.at[1, 0, 1, c], peer)

    def p_got(c):
        return remote(give.at[c], res_ref.at[1 - section, pl.ds(c * CHUNK, CHUNK)], ra_s.at[1, 0, 1, c], ra_r.at[1, 0, 1, c], peer)

    grads = reduce_flow(0, ga_ref, gb_ref, (all_a, all_b), *flow, ns=ns, ny=ny)
    next(grads)
    for f in range(2):
        for c in range(per):
            for x in range(PAIR):
                p_peer(f, x, c).start()
    for f in range(2):
        for c in range(per):
            for x in range(PAIR):
                p_peer(f, x, c).wait_recv()
                held[f, x, c] = (flows[f][x * 2 + section, pl.ds(c * CHUNK, CHUNK)].astype(F32) + got_p[f, x, c].astype(F32)).astype(BF)
            p_beside(f, c).start()
    total = vec_ref[...]
    for k in range(1, ny):
        over_y(k).wait()
        total = total + vec_y[k - 1]
    vec_h[...] = total
    for k in range(1, ns):
        over_z(k).start()
    next(grads)

    def finish(f, c):
        span = pl.ds(c * CHUNK, CHUNK)
        p_beside(f, c).wait_recv()
        total = held[f, xb, c].astype(F32) + got_x[f, c].astype(F32)
        seq = xb * 2 + section
        if f == 0:
            rows = rows_ref[seq, span].astype(F32)
            inv = rms(rows)
            hat = rows * inv
            d_hat = total * gain_ref[...]
            d_rows = inv * (d_hat - hat * jnp.mean(d_hat * hat, axis=-1, keepdims=True))
            low = (cot_ref[seq, span].astype(F32) + d_rows).astype(BF)
        else:
            scale = as_column(scale_ref[pl.ds(seq * per + c, 1), :])
            low = (hidden_ref[seq, span].astype(F32) + scale * total).astype(BF)

        @pl.when(section == f)
        def _():
            res_ref[section, span] = low

        @pl.when(section != f)
        def _():
            give[c] = low

    next(grads)
    total = vec_h[...]
    for k in range(1, ns):
        over_z(k).wait()
        total = total + vec_z[k - 1]
    vec_t[...] = total
    to_chip.start()
    vec_out[section, xb] = vec_t[section]
    for c in range(per):
        for f in range(2):
            finish(f, c)
    next(grads)
    for c in range(per):
        p_give(c).start()
    to_chip.wait_send()
    remote(vec_t.at[0], vec_out.at[1 - section, xb], v_s.at[0], v_r.at[0], peer).wait_recv()
    for t in range(2):
        to_side(t).start()
    next(grads)
    for t in range(2):
        to_side(t).wait_send()
        remote(vec_out.at[t, xb], vec_out.at[t, 1 - xb], v_s.at[ny + ns + t], v_r.at[ny + ns + t], beside).wait_recv()
    for _ in grads:
        pass
    for f in range(2):
        for c in range(per):
            for x in range(PAIR):
                p_peer(f, x, c).wait_send()
            p_beside(f, c).wait_send()
    for c in range(per):
        p_give(c).wait_send()
        p_got(c).wait_recv()


def run_tail(ga, gb, vec, p0, p1, rows, cot, hidden, scale, gain):
    ny, ns = ga.shape[:2]
    seq_len, width = p0.shape[1:]
    per = seq_len // CHUNK
    block = (CHUNK, width)
    dma = pltpu.SemaphoreType.DMA
    outs, scratch = reduce_shapes(ga, gb)
    return pl.pallas_call(
        functools.partial(tail_kernel, ns=ns, ny=ny),
        in_specs=[VM] * 10,
        out_specs=[VM] * 4,
        out_shape=outs + [jax.ShapeDtypeStruct((2, PAIR) + vec.shape[1:], F32), jax.ShapeDtypeStruct((2, seq_len, width), BF)],
        scratch_shapes=scratch
        + [
            pltpu.VMEM((2, PAIR, per) + block, BF),
            pltpu.VMEM((2, PAIR, per) + block, BF),
            pltpu.VMEM((2, per) + block, BF),
            pltpu.VMEM((per,) + block, BF),
            pltpu.VMEM((ny - 1,) + vec.shape, F32),
            pltpu.VMEM(vec.shape, F32),
            pltpu.VMEM((ns - 1,) + vec.shape, F32),
            pltpu.VMEM(vec.shape, F32),
            dma((2, 2, PAIR, per)), dma((2, 2, PAIR, per)),
            dma((ny + ns + 2,)), dma((ny + ns + 2,)),
        ],
        compiler_params=comm_params(4),
        cost_estimate=pl.CostEstimate(flops=50_000_000, bytes_accessed=300_000_000, transcendentals=0),
        name="tail",
    )(ga, gb, vec, p0, p1, rows, cot, hidden, scale, gain)


def place_kernel(s_ref, a0_ref, b0_ref, a1_ref, b1_ref, in_ref, out_ref, dt_ref, *, places, dts, ny):
    def copy(a_ref, b_ref):
        for col, size, index, off in places:
            in_ref[:, col : col + size] = a_ref[index + (slice(None), slice(off, off + size))].astype(F32)
        for col, size, index, off in dts:
            dt_ref[:, col : col + size] = a_ref[index + (slice(None), slice(off, off + size))].astype(F32)
        part = b_ref.shape[-1]
        for q in range(PAIR):
            for t in range(2):
                for y in range(ny):
                    col = (t * ny + y) * part
                    out_ref[q, :, col : col + part] = b_ref[q, y, t].astype(F32)

    @pl.when(s_ref[0] == 0)
    def _():
        copy(a0_ref, b0_ref)

    @pl.when(s_ref[0] != 0)
    def _():
        copy(a1_ref, b1_ref)


def run_place(section, of0, of1, places, dts, columns, heads, block):
    ny = of0[0].shape[1]
    rows = of0[0].shape[3]
    lead = (PAIR, ny, 2)
    spec = lambda v: pl.BlockSpec(lead + (block, v.shape[4]), lambda i, s: (0, 0, 0, i, 0))
    width = 2 * ny * of0[1].shape[4]
    return pl.pallas_call(
        functools.partial(place_kernel, places=places, dts=dts, ny=ny),
        grid_spec=pltpu.PrefetchScalarGridSpec(
            num_scalar_prefetch=1,
            grid=(rows // block,),
            in_specs=[spec(v) for v in (*of0, *of1)],
            out_specs=[
                pl.BlockSpec((block, columns), lambda i, s: (i, 0)),
                pl.BlockSpec((PAIR, block, width), lambda i, s: (0, i, 0)),
                pl.BlockSpec((block, heads), lambda i, s: (i, 0)),
            ],
        ),
        out_shape=[
            jax.ShapeDtypeStruct((rows, columns), F32),
            jax.ShapeDtypeStruct((PAIR, rows, width), F32),
            jax.ShapeDtypeStruct((rows, heads), F32),
        ],
        compiler_params=PARAMS,
        cost_estimate=pl.CostEstimate(flops=1_000_000, bytes_accessed=30_000_000, transcendentals=0),
        name="place",
    )(section, *of0, *of1)


def smalls_kernel(z_ref, v_ref, conv_ref, heads_ref, pre_ref, out_ref, full, *, taps, ns, mine_w, states2, heads, width):
    half = ns // 2
    cw = mine_w // half
    unit = heads // ns // PAIR
    gx, gbc, gh = 0, mine_w, mine_w + states2
    spread = head_map(mine_w, 2 * mine_w * PAIR // heads)
    shared = v_ref[0, 0] + v_ref[0, 1] + v_ref[1, 0] + v_ref[1, 1]
    full[:, 2 * PAIR * mine_w :] = shared[:8, gbc : gbc + states2]
    for t in range(2):
        for q in range(PAIR):
            for k in range(half):
                col = ((t * half + k) * PAIR + q) * cw
                full[:, col : col + cw] = v_ref[t, q, :8, k * cw : (k + 1) * cw]
    channels = (2 * PAIR * mine_w + states2) // ns
    inner = 2 * PAIR * mine_w // ns
    part = width // ns
    wide = v_ref.shape[3]
    skips = []
    for t in range(2):
        skips.append([])
        for q in range(PAIR):
            row = v_ref[t, q, taps + 1 : taps + 2, :mine_w]
            high = row.astype(BF)
            rest = row - high.astype(F32)
            mid = rest.astype(BF)
            rows8 = lambda v: jnp.broadcast_to(v, (8, mine_w))
            skips[t].append((mm_t(rows8(high), spread) + mm_t(rows8(mid), spread) + mm_t(rows8(rest - mid.astype(F32)), spread))[0:1])
    heads_ref[...] = jnp.zeros_like(heads_ref)
    for at in range(ns):
        @pl.when(z_ref[0] == at)
        def _():
            conv_ref[...] = full[:, at * channels : (at + 1) * channels]
            out_ref[...] = full[taps + 2 : taps + 3, at * inner : (at + 1) * inner]
            t, k = at // half, at % half
            for q in range(PAIR):
                span = slice(gh + k * unit, gh + (k + 1) * unit)
                put = slice(q * unit, (q + 1) * unit)
                heads_ref[0:1, put] = v_ref[t, q, 0:1, span]
                heads_ref[1:2, put] = v_ref[t, q, 1:2, span]
                heads_ref[2:3, put] = skips[t][q][:, k * unit : (k + 1) * unit]
            for row in range(-(-width // wide)):
                low, high = max(at * part, row * wide), min((at + 1) * part, (row + 1) * wide)
                if low < high:
                    pre_ref[:, low - at * part : high - at * part] = shared[8 + row : 9 + row, low - row * wide : high - row * wide]


def run_smalls(z, v, taps, ns, mine_w, states2, heads, width):
    channels = (2 * PAIR * mine_w + states2) // ns
    whole = lambda *dims: pl.BlockSpec(dims, lambda i, z: (0,) * len(dims))
    return pl.pallas_call(
        functools.partial(smalls_kernel, taps=taps, ns=ns, mine_w=mine_w, states2=states2, heads=heads, width=width),
        grid_spec=pltpu.PrefetchScalarGridSpec(
            num_scalar_prefetch=1,
            grid=(1,),
            in_specs=[whole(*v.shape)],
            out_specs=[whole(8, channels), whole(8, LANES), whole(1, width // ns), whole(1, 2 * PAIR * mine_w // ns)],
            scratch_shapes=[pltpu.VMEM((8, channels * ns), F32)],
        ),
        out_shape=[
            jax.ShapeDtypeStruct((8, channels), F32),
            jax.ShapeDtypeStruct((8, LANES), F32),
            jax.ShapeDtypeStruct((1, width // ns), F32),
            jax.ShapeDtypeStruct((1, 2 * PAIR * mine_w // ns), F32),
        ],
        compiler_params=PARAMS,
        cost_estimate=pl.CostEstimate(flops=1_000_000, bytes_accessed=1_000_000, transcendentals=0),
        name="smalls",
    )(z, v)


def dot(a, b):
    return jnp.dot(a, b, preferred_element_type=F32)


def pick(index, options):
    result = options[-1]
    for place in reversed(range(len(options) - 1)):
        result = jnp.where(index == place, options[place], result)
    return result


def ordered(index, own, other, axis):
    return jnp.stack([pick(index, (own, other)), pick(index, (other, own))], axis=axis)


def joined(index, own, other, axis):
    return jnp.concatenate([pick(index, (own, other)), pick(index, (other, own))], axis=axis)


def on_device(boundary, lengths, in_proj, dt_proj, out_proj, conv_weight, conv_bias, dt_bias, a_log, d_skip, pre_gain, out_gain):
    ns = lax.axis_size("shard")
    nr = lax.axis_size("rep")
    ny = nr // PAIR
    s = lax.axis_index("section")
    z = lax.axis_index("shard")
    rep = lax.axis_index("rep")
    xb = rep % PAIR
    yb = rep // PAIR

    def swap(v):
        return lax.ppermute(v, "section", [(0, 1), (1, 0)])

    def x_swap(v):
        return lax.ppermute(v, "rep", [(i, i ^ 1) for i in range(nr)])

    def y_send(v, k):
        return lax.ppermute(v, "rep", [(i, (i // PAIR + k) % ny * PAIR + i % PAIR) for i in range(nr)])

    micro, seq_len, width = boundary.shape[1], boundary.shape[3], boundary.shape[4]
    inner = out_proj.shape[1] * ns
    heads = dt_bias.shape[1] * ns
    taps, channels = conv_weight.shape[1], conv_weight.shape[2] * ns
    states2 = channels - inner
    cw = inner // ns // PAIR
    half = ns // 2
    mine_w = half * cw
    mine_h = heads // (2 * PAIR)
    part_w = 2 * mine_w // ny

    def column_chunks(v, first):
        out = []
        for t in range(2):
            for shard in range(t * half, (t + 1) * half):
                start = first + shard * PAIR * cw
                out.append(pick(xb, tuple(v[:, start + q * cw : start + (q + 1) * cw] for q in range(PAIR))))
        return [jnp.concatenate(out[:half], axis=1), jnp.concatenate(out[half:], axis=1)]

    own_in = in_proj[0]
    q_own = []
    for a, b in zip(column_chunks(own_in, 0), column_chunks(own_in, inner)):
        if ny == 2:
            q_own += [a, b]
        else:
            q_own += [v[:, k * part_w : (k + 1) * part_w] for v in (a, b) for k in range(ny // 2)]
    q_own = jnp.stack(q_own).reshape(2, ny, width // ns, part_w)
    own_out = out_proj[0]
    o_own = pick(xb, (own_out[:cw], own_out[cw : 2 * cw])).reshape(ny, cw // ny, width)

    flat = lambda v: v.reshape(-1, v.shape[-1])
    smalls_own = tuple(flat(v) for v in (conv_weight, conv_bias, dt_bias, a_log, d_skip, pre_gain, out_gain))
    counts = jnp.broadcast_to(lengths.astype(F32), (micro, LANES))
    tokens, normed0, g_out1, live8, px, pbc, ph, gains, w_bcdt, in0, out0 = run_start(
        boundary[0, :, 0], counts, smalls_own, own_in[:, 2 * inner :], dt_proj[0], q_own, o_own, heads
    )
    smalls = [(px[b], pbc[b], ph[b]) for b in range(2)]
    unit_h = heads // ns // PAIR
    w_in, w_out = [in0.reshape(ny, width, part_w)], [out0.reshape(mine_w, width)]
    seqs = PAIR * micro

    def by_seq(v):
        return v.reshape((seqs, seq_len) + v.shape[1:])

    def of_own(v):
        return pick(xb, (v[0], v[1]))

    chunks = seq_len // CHUNK

    def forward(b, normed, dmix):
        normed = normed.reshape(seqs * seq_len, width)
        proj = [dot(normed, w_in[b][j]).astype(BF) for j in range(ny)]
        if ny > 2:
            proj = [jnp.concatenate(proj[: ny // 2], axis=1), jnp.concatenate(proj[ny // 2 :], axis=1)]
        gate, x = by_seq(proj[0]), by_seq(proj[1])
        bcdt = by_seq(dot(normed, w_bcdt[b]))
        gg, y, state, *sums = run_forward(smalls[b], gate, x, bcdt, dmix, taps, mine_h)
        gg = gg.reshape(seqs * seq_len, mine_w)
        part = by_seq(dot(gg, w_out[b]).astype(BF))
        return part, sums, (normed, gate, x, bcdt, gg, y, state)

    def mixed_back(b, g_out):
        dmix = lax.dot_general(g_out, w_out[b], (((1,), (1,)), ((), ())), preferred_element_type=F32)
        return by_seq(dmix.astype(BF))

    rows = tokens[0].reshape(seqs, seq_len, width)
    cot = tokens[1].reshape(seqs, seq_len, width)
    part0, sums, stored0 = forward(0, normed0, None)
    hidden, normed, r0, gained0, in1, out1 = run_onward(
        part0, rows, sums[0].reshape(seqs * chunks, LANES), live8, gains[1], q_own, o_own, float(inner), ns
    )
    w_in.append(in1.reshape(ny, width, part_w))
    w_out.append(out1.reshape(mine_w, width))
    g_out1 = g_out1.reshape(seqs * seq_len, width)
    dmix1 = mixed_back(1, g_out1)
    part1, sums, stored1 = forward(1, normed, dmix1)
    both_sums = run_sums(jnp.concatenate([v.reshape(seqs * chunks, LANES) for v in sums]), 3)
    r1 = lax.rsqrt(both_sums[: seqs * chunks] / inner + EPSILON)

    def backward(b, dmix, stored, r, coef):
        normed, gate, x, bcdt, gg, y, state = stored
        scalars = jnp.concatenate([r.reshape(seqs, chunks, LANES), coef.reshape(seqs, chunks, LANES)], axis=1)
        dgate, dx, dbcdt, gsmall = run_backward(smalls[b], gate, x, bcdt, y, state, dmix, scalars, taps, mine_h)
        flat = lambda v: v.reshape(seqs * seq_len, v.shape[-1])
        dgate, dx, dbcdt = flat(dgate), flat(dx), flat(dbcdt)
        if ny == 2:
            dparts = [dgate, dx]
        else:
            dparts = [v[:, k * part_w : (k + 1) * part_w] for v in (dgate, dx) for k in range(ny // 2)]
        against = lambda a, w: lax.dot_general(a, w, (((1,), (1,)), ((), ())), preferred_element_type=F32)
        d_normed = against(dbcdt, w_bcdt[b])
        for j in range(ny):
            d_normed = d_normed + against(dparts[j], w_in[b][j])
        gpre = jnp.sum(d_normed * normed.astype(F32), axis=0) / gains[b, 0]
        across = lambda a, c: lax.dot_general(a, c, (((0,), (0,)), ((), ())), preferred_element_type=F32)

        dbc = dbcdt[:, :states2]
        cols = [dbc[:, : states2 // 2], dbc[:, states2 // 2 :]]
        total = (pick(s, cols).astype(F32) + swap(pick(s, cols[::-1])).astype(F32)).astype(BF)
        cols = [total[:, : states2 // 4], total[:, states2 // 4 :]]
        total = (pick(xb, cols).astype(F32) + x_swap(pick(xb, cols[::-1])).astype(F32)).astype(BF)
        mine = jnp.concatenate([total, dbcdt[:, states2 : states2 + states2 // 4]], axis=1)
        grad_in = [across(normed, jnp.concatenate([v, mine], axis=1)).astype(BF) for v in dparts]
        grad_in = jnp.stack(grad_in).reshape(ny, ns, width // ns, -1)
        wide = gsmall.shape[1]
        gpre = jnp.pad(gpre, (0, 8 * wide - width)).reshape(8, wide)
        return by_seq(d_normed.astype(BF)), grad_in, jnp.concatenate([gsmall, gpre])

    def out_chip(b, g_out, gg, r):
        g_scaled = (g_out.astype(F32) * r.reshape(-1, 1)).astype(BF)
        across = lambda a, c: lax.dot_general(a, c, (((0,), (0,)), ((), ())), preferred_element_type=F32)
        grad = across(gg, g_scaled).astype(BF)
        cols = [grad[:, : width // 2], grad[:, width // 2 :]]
        return joined(s, pick(s, cols), swap(pick(s, cols[::-1])), 0)

    def out_grad(v):
        step = width // 2 // ny
        parts = [v[:, j * step : (j + 1) * step] for j in range(ny)]
        total = pick(yb, parts).astype(F32)
        for k in range(1, ny):
            total = total + y_send(pick((yb + k) % ny, parts), k).astype(F32)
        return total.astype(BF).reshape(ns, cw, -1)

    v1 = out_chip(1, g_out1, stored1[4], r1)
    dmix1, v1 = lax.optimization_barrier((dmix1, v1))
    gout1 = out_grad(v1)
    d_normed1, gin1, gsmall1 = backward(1, dmix1, stored1, r1, r1 * r1 * r1 * both_sums[seqs * chunks :] / inner)
    cot0, g_out0, dots0, *of1 = run_back(d_normed1, hidden, cot, gained0, live8, gains[1], gin1, gout1)

    g_out0 = g_out0.reshape(-1, width)
    dmix0 = mixed_back(0, g_out0)
    v0 = out_chip(0, g_out0, stored0[4], r0)
    dmix0, v0 = lax.optimization_barrier((dmix0, v0))
    gout0 = out_grad(v0)
    d_normed0, gin0, gsmall0 = backward(0, dmix0, stored0, r0, r0 * r0 * dots0 / inner)
    *of0, vec, res = run_tail(
        gin0, gout0, jnp.stack([gsmall0, gsmall1]), d_normed0, part1, rows, cot0, hidden, live8 * r1, gains[0]
    )
    activations = pick(s, (of_own(hidden.reshape(PAIR, micro, seq_len, width)), res))
    input_grads = pick(s, (res, of_own(cot0.reshape(PAIR, micro, seq_len, width))))
    places, dts = [], []
    col = 0
    for plane in range(2):
        for t in range(2):
            for k in range(half):
                for q in range(PAIR):
                    y_at, off = divmod(plane * mine_w + k * cw, part_w)
                    places.append((col, cw, (q, y_at, t), off))
                    col += cw
    quad = states2 // 4
    for t in range(2):
        for q in range(PAIR):
            places.append((col, quad, (q, 0, t), part_w))
            col += quad
    for t in range(2):
        for k in range(half):
            for q in range(PAIR):
                dts.append((((t * half + k) * PAIR + q) * unit_h, unit_h, (q, 0, t), part_w + quad + k * unit_h))
    grad_in, grad_out, grad_dt = run_place(s[None], of0, of1, tuple(places), tuple(dts), col, heads, 64)
    grad_out = grad_out.reshape(PAIR * cw, width)
    g_conv, g_heads, g_pre, g_og = run_smalls(z[None], vec, taps, ns, mine_w, states2, heads, width)
    g_cw, g_cb = g_conv[:taps], g_conv[taps]
    g_dtb, g_alg, g_dsk = (g_heads[i, : heads // ns] for i in range(3))
    g_pre, g_og = g_pre[0], g_og[0]

    return (
        activations[None, :, None],
        input_grads[None, :, None],
        grad_in[None],
        grad_dt[None],
        grad_out[None],
        g_cw[None],
        g_cb[None],
        g_dtb[None],
        g_alg[None],
        g_dsk[None],
        g_pre[None],
        g_og[None],
    )


def solution(mesh):
    shard1 = P("section", "shard")
    shard2 = P("section", "shard", None)
    tokens = P("section", None, ("shard", "rep"), None, None)
    taps = P("section", None, "shard")
    weights = (shard2, shard2, shard2, taps, shard1, shard1, shard1, shard1, shard1, shard1)
    return jax.shard_map(
        on_device,
        mesh=mesh,
        in_specs=(tokens, P(None, ("shard", "rep"))) + weights,
        out_specs=(tokens, tokens) + weights,
        check_vma=False,
    )
```

```python
import functools

import jax
import jax.numpy as jnp
from jax import lax
from jax.experimental import pallas as pl
from jax.experimental.pallas import tpu as pltpu
from jax.sharding import PartitionSpec as P


BF = jnp.bfloat16
F32 = jnp.float32
HIGH = lax.Precision.HIGHEST
EPSILON = 1e-05
CHUNK = 128
LANES = 128
PAIR = 2


def mm(a, b):
    return jnp.dot(a.astype(BF), b.astype(BF), preferred_element_type=F32)


def mm_t(a, b):
    return lax.dot_general(a.astype(BF), b.astype(BF), (((1,), (1,)), ((), ())), preferred_element_type=F32)


def t_mm(a, b):
    return lax.dot_general(a.astype(BF), b.astype(BF), (((0,), (0,)), ((), ())), preferred_element_type=F32)


def rows_of(shape):
    return lax.broadcasted_iota(jnp.int32, shape, 0)


def lanes_of(shape):
    return lax.broadcasted_iota(jnp.int32, shape, 1)


def shift_down(v, steps):
    return jnp.where(rows_of(v.shape) >= steps, pltpu.roll(v, steps, 0), 0.0)


def shift_up(v, steps):
    size = v.shape[0]
    return jnp.where(rows_of(v.shape) < size - steps, pltpu.roll(v, size - steps, 0), 0.0)


def conv(v, taps_ref, taps):
    total = taps_ref[taps : taps + 1, :] + taps_ref[taps - 1 : taps, :] * v
    for k in range(taps - 1):
        total = total + taps_ref[k : k + 1, :] * shift_down(v, taps - 1 - k)
    return total


def conv_back(d_sum, v, taps_ref, taps):
    d_v = taps_ref[taps - 1 : taps, :] * d_sum
    d_taps = []
    for k in range(taps - 1):
        d_v = d_v + taps_ref[k : k + 1, :] * shift_up(d_sum, taps - 1 - k)
        d_taps.append(jnp.sum(d_sum * shift_down(v, taps - 1 - k), axis=0, keepdims=True))
    d_taps.append(jnp.sum(d_sum * v, axis=0, keepdims=True))
    d_taps.append(jnp.sum(d_sum, axis=0, keepdims=True))
    return d_v, d_taps


def head_map(width, head_dim):
    shape = (LANES, width)
    return (rows_of(shape) == lanes_of(shape) // head_dim).astype(BF)


def expand(v, spread):
    high = v.astype(BF)
    low = (v - high.astype(F32)).astype(BF)
    return mm(high, spread) + mm(low, spread)


def step_of(dt, ph_ref):
    pre = dt + ph_ref[0:1, :]
    step = jnp.maximum(pre, 0.0) + jnp.log1p(jnp.exp(-jnp.abs(pre)))
    rate = -jnp.exp(ph_ref[1:2, :])
    return pre, step, rate


def lower_mask():
    shape = (CHUNK, CHUNK)
    return rows_of(shape) >= lanes_of(shape)


def pair_rows(v, first):
    return jnp.concatenate([jnp.where(first, v, 0.0), jnp.where(first, 0.0, v)], axis=0)


def as_row(column):
    return jnp.broadcast_to(column, (CHUNK, LANES)).T[0:1, :]


def as_column(row):
    return jnp.broadcast_to(row, (CHUNK, LANES)).T[:, 0:1]


def forward_kernel(px_ref, pbc_ref, ph_ref, gate_ref, x_ref, bcdt_ref, *refs, taps, heads, with_dots):
    if with_dots:
        dmix_ref, gg_ref, y_ref, st_ref, ss_ref, dot_ref = refs
    else:
        gg_ref, y_ref, st_ref, ss_ref = refs
    width = x_ref.shape[1]
    head_dim = width // heads
    states = pbc_ref.shape[1] // 2
    spread = head_map(width, head_dim)
    bcdt = bcdt_ref[...].astype(F32)
    sums = conv(bcdt[:, : 2 * states], pbc_ref, taps)
    bc = sums * jax.nn.sigmoid(sums)
    _, step, rate = step_of(bcdt[:, 2 * states :], ph_ref)
    decay = rate * step
    sums = conv(x_ref[...].astype(F32), px_ref, taps)
    act = sums * jax.nn.sigmoid(sums)
    xs = act * expand(step, spread)
    lower = lower_mask()
    tri = lower.astype(F32)
    first = lanes_of((CHUNK, 2 * head_dim)) < head_dim
    state = None
    chunks = x_ref.shape[0] // CHUNK
    for c in range(chunks):
        span = slice(c * CHUNK, (c + 1) * CHUNK)
        cum = jnp.dot(tri, decay[span], precision=HIGH, preferred_element_type=F32)
        cum_t = cum.T
        b_c = bc[span, :states].astype(BF)
        c_c = bc[span, states:].astype(BF)
        scores = mm_t(c_c, b_c)
        xs_c = xs[span]
        pieces = []
        for p in range(heads // 2):
            two = slice(p * 2 * head_dim, (p + 1) * 2 * head_dim)
            mixes = []
            for h in (2 * p, 2 * p + 1):
                gap = jnp.minimum(cum[:, h : h + 1] - cum_t[h : h + 1, :], 0.0)
                mixes.append(jnp.where(lower, jnp.exp(gap) * scores, 0.0).astype(BF))
            pieces.append(mm(jnp.concatenate(mixes, axis=1), pair_rows(xs_c[:, two], first)))
        y = jnp.concatenate(pieces, axis=1)
        if c > 0:
            y = y + mm(c_c, state) * expand(jnp.exp(cum), spread)
        if c + 1 < chunks:
            last = cum[CHUNK - 1 : CHUNK, :]
            fresh = t_mm(b_c, xs_c * expand(jnp.exp(last - cum), spread))
            state = fresh if c == 0 else fresh + state * expand(jnp.exp(jnp.broadcast_to(last, (states, LANES))), spread)
            st_ref[c] = state
        y = y + px_ref[taps + 1 : taps + 2, :] * act[span]
        y_low = y.astype(BF)
        y_ref[span, :] = y_low
        y = y_low.astype(F32)
        gate = gate_ref[span, :].astype(F32)
        gated = y * (gate * jax.nn.sigmoid(gate))
        ss_ref[c : c + 1, :] = as_row(jnp.sum(gated * gated, axis=1, keepdims=True))
        gg = gated * px_ref[taps + 2 : taps + 3, :]
        gg_ref[span, :] = gg.astype(BF)
        if with_dots:
            dot_ref[c : c + 1, :] = as_row(jnp.sum(gg * dmix_ref[span, :].astype(F32), axis=1, keepdims=True))


def backward_kernel(
    px_ref, pbc_ref, ph_ref, gate_ref, x_ref, bcdt_ref, y_ref, st_ref, dmix_ref, sc_ref,
    dgate_ref, dx_ref, dbcdt_ref, small_ref, *, taps, heads,
):
    length, width = x_ref.shape
    head_dim = width // heads
    states = pbc_ref.shape[1] // 2
    spread = head_map(width, head_dim)

    @pl.when(pl.program_id(0) == 0)
    def _():
        small_ref[...] = jnp.zeros_like(small_ref)

    gx_ref = small_ref.at[:, :width]
    gbc_ref = small_ref.at[:, width : width + 2 * states]
    gh_ref = small_ref.at[:, width + 2 * states :]

    gate = gate_ref[...].astype(F32)
    y = y_ref[...].astype(F32)
    dmix = dmix_ref[...].astype(F32)
    chunks = length // CHUNK
    r = jnp.concatenate([as_column(sc_ref[c : c + 1, :]) for c in range(chunks)], axis=0)
    coef = jnp.concatenate([as_column(sc_ref[chunks + c : chunks + c + 1, :]) for c in range(chunks)], axis=0)
    sig = jax.nn.sigmoid(gate)
    gated = y * gate * sig
    gx_ref[taps + 2 : taps + 3, :] += jnp.sum(dmix * gated * r, axis=0, keepdims=True)
    dgated = r * px_ref[taps + 2 : taps + 3, :] * dmix - coef * gated
    dgate_ref[...] = (dgated * y * (sig * (1.0 + gate * (1.0 - sig)))).astype(BF)
    dy = dgated * gate * sig

    bcdt = bcdt_ref[...].astype(F32)
    bc_in = bcdt[:, : 2 * states]
    bc_sum = conv(bc_in, pbc_ref, taps)
    bc_sig = jax.nn.sigmoid(bc_sum)
    bc = bc_sum * bc_sig
    pre, step, rate = step_of(bcdt[:, 2 * states :], ph_ref)
    decay = rate * step
    x_in = x_ref[...].astype(F32)
    x_sum = conv(x_in, px_ref, taps)
    x_sig = jax.nn.sigmoid(x_sum)
    act = x_sum * x_sig
    step_wide = expand(step, spread)
    xs = act * step_wide
    gx_ref[taps + 1 : taps + 2, :] += jnp.sum(dy * act, axis=0, keepdims=True)

    lower = lower_mask()
    tri = lower.astype(F32)
    upper = (rows_of((CHUNK, CHUNK)) <= lanes_of((CHUNK, CHUNK))).astype(F32)
    last_row = rows_of((CHUNK, LANES)) == CHUNK - 1
    head_lane = lanes_of((CHUNK, LANES))
    head_row = rows_of((LANES, CHUNK))
    first = lanes_of((CHUNK, 2 * head_dim)) < head_dim
    d_state = None
    d_xs, d_bc, d_decay = [None] * chunks, [None] * chunks, [None] * chunks
    for c in reversed(range(chunks)):
        span = slice(c * CHUNK, (c + 1) * CHUNK)
        cum = jnp.dot(tri, decay[span], precision=HIGH, preferred_element_type=F32)
        cum_t = cum.T
        b_c = bc[span, :states].astype(BF)
        c_c = bc[span, states:].astype(BF)
        xs_c = xs[span]
        dy_c = dy[span]
        scores = mm_t(c_c, b_c)
        d_scores = jnp.zeros((CHUNK, CHUNK), F32)
        by_row = jnp.zeros((CHUNK, LANES), F32)
        by_col = jnp.zeros((LANES, CHUNK), F32)
        pieces = []
        for p in range(heads // 2):
            two = slice(p * 2 * head_dim, (p + 1) * 2 * head_dim)
            dy_two = pair_rows(dy_c[:, two], first).astype(BF)
            d_mix = mm_t(dy_two, xs_c[:, two])
            mixes = []
            for i, h in enumerate((2 * p, 2 * p + 1)):
                gap = jnp.minimum(cum[:, h : h + 1] - cum_t[h : h + 1, :], 0.0)
                fall = jnp.where(lower, jnp.exp(gap), 0.0)
                mixes.append((fall * scores).astype(BF))
                d_fall = d_mix[i * CHUNK : (i + 1) * CHUNK] * fall
                d_scores = d_scores + d_fall
                both = d_fall * scores
                by_row = jnp.where(head_lane == h, jnp.sum(both, axis=1, keepdims=True), by_row)
                by_col = jnp.where(head_row == h, jnp.sum(both, axis=0, keepdims=True), by_col)
            pieces.append(t_mm(jnp.concatenate(mixes, axis=0), dy_two))
        d_xs_c = jnp.concatenate(pieces, axis=1)
        d_c = mm(d_scores, b_c)
        d_b = t_mm(d_scores, c_c)
        d_cum = by_row - by_col.T
        new_state = None
        if c > 0:
            before = st_ref[c - 1]
            grow = expand(jnp.exp(cum), spread)
            d_off = dy_c * grow
            new_state = t_mm(c_c, d_off)
            d_c = d_c + mm_t(d_off, before)
            d_cum = d_cum + mm_t(d_off * mm(c_c, before), spread)
        if c + 1 < chunks:
            last = cum[CHUNK - 1 : CHUNK, :]
            tail = expand(jnp.exp(last - cum), spread)
            tailed = xs_c * tail
            d_tailed = mm(b_c, d_state)
            d_b = d_b + mm_t(tailed, d_state)
            d_xs_c = d_xs_c + d_tailed * tail
            lost = mm_t(d_tailed * tailed, spread)
            d_last = jnp.sum(lost, axis=0, keepdims=True)
            if c > 0:
                whole = expand(jnp.exp(jnp.broadcast_to(last, (states, LANES))), spread)
                d_last = d_last + jnp.sum(mm_t(d_state * before * whole, spread), axis=0, keepdims=True)
                new_state = new_state + d_state * whole
            d_cum = d_cum - lost + jnp.where(last_row, d_last, 0.0)
        d_state = new_state
        d_xs[c] = d_xs_c
        d_bc[c] = jnp.concatenate([d_b, d_c], axis=1)
        d_decay[c] = jnp.dot(upper, d_cum, precision=HIGH, preferred_element_type=F32)
    d_xs = jnp.concatenate(d_xs, axis=0)
    d_bc = jnp.concatenate(d_bc, axis=0)
    d_decay = jnp.concatenate(d_decay, axis=0)

    d_step = mm_t(act * d_xs, spread) + d_decay * rate
    gh_ref[1:2, :] += jnp.sum(d_decay * decay, axis=0, keepdims=True)
    d_dt = d_step * jax.nn.sigmoid(pre)
    gh_ref[0:1, :] += jnp.sum(d_dt, axis=0, keepdims=True)

    d_act = dy * px_ref[taps + 1 : taps + 2, :] + d_xs * step_wide
    d_sum = d_act * (x_sig * (1.0 + x_sum * (1.0 - x_sig)))
    d_x, d_taps = conv_back(d_sum, x_in, px_ref, taps)
    dx_ref[...] = d_x.astype(BF)
    for k, value in enumerate(d_taps):
        gx_ref[k : k + 1, :] += value
    d_sum = d_bc * (bc_sig * (1.0 + bc_sum * (1.0 - bc_sig)))
    d_bc_in, d_taps = conv_back(d_sum, bc_in, pbc_ref, taps)
    for k, value in enumerate(d_taps):
        gbc_ref[k : k + 1, :] += value
    dbcdt_ref[:, : 2 * states] = d_bc_in.astype(BF)
    dbcdt_ref[:, 2 * states :] = d_dt.astype(BF)


def per_seq(*dims):
    return pl.BlockSpec((None,) + dims, lambda i: (i,) + (0,) * len(dims))


def fixed(*dims):
    return pl.BlockSpec(dims, lambda i: (0,) * len(dims))


PARAMS = pltpu.CompilerParams(dimension_semantics=("arbitrary",), vmem_limit_bytes=60 << 20)


def run_forward(small, gate, x, bcdt, dmix, taps, heads):
    px, pbc, ph = small
    seqs, length, width = x.shape
    states = pbc.shape[1] // 2
    chunks = length // CHUNK
    more = [] if dmix is None else [dmix]
    sums = [jax.ShapeDtypeStruct((seqs, chunks, LANES), F32)] * (1 + len(more))
    return pl.pallas_call(
        functools.partial(forward_kernel, taps=taps, heads=heads, with_dots=bool(more)),
        grid=(seqs,),
        in_specs=[fixed(*px.shape), fixed(*pbc.shape), fixed(*ph.shape), per_seq(length, width), per_seq(length, width), per_seq(length, bcdt.shape[2])]
        + [per_seq(length, width)] * len(more),
        out_specs=[per_seq(length, width), per_seq(length, width), per_seq(chunks - 1, states, width)] + [per_seq(chunks, LANES)] * len(sums),
        out_shape=[
            jax.ShapeDtypeStruct((seqs, length, width), BF),
            jax.ShapeDtypeStruct((seqs, length, width), BF),
            jax.ShapeDtypeStruct((seqs, chunks - 1, states, width), F32),
        ]
        + sums,
        compiler_params=PARAMS,
        cost_estimate=pl.CostEstimate(flops=seqs * 400_000_000, bytes_accessed=seqs * 4_000_000, transcendentals=seqs * 2_000_000),
        name="mix_forward",
    )(px, pbc, ph, gate, x, bcdt, *more)


def run_backward(small, gate, x, bcdt, y, state, dmix, scalars, taps, heads):
    px, pbc, ph = small
    seqs, length, width = x.shape
    smalls = px.shape[1] + pbc.shape[1] + ph.shape[1]
    return pl.pallas_call(
        functools.partial(backward_kernel, taps=taps, heads=heads),
        grid=(seqs,),
        in_specs=[
            fixed(*px.shape), fixed(*pbc.shape), fixed(*ph.shape), per_seq(length, width), per_seq(length, width),
            per_seq(length, bcdt.shape[2]), per_seq(length, width), per_seq(*state.shape[1:]), per_seq(length, width), per_seq(*scalars.shape[1:]),
        ],
        out_specs=[per_seq(length, width), per_seq(length, width), per_seq(length, bcdt.shape[2]), fixed(8, smalls)],
        out_shape=[
            jax.ShapeDtypeStruct((seqs, length, width), BF),
            jax.ShapeDtypeStruct((seqs, length, width), BF),
            jax.ShapeDtypeStruct((seqs, length, bcdt.shape[2]), BF),
            jax.ShapeDtypeStruct((8, smalls), F32),
        ],
        compiler_params=PARAMS,
        cost_estimate=pl.CostEstimate(flops=seqs * 1_200_000_000, bytes_accessed=seqs * 6_000_000, transcendentals=seqs * 4_000_000),
        name="mix_backward",
    )(px, pbc, ph, gate, x, bcdt, y, state, dmix, scalars)


MESH = pl.DeviceIdType.MESH
VM = pl.BlockSpec(memory_space=pltpu.VMEM)


def partners():
    section = lax.axis_index("section")
    rep = lax.axis_index("rep")
    xb = rep % PAIR
    return section, xb, {"section": 1 - section}, {"rep": rep + 1 - 2 * xb}


def greet(*devices):
    barrier = pltpu.get_barrier_semaphore()
    for device in devices:
        pl.semaphore_signal(barrier, inc=1, device_id=device, device_id_type=MESH)
    pl.semaphore_wait(barrier, len(devices))


def remote(src, dst, send, recv, device):
    return pltpu.make_async_remote_copy(src_ref=src, dst_ref=dst, send_sem=send, recv_sem=recv, device_id=device, device_id_type=MESH)


def sums_kernel(v_ref, out_ref, got_ref, half_ref, send, recv):
    _, _, peer, beside = partners()
    greet(peer, beside)
    first = remote(v_ref, got_ref.at[0], send.at[0], recv.at[0], peer)
    first.start()
    first.wait()
    half_ref[...] = v_ref[...] + got_ref[0]
    second = remote(half_ref, got_ref.at[1], send.at[1], recv.at[1], beside)
    second.start()
    second.wait()
    out_ref[...] = half_ref[...] + got_ref[1]


def run_sums(v, collective_id):
    return pl.pallas_call(
        sums_kernel,
        in_specs=[VM],
        out_specs=VM,
        out_shape=jax.ShapeDtypeStruct(v.shape, F32),
        scratch_shapes=[pltpu.VMEM((2,) + v.shape, F32), pltpu.VMEM(v.shape, F32), pltpu.SemaphoreType.DMA((2,)), pltpu.SemaphoreType.DMA((2,))],
        compiler_params=pltpu.CompilerParams(collective_id=collective_id, has_side_effects=True),
        cost_estimate=pl.CostEstimate(flops=10_000_000, bytes_accessed=20_000_000, transcendentals=0),
        name="token_sums",
    )(v)


def exchange(part_ref, got_a, held, got_x, send, recv, use):
    section, _, peer, beside = partners()
    per = part_ref.shape[1] // CHUNK
    steps = PAIR * per

    def at(i):
        return i // per, pl.ds(pl.multiple_of(i % per * CHUNK, CHUNK), CHUNK)

    def to_peer(i):
        x, span = at(i)
        return remote(part_ref.at[x * 2 + 1 - section, span], got_a.at[i], send.at[0, i], recv.at[0, i], peer)

    def to_beside(i):
        return remote(held.at[i], got_x.at[i], send.at[1, i], recv.at[1, i], beside)

    def start_peer(i, _):
        to_peer(i).start()
        return 0

    def add(i, _):
        to_peer(i).wait_recv()
        x, span = at(i)
        held[i] = (part_ref[x * 2 + section, span].astype(F32) + got_a[i].astype(F32)).astype(BF)

        @pl.when(i > 0)
        def _():
            to_beside(i - 1).start()

        return 0

    def finish(i):
        to_beside(i).wait_recv()
        x, span = at(i)
        use(i, x, span, held[i].astype(F32) + got_x[i].astype(F32))

    def drain(i, _):
        to_peer(i).wait_send()
        to_beside(i).wait_send()
        return 0

    lax.fori_loop(0, steps, start_peer, 0)
    yield
    lax.fori_loop(0, steps, add, 0)
    yield
    to_beside(steps - 1).start()
    yield
    for i in range(steps):
        finish(i)
        yield
    lax.fori_loop(0, steps, drain, 0)


def weights_flow(b, q_ref, o_ref, w_in, w_out, qs, qr, os_, or_, *, ns, ny, split=False):
    section, xb, peer, _ = partners()
    z = lax.axis_index("shard")
    yb = lax.axis_index("rep") // PAIR
    half = ns // 2
    part = q_ref.shape[2] // PARTS
    home = z // half

    def y_peer(k):
        return {"rep": (yb + k) % ny * PAIR + xb}

    def rows_at(h):
        return pl.ds(h * part, part)

    def there(way):
        return z < ns - 1 if way > 0 else z > 0

    def first(src, way, h):
        return remote(src, w_in.at[yb, z, rows_at(h)], qs.at[0, (way + 1) // 2, h], qr.at[yb, z, h], {"shard": z + way})

    def chip(j, h):
        return remote(q_ref.at[1 - b, j, rows_at(h)], w_in.at[j, z, rows_at(h)], qs.at[1, j, h], qr.at[j, z, h], peer)

    def stay(j, h):
        return pltpu.make_async_copy(q_ref.at[b, j, rows_at(h)], w_in.at[j, z, rows_at(h)], qs.at[2 + ny, j, h])

    def onward(place, way, h):
        block = w_in.at[yb, place, rows_at(h)]
        return remote(block, block, qs.at[2, place, h], qr.at[yb, place, h], {"shard": z + way})

    def across(place, k, h):
        block = w_in.at[yb, place, rows_at(h)]
        return remote(block, block, qs.at[2 + k, place, h], qr.at[yb, place, h], y_peer(k))

    def arrival(j, place, h):
        block = w_in.at[j, place, rows_at(h)]
        return remote(block, block, qs.at[2, place, h], qr.at[j, place, h], peer)

    def o_first(src, way):
        return remote(src, w_out.at[z % half, yb], os_.at[0, (way + 1) // 2], or_.at[z % half, yb], {"shard": z + way})

    def o_chip(j):
        return remote(o_ref.at[j], w_out.at[z % half, j], os_.at[1, j], or_.at[z % half, j], peer)

    def o_stay(j):
        return pltpu.make_async_copy(o_ref.at[j], w_out.at[z % half, j], os_.at[1, j])

    def o_onward(k, way):
        block = w_out.at[k, yb]
        return remote(block, block, os_.at[2, k], or_.at[k, yb], {"shard": z + way})

    def o_across(k, i):
        block = w_out.at[k, yb]
        return remote(block, block, os_.at[2 + i, k], or_.at[k, yb], y_peer(i))

    def o_arrival(k, j):
        block = w_out.at[k, j]
        return remote(block, block, os_.at[2, k], or_.at[k, j], peer)

    def along(copy):
        for way in (1, -1):
            @pl.when(there(way))
            def _():
                copy(way).start()

    def start():
        @pl.when(section == b)
        def _():
            for h in range(PARTS):
                chip(yb, h).start()

            @pl.when(home != b)
            def _():
                o_chip(yb).start()

            for h in range(PARTS):
                along(lambda way: first(q_ref.at[b, yb, rows_at(h)], way, h))

            @pl.when(home == b)
            def _():
                along(lambda way: o_first(o_ref.at[yb], way))

            for k in range(ny):
                j = (yb + k) % ny
                for h in range(PARTS):
                    if k:
                        chip(j, h).start()
                    stay(j, h).start()

                @pl.when(home == b)
                def _():
                    o_stay(j).start()

                if k:
                    @pl.when(home != b)
                    def _():
                        o_chip(j).start()

        @pl.when(section != b)
        def _():
            for h in range(PARTS):
                arrival(yb, z, h).wait_recv()
                along(lambda way: first(w_in.at[yb, z, rows_at(h)], way, h))

            @pl.when(home != b)
            def _():
                o_arrival(z % half, yb).wait_recv()
                along(lambda way: o_first(w_out.at[z % half, yb], way))

    def relay_in(d, h=None):
        for h in range(PARTS) if h is None else (h,):
            for way in (1, -1):
                place = z - way * d

                @pl.when((place >= 0) & (place < ns))
                def _():
                    arrival(yb, place, h).wait_recv()

                    @pl.when(there(way))
                    def _():
                        onward(place, way, h).start()

                    for k in range(1, ny):
                        across(place, k, h).start()

    def relay_out(d):
        for way in (1, -1):
            place = z - way * d
            k = place - section * half

            @pl.when((place >= 0) & (place < ns) & (k >= 0) & (k < half))
            def _():
                o_arrival(k, yb).wait_recv()

                @pl.when(there(way))
                def _():
                    o_onward(k, way).start()

                for i in range(1, ny):
                    o_across(k, i).start()

    def finish_in():
        for place in range(ns):
            @pl.when(place != z)
            def _():
                for h in range(PARTS):
                    for k in range(1, ny):
                        arrival((yb + k) % ny, place, h).wait_recv()
                        across(place, k, h).wait_send()

                    @pl.when(jnp.where(place < z, z < ns - 1, z > 0))
                    def _():
                        onward(place, 1, h).wait_send()

        for way in (1, -1):
            @pl.when(there(way))
            def _():
                for h in range(PARTS):
                    first(w_in.at[yb, z, rows_at(h)], way, h).wait_send()

        @pl.when(section != b)
        def _():
            for k in range(1, ny):
                for h in range(PARTS):
                    arrival((yb + k) % ny, z, h).wait_recv()

        @pl.when(section == b)
        def _():
            for j in range(ny):
                for h in range(PARTS):
                    chip(j, h).wait_send()
                    stay(j, h).wait()

    def finish_out():
        @pl.when((section != b) & (home != b))
        def _():
            for k in range(1, ny):
                o_arrival(z % half, (yb + k) % ny).wait_recv()

        @pl.when(section == home)
        def _():
            for way in (1, -1):
                @pl.when(there(way))
                def _():
                    o_first(w_out.at[z % half, yb], way).wait_send()

        for k in range(half):
            place = section * half + k

            @pl.when(place != z)
            def _():
                for i in range(1, ny):
                    o_arrival(k, (yb + i) % ny).wait_recv()
                    o_across(k, i).wait_send()

                @pl.when(jnp.where(place < z, z < ns - 1, z > 0))
                def _():
                    o_onward(k, 1).wait_send()

        @pl.when(section == b)
        def _():
            for j in range(ny):
                @pl.when(home == b)
                def _():
                    o_stay(j).wait()

                @pl.when(home != b)
                def _():
                    o_chip(j).wait_send()

    def relay(d):
        relay_in(d)
        relay_out(d)

    def finish():
        finish_in()
        finish_out()

    if split:
        return start, relay_in, relay_out, finish
    return start, relay, finish


def weights_shapes(q, o, ns):
    ny = q.shape[1]
    outs = [
        jax.ShapeDtypeStruct((ny, ns) + q.shape[2:], BF),
        jax.ShapeDtypeStruct((ns // 2,) + o.shape, BF),
    ]
    dma = pltpu.SemaphoreType.DMA
    sems = [dma((3 + ny, max(ns, 4), PARTS)), dma((ny, ns, PARTS)), dma((2 + ny, max(ns, 2))), dma((ns // 2, ny))]
    return outs, sems


def greet_line(ns, ny):
    section, xb, peer, beside = partners()
    z = lax.axis_index("shard")
    yb = lax.axis_index("rep") // PAIR
    found = [peer, beside] + [{"rep": (yb + k) % ny * PAIR + xb} for k in range(1, ny)]
    for k in (1, ns - 1):
        found += [{"shard": (z + k) % ns}, {"section": 1 - section, "shard": (z + k) % ns}]
    greet(*found)


def start_kernel(tokens_ref, counts_ref, cw_ref, cb_ref, dtb_ref, alg_ref, dsk_ref, pgn_ref, ogn_ref, bc_ref, dt_ref, q_ref, o_ref,
                 all_tokens, normed_ref, live_out_ref, live_ref, px_ref, pbc_ref, ph_ref, gain_ref, wbc_ref, w_in, w_out,
                 small, all_small, mine, packs, full, row8, all_counts,
                 qs, qr, os_, or_, ts, tr, ss, sr, ps, pr, cs, cr, *, ns, ny, taps, heads):
    section, xb, peer, beside = partners()
    z = lax.axis_index("shard")
    yb = lax.axis_index("rep") // PAIR
    half = ns // 2
    greet_all(ns, ny)
    start, relay, finish = weights_flow(0, q_ref, o_ref, w_in, w_out, qs, qr, os_, or_, ns=ns, ny=ny)

    part = cw_ref.shape[1]
    mine[...] = jnp.zeros_like(mine)
    unit3 = LANES
    mine[0:taps, :part] = cw_ref[...].astype(F32)
    mine[taps : taps + 1, :part] = cb_ref[...].astype(F32)
    for i, ref in enumerate((pgn_ref, ogn_ref)):
        mine[taps + 1 + i : taps + 2 + i, : ref.shape[1]] = ref[...].astype(F32)
    for i, ref in enumerate((dtb_ref, alg_ref, dsk_ref)):
        mine[taps + 3 : taps + 4, i * unit3 : i * unit3 + ref.shape[1]] = ref[...].astype(F32)

    def pack_to(k):
        return remote(mine, packs.at[section, z], ps.at[0, k], pr.at[section, z], {"shard": (z + k) % ns})

    def pack_chip(place):
        return remote(packs.at[section, place], packs.at[section, place], ps.at[1, place], pr.at[section, place], peer)

    def pack_from(t, place):
        return remote(mine, packs.at[t, place], ps.at[0, 0], pr.at[t, place], peer)

    counts = remote(counts_ref, all_counts.at[xb], cs, cr, beside)
    counts.start()
    for k in range(1, ns):
        pack_to(k).start()
    remote(mine, packs.at[section, z], ps.at[0, 0], pr.at[section, z], peer).start()
    packs[section, z] = mine[...]
    all_counts[xb] = counts_ref[...]

    def there(way):
        return z < ns - 1 if way > 0 else z > 0

    lanes = bc_ref.shape[1]
    rows = bc_ref.shape[0] // ny
    for j in range(ny):
        small[j] = jnp.zeros_like(small[j])
        small[j, :, :lanes] = bc_ref[j * rows : (j + 1) * rows]
        small[j, :, lanes : lanes + heads] = dt_ref[j * rows : (j + 1) * rows]

    def first(way):
        return remote(small.at[yb], all_small.at[section, z, yb], ss.at[0, (way + 1) // 2, 0], sr.at[section, z, yb], {"shard": z + way})

    def held(place, j):
        return all_small.at[section, place, j]

    def onward(place, way):
        return remote(held(place, yb), held(place, yb), ss.at[1, place, 0], sr.at[section, place, yb], {"shard": z + way})

    def across(place, k):
        return remote(held(place, yb), held(place, yb), ss.at[1 + k, place, 0], sr.at[section, place, yb], {"rep": (yb + k) % ny * PAIR + xb})

    def chip(place, j):
        return remote(held(place, j), held(place, j), ss.at[1 + ny, place, j], sr.at[section, place, j], peer)

    def arrival(b, place, j):
        return remote(all_small.at[b, place, j], all_small.at[b, place, j], ss.at[1, place, 0], sr.at[b, place, j], peer)

    for way in (1, -1):
        @pl.when(there(way))
        def _():
            first(way).start()

    def tokens_beside(m):
        return remote(tokens_ref.at[m], all_tokens.at[section, xb, m], ts.at[0, m], tr.at[section, xb, m], beside)

    def tokens_chip(x, m):
        if x is None:
            return remote(tokens_ref.at[m], all_tokens.at[section, xb, m], ts.at[1, m], tr.at[section, xb, m], peer)
        place = all_tokens.at[section, x, m]
        return remote(place, place, ts.at[2, m], tr.at[section, x, m], peer)

    def tokens_arrival(b, x, m):
        place = all_tokens.at[b, x, m]
        return remote(place, place, ts.at[0, m], tr.at[b, x, m], peer)

    micro, seq_len, _ = tokens_ref.shape
    start()
    for m in range(micro):
        tokens_beside(m).start()
        tokens_chip(None, m).start()
        all_tokens[section, xb, m] = tokens_ref[m]
    for j in range(ny):
        all_small[section, z, j] = small[j]

    def relay_small(d):
        for way in (1, -1):
            place = z - way * d

            @pl.when((place >= 0) & (place < ns))
            def _():
                arrival(section, place, yb).wait_recv()

                @pl.when(there(way))
                def _():
                    onward(place, way).start()

                for k in range(1, ny):
                    across(place, k).start()
                chip(place, yb).start()

    def unpack():
        channels = part * ns
        inner = ogn_ref.shape[1] * ns
        cw = inner // ns // PAIR
        unit = dtb_ref.shape[1] // PAIR
        mine_w = half * cw
        for place in range(ns):
            pack_from(1 - section, place).wait_recv()
        ph_ref[...] = jnp.zeros_like(ph_ref)
        px_ref[...] = jnp.zeros_like(px_ref)
        pbc_ref[...] = jnp.zeros_like(pbc_ref)
        spread = head_map(mine_w, 2 * PAIR * mine_w // heads)
        for b in range(2):
            for at in range(ns):
                full[0 : taps + 1, at * part : (at + 1) * part] = packs[b, at, 0 : taps + 1, :part]
                size = pgn_ref.shape[1]
                gain_ref[b, :, at * size : (at + 1) * size] = packs[b, at, taps + 1 : taps + 2, :size]
            pbc_ref[b, 0 : taps + 1, :] = full[0 : taps + 1, inner:channels]
            row8[...] = jnp.zeros_like(row8)
            for t in range(2):
                for q in range(PAIR):
                    @pl.when((section == t) & (xb == q))
                    def _():
                        for k in range(half):
                            at = t * half + k
                            col = (at * PAIR + q) * cw
                            put = slice(k * cw, (k + 1) * cw)
                            lane = slice(k * unit, (k + 1) * unit)
                            take = slice(q * unit, (q + 1) * unit)
                            px_ref[b, 0 : taps + 1, put] = full[0 : taps + 1, col : col + cw]
                            px_ref[b, taps + 2 : taps + 3, put] = packs[b, at, taps + 2 : taps + 3, q * cw : (q + 1) * cw]
                            ph_ref[b, 0:1, lane] = packs[b, at, taps + 3 : taps + 4, take]
                            ph_ref[b, 1:2, lane] = packs[b, at, taps + 3 : taps + 4, unit3 + q * unit : unit3 + (q + 1) * unit]
                            row8[0:1, lane] = packs[b, at, taps + 3 : taps + 4, 2 * unit3 + q * unit : 2 * unit3 + (q + 1) * unit]
            px_ref[b, taps + 1 : taps + 2, :] = mm(row8[...], spread)[0:1]

    def shared_columns():
        unit = dtb_ref.shape[1] // PAIR
        shape = (wbc_ref.shape[2] - lanes, LANES)
        source, head = rows_of(shape), lanes_of(shape)
        wanted = ((section * half + head // unit) * PAIR + xb) * unit + head % unit
        chosen = ((source == wanted) & (head < half * unit)).astype(BF)
        for b in range(2):
            for at in range(ns):
                for j in range(ny):
                    low = (at * ny + j) * rows
                    wbc_ref[b, low : low + rows, :lanes] = all_small[b, at, j, :, :lanes]
                    wbc_ref[b, low : low + rows, lanes:] = mm(all_small[b, at, j, :, lanes:], chosen).astype(BF)

    def prepare():
        per = seq_len // CHUNK
        for x in range(PAIR):
            for m in range(micro):
                for c in range(per):
                    row = (x * micro + m) * per + c
                    at = lanes_of((1, LANES)).astype(F32) + float(c * CHUNK)
                    live_ref[row : row + 1, :] = (at < all_counts[x, m : m + 1, :]).astype(F32)

        def step(i, _):
            x, m, c = i // (micro * per), i // per % micro, i % per
            span = pl.ds(pl.multiple_of(c * CHUNK, CHUNK), CHUNK)
            wide = all_tokens[0, x, m, span].astype(F32)
            normed_ref[x * micro + m, span] = (wide * rms(wide) * gain_ref[0]).astype(BF)
            live = as_column(live_ref[pl.ds(i, 1), :])
            live_out_ref[x * micro + m, span] = (all_tokens[1, x, m, span].astype(F32) * live).astype(BF)
            return 0

        lax.fori_loop(0, PAIR * micro * per, step, 0)

    relay_small(1)
    for k in range(1, ns):
        pack_from(section, (z + k) % ns).wait_recv()
        pack_chip((z + k) % ns).start()
    for j in range(ny):
        chip(z, j).start()
    for d in range(1, ns):
        if d == ns - 1:
            unpack()
            for m in range(micro):
                tokens_arrival(section, 1 - xb, m).wait_recv()
                tokens_chip(1 - xb, m).start()
            counts.wait_send()
            remote(counts_ref, all_counts.at[1 - xb], cs, cr, beside).wait_recv()
            for m in range(micro):
                for x in range(PAIR):
                    tokens_arrival(1 - section, x, m).wait_recv()
            prepare()
        relay(d)
        if d + 1 < ns:
            relay_small(d + 1)
    for place in range(ns):
        @pl.when(place != z)
        def _():
            for k in range(1, ny):
                j = (yb + k) % ny
                arrival(section, place, j).wait_recv()
                chip(place, j).start()
    for place in range(ns):
        for j in range(ny):
            arrival(1 - section, place, j).wait_recv()
    shared_columns()
    finish()
    for m in range(micro):
        tokens_beside(m).wait_send()
        tokens_chip(None, m).wait_send()
        tokens_chip(1 - xb, m).wait_send()
    for k in range(1, ns):
        pack_to(k).wait_send()
        pack_chip((z + k) % ns).wait_send()
    pack_from(section, z).wait_send()
    for way in (1, -1):
        @pl.when(there(way))
        def _():
            first(way).wait_send()
    for place in range(ns):
        for j in range(ny):
            chip(place, j).wait_send()

        @pl.when(place != z)
        def _():
            for k in range(1, ny):
                across(place, k).wait_send()

            @pl.when(jnp.where(place < z, z < ns - 1, z > 0))
            def _():
                onward(place, 1).wait_send()


def greet_all(ns, ny):
    section, xb, peer, beside = partners()
    z = lax.axis_index("shard")
    yb = lax.axis_index("rep") // PAIR
    found = [peer, beside] + [{"rep": (yb + k) % ny * PAIR + xb} for k in range(1, ny)]
    for k in range(1, ns):
        found += [{"shard": (z + k) % ns}, {"section": 1 - section, "shard": (z + k) % ns}]
    greet(*found)


def run_start(tokens, counts, smalls, bc, dt, q, o, heads):
    conv_weight, _, dt_bias, _, _, _, out_gain = smalls
    ny = q.shape[1]
    ns = heads // dt_bias.shape[1]
    micro, seq_len, width = tokens.shape
    taps = conv_weight.shape[0]
    inner = out_gain.shape[1] * ns
    mine_w = inner // (2 * PAIR)
    states2 = bc.shape[1]
    seqs = PAIR * micro
    outs, sems = weights_shapes(q, o, ns)
    dma = pltpu.SemaphoreType.DMA
    hbm = pl.BlockSpec(memory_space=pl.ANY)
    shape = jax.ShapeDtypeStruct
    rows = bc.shape[0] // ny
    pack = (8, -(-max(conv_weight.shape[1], out_gain.shape[1]) // LANES) * LANES)
    return pl.pallas_call(
        functools.partial(start_kernel, ns=ns, ny=ny, taps=taps, heads=heads),
        in_specs=[VM] * 13,
        out_specs=[VM] * 9 + [hbm, hbm],
        out_shape=[
            shape((2, PAIR) + tokens.shape, BF),
            shape((seqs, seq_len, width), BF),
            shape((seqs, seq_len, width), BF),
            shape((seqs * seq_len // CHUNK, LANES), F32),
            shape((2, 8, mine_w), F32),
            shape((2, 8, states2), F32),
            shape((2, 8, LANES), F32),
            shape((2, 1, width), F32),
            shape((2, width, states2 + LANES), BF),
        ]
        + outs,
        scratch_shapes=[
            pltpu.VMEM((ny, rows, states2 + LANES), BF),
            pltpu.VMEM((2, ns, ny, rows, states2 + LANES), BF),
            pltpu.VMEM(pack, F32),
            pltpu.VMEM((2, ns) + pack, F32),
            pltpu.VMEM((8, conv_weight.shape[1] * ns), F32),
            pltpu.VMEM((8, LANES), F32),
            pltpu.VMEM((PAIR,) + counts.shape, F32),
        ]
        + sems
        + [
            dma((3, 2)), dma((2, PAIR, 2)), dma((2 + ny, max(ns, 2), ny)), dma((2, ns, ny)),
            dma((2, ns)), dma((2, ns)), dma(()), dma(()),
        ],
        compiler_params=comm_params(5),
        cost_estimate=pl.CostEstimate(flops=50_000_000, bytes_accessed=200_000_000, transcendentals=0),
        name="start",
    )(tokens, counts, *smalls, bc, dt, q, o)


def rms(v):
    return lax.rsqrt(jnp.mean(v * v, axis=-1, keepdims=True) + EPSILON)


def spread_out(out_ref, send, recv, peer, per):
    def copy(i, owner):
        span = pl.ds(pl.multiple_of(i % per * CHUNK, CHUNK), CHUNK)
        place = out_ref.at[i // per * 2 + owner, span]
        return remote(place, place, send.at[2, i], recv.at[2, i], peer)

    return copy


def onward_kernel(part_ref, tokens_ref, sums_ref, live_ref, gain_ref, q_ref, o_ref, hidden_ref, normed_ref, rate_ref, gain_out_ref, w_in, w_out,
                  got_a, held, got_x, got_s, half_s, rows_ref, send, recv, send_s, recv_s, rows_s, qs, qr, os_, or_, *, inner, ns, ny):
    section, _, peer, beside = partners()
    per = part_ref.shape[1] // CHUNK
    steps = PAIR * per
    greet_line(ns, ny)
    start, relay_in, relay_out, finish = weights_flow(1, q_ref, o_ref, w_in, w_out, qs, qr, os_, or_, ns=ns, ny=ny, split=True)

    def rows_at(x):
        return pltpu.make_async_copy(tokens_ref.at[0, x, section], rows_ref.at[x], rows_s.at[x])

    for x in range(PAIR):
        rows_at(x).start()
    first = remote(sums_ref, got_s.at[0], send_s.at[0], recv_s.at[0], peer)
    second = remote(half_s, got_s.at[1], send_s.at[1], recv_s.at[1], beside)
    first.start()
    copy = spread_out(hidden_ref, send, recv, peer, per)

    def use(i, x, span, total):
        seq = x * 2 + section
        scale = as_column(rate_ref[pl.ds(seq * per + i % per, 1), :] * live_ref[pl.ds(seq * per + i % per, 1), :])
        gained = scale * total
        gain_out_ref[i] = gained.astype(BF)
        low = (rows_ref[x, span].astype(F32) + gained).astype(BF)
        hidden_ref[seq, span] = low

        @pl.when(i > 0)
        def _():
            copy(i - 1, section).start()

        wide = low.astype(F32)
        normed_ref[seq, span] = (wide * rms(wide) * gain_ref[...]).astype(BF)

    def other(i, _):
        copy(i, section).wait_recv()
        seq = i // per * 2 + 1 - section
        span = pl.ds(pl.multiple_of(i % per * CHUNK, CHUNK), CHUNK)
        wide = hidden_ref[seq, span].astype(F32)
        normed_ref[seq, span] = (wide * rms(wide) * gain_ref[...]).astype(BF)
        return 0

    def drain(i, _):
        copy(i, section).wait_send()
        return 0

    stages = exchange(part_ref, got_a, held, got_x, send, recv, use)
    next(stages)
    first.wait()
    half_s[...] = sums_ref[...] + got_s[0]
    second.start()
    start()
    next(stages)
    next(stages)
    second.wait()
    rate_ref[...] = lax.rsqrt((half_s[...] + got_s[1]) / inner + EPSILON)
    work = [lambda d=d, h=h: relay_in(d, h) if h < PARTS else relay_out(d) for d in range(1, ns) for h in range(PARTS + 1)]

    def relays(count):
        for _ in range(min(count, len(work))):
            work.pop(0)()

    for x in range(PAIR):
        rows_at(x).wait()
    relays(PARTS + 2)
    for _ in range(steps):
        next(stages)
        relays(1)
    copy(steps - 1, section).start()
    lax.fori_loop(0, steps, other, 0)
    for step in work:
        step()
    finish()
    for _ in stages:
        pass
    lax.fori_loop(0, steps, drain, 0)


def back_kernel(part_ref, hidden_ref, tokens_ref, gained_ref, live_ref, gain_ref, out_ref, live_out_ref, dots_ref,
                got_a, held, got_x, dots_own, dots_got, rows_ref, cot_ref, send, recv, send_s, recv_s, rows_s, cot_s):
    section, _, peer, beside = partners()
    per = part_ref.shape[1] // CHUNK
    steps = PAIR * per
    greet(peer, beside)

    def rows_at(x):
        return pltpu.make_async_copy(hidden_ref.at[x * 2 + section], rows_ref.at[x], rows_s.at[x])

    def cot_at(x):
        return pltpu.make_async_copy(tokens_ref.at[1, x, section], cot_ref.at[x], cot_s.at[x])

    for x in range(PAIR):
        rows_at(x).start()
        cot_at(x).start()
    dots_own[...] = jnp.zeros_like(dots_own)
    copy = spread_out(out_ref, send, recv, peer, per)

    def live_of(seq, i):
        return as_column(live_ref[pl.ds(seq * per + i % per, 1), :])

    def use(i, x, span, total):
        seq = x * 2 + section
        rows = rows_ref[x, span].astype(F32)
        inv = rms(rows)
        hat = rows * inv
        d_hat = total * gain_ref[...]
        d_rows = inv * (d_hat - hat * jnp.mean(d_hat * hat, axis=-1, keepdims=True))
        low = (cot_ref[x, span].astype(F32) + d_rows).astype(BF)
        out_ref[seq, span] = low

        @pl.when(i > 0)
        def _():
            copy(i - 1, section).start()

        live = low.astype(F32) * live_of(seq, i)
        live_out_ref[seq, span] = live.astype(BF)
        dots_own[pl.ds(i, 1), :] = as_row(jnp.sum(live * gained_ref[i].astype(F32), axis=1, keepdims=True))

    def other(i, _):
        copy(i, section).wait_recv()
        seq = i // per * 2 + 1 - section
        span = pl.ds(pl.multiple_of(i % per * CHUNK, CHUNK), CHUNK)
        live_out_ref[seq, span] = (out_ref[seq, span].astype(F32) * live_of(seq, i)).astype(BF)
        return 0

    def drain(i, _):
        copy(i, section).wait_send()
        return 0

    stages = exchange(part_ref, got_a, held, got_x, send, recv, use)
    for _ in range(3):
        next(stages)
    for x in range(PAIR):
        rows_at(x).wait()
        cot_at(x).wait()
    for i in range(steps):
        next(stages)
    copy(steps - 1, section).start()
    dots = remote(dots_own, dots_got, send_s.at[0], recv_s.at[0], peer)
    lax.fori_loop(0, steps, other, 0)
    dots.start()
    for _ in stages:
        pass
    lax.fori_loop(0, steps, drain, 0)
    dots.wait()
    for x in range(PAIR):
        for c in range(per):
            i = x * per + c
            dots_ref[pl.ds((x * 2 + section) * per + c, 1), :] = dots_own[i : i + 1, :]
            dots_ref[pl.ds((x * 2 + 1 - section) * per + c, 1), :] = dots_got[i : i + 1, :]


def exchange_scratch(part):
    steps = PAIR * part.shape[1] // CHUNK
    block = (steps, CHUNK, part.shape[2])
    return [pltpu.VMEM(block, BF)] * 3, [pltpu.SemaphoreType.DMA((3, steps)), pltpu.SemaphoreType.DMA((3, steps))]


def own_rows(part):
    return pltpu.VMEM((PAIR,) + part.shape[1:], BF)


def comm_params(collective_id):
    return pltpu.CompilerParams(collective_id=collective_id, has_side_effects=True, vmem_limit_bytes=60 << 20)


def run_onward(part, rows, sums, live, gain, q, o, inner, ns):
    wide, sems = exchange_scratch(part)
    steps = PAIR * part.shape[1] // CHUNK
    small = pltpu.VMEM(sums.shape, F32)
    ny = q.shape[1]
    outs, more = weights_shapes(q, o, ns)
    return pl.pallas_call(
        functools.partial(onward_kernel, inner=inner, ns=ns, ny=ny),
        in_specs=[VM, pl.BlockSpec(memory_space=pl.ANY)] + [VM] * 5,
        out_specs=[VM] * 4 + [pl.BlockSpec(memory_space=pl.ANY)] * 2,
        out_shape=[
            jax.ShapeDtypeStruct(part.shape, BF),
            jax.ShapeDtypeStruct(part.shape, BF),
            jax.ShapeDtypeStruct(sums.shape, F32),
            jax.ShapeDtypeStruct((steps, CHUNK, part.shape[2]), BF),
        ]
        + outs,
        scratch_shapes=wide + [pltpu.VMEM((2,) + sums.shape, F32), small, own_rows(part)] + sems + [pltpu.SemaphoreType.DMA((2,))] * 3 + more,
        compiler_params=comm_params(1),
        cost_estimate=pl.CostEstimate(flops=50_000_000, bytes_accessed=150_000_000, transcendentals=0),
        name="onward",
    )(part, rows, sums, live, gain, q, o)


def run_back(part, hidden, tokens, gained, live, gain):
    wide, sems = exchange_scratch(part)
    small = pltpu.VMEM((8, LANES), F32)
    hbm = pl.BlockSpec(memory_space=pl.ANY)
    return pl.pallas_call(
        back_kernel,
        in_specs=[VM, hbm, hbm, VM, VM, VM],
        out_specs=[VM] * 3,
        out_shape=[
            jax.ShapeDtypeStruct(part.shape, BF),
            jax.ShapeDtypeStruct(part.shape, BF),
            jax.ShapeDtypeStruct(live.shape, F32),
        ],
        scratch_shapes=wide + [small, small, own_rows(part), own_rows(part)] + sems + [pltpu.SemaphoreType.DMA((2,))] * 4,
        compiler_params=comm_params(2),
        cost_estimate=pl.CostEstimate(flops=50_000_000, bytes_accessed=150_000_000, transcendentals=0),
        name="back",
    )(part, hidden, tokens, gained, live, gain)


PARTS = 2
PIECE_ROWS = 48
BLOCK = 16


def by_rows(count, body):
    def step(i, _):
        body(pl.multiple_of(i * BLOCK, BLOCK))
        return 0

    lax.fori_loop(0, count // BLOCK, step, 0)


def line_steps(n):
    return [step for i in range(n - 1) for step in ((1, n - 1 - i), (-1, i))]


def hand_out(b, boards, owns, pc_s, pc_r, *, ny):
    section, xb, peer, beside = partners()
    yb = lax.axis_index("rep") // PAIR

    def y_peer(k):
        return {"rep": (yb + k) % ny * PAIR + xb}

    def y_from(k):
        return (yb + ny - k) % ny

    def span_of(h):
        return pl.ds(pl.multiple_of(h * PIECE_ROWS, PIECE_ROWS), PIECE_ROWS)

    def piece(i, x, y, t, h, kind, device):
        place = boards[i].at[x, y, t, span_of(h)]
        return remote(place, place, pc_s.at[i, kind, x, y, t, h], pc_r.at[i, x, y, t, h], device)

    def offer(i, h):
        return remote(owns[i].at[span_of(h)], boards[i].at[xb, yb, 1 - b, span_of(h)],
                      pc_s.at[i, 0, xb, yb, 1 - b, h], pc_r.at[i, xb, yb, 1 - b, h], peer)

    def gather_chip(i, h):
        @pl.when(section == b)
        def _():
            boards[i][xb, yb, b, span_of(h)] = owns[i][span_of(h)]

        @pl.when(section != b)
        def _():
            offer(i, h).start()

    def gather_side(i, h):
        @pl.when(section == b)
        def _():
            piece(i, xb, yb, 1 - b, h, 0, peer).wait_recv()
            for t in range(2):
                piece(i, xb, yb, t, h, ny, beside).start()

    def gather_y(i, h):
        @pl.when(section == b)
        def _():
            for t in range(2):
                for k in range(1, ny):
                    piece(i, xb, yb, t, h, k, y_peer(k)).start()

    def gather_x(i, h):
        @pl.when(section == b)
        def _():
            for k in range(1, ny):
                for t in range(2):
                    piece(i, xb, y_from(k), t, h, k, peer).wait_recv()
                    piece(i, xb, y_from(k), t, h, ny, beside).start()

    def gather_end(i, h):
        @pl.when(section == b)
        def _():
            for y in range(ny):
                for t in range(2):
                    piece(i, 1 - xb, y, t, h, ny, beside).wait_recv()
                    piece(i, xb, y, t, h, ny, peer).wait_send()
            for t in range(2):
                for k in range(1, ny):
                    piece(i, xb, yb, t, h, k, peer).wait_send()

        @pl.when(section != b)
        def _():
            offer(i, h).wait_send()

    return gather_chip, gather_side, gather_y, gather_x, gather_end


def each(count, body):
    def step(i, _):
        body(i)
        return 0

    lax.fori_loop(0, count, step, 0)


def reduce_flow(b, ga_ref, gb_ref, boards, got_ya, acc_a, got_za, own_a, acc_b, got_zb, own_b, ya_s, ya_r, za_s, za_r, zb_s, zb_r, pc_s, pc_r, *, ns, ny):
    _, xb, peer, _ = partners()
    z = lax.axis_index("shard")
    yb = lax.axis_index("rep") // PAIR
    count = ga_ref.shape[2] // PIECE_ROWS
    steps = line_steps(ns)
    order = []
    for _, target in steps:
        if target not in order:
            order.append(target)
    gather_chip, gather_side, gather_y, gather_x, gather_end = hand_out(b, boards, (own_a, own_b), pc_s, pc_r, ny=ny)

    def y_peer(k):
        return {"rep": (yb + k) % ny * PAIR + xb}

    def span_of(h):
        return pl.ds(pl.multiple_of(h * PIECE_ROWS, PIECE_ROWS), PIECE_ROWS)

    def ya(k, target, h):
        return remote(ga_ref.at[(yb + k) % ny, target, span_of(h)], got_ya.at[k - 1, target, span_of(h)],
                      ya_s.at[k - 1, target, h], ya_r.at[k - 1, target, h], y_peer(k))

    def start(h):
        for target in order:
            @pl.when(target != z)
            def _():
                for k in range(1, ny):
                    ya(k, target, h).start()
        for k in range(1, ny):
            ya(k, z, h).start()

    streams = ((acc_a, got_za, za_s, za_r), (acc_b, got_zb, zb_s, zb_r))

    def line(i, way, target, h):
        acc, got, send, recv = streams[i]
        place = jnp.where(target == z - 1, ns, target) if way < 0 else target
        return remote(acc.at[target, span_of(h)], got.at[place, span_of(h)], send.at[target, h], recv.at[place, h], {"shard": z + way})

    def wait_line(place, h):
        for acc, got, send, recv in streams:
            remote(acc.at[0, span_of(h)], got.at[place, span_of(h)], send.at[0, h], recv.at[place, h], peer).wait_recv()

    def wait_y(target, h):
        for k in range(1, ny):
            remote(ga_ref.at[0, target, span_of(h)], got_ya.at[k - 1, target, span_of(h)], ya_s.at[k - 1, target, h],
                   ya_r.at[k - 1, target, h], peer).wait_recv()

    def add(target, h, into_a, into_b, start, extra):
        span = span_of(h)
        total = ga_ref[yb, target, span].astype(F32)
        for k in range(1, ny):
            total = total + got_ya[k - 1, target, span].astype(F32)
        for place in extra:
            total = total + got_za[place, span].astype(F32)
        into_a[start + (span,)] = total.astype(BF)
        total = gb_ref[target, span].astype(F32)
        for place in extra:
            total = total + got_zb[place, span].astype(F32)
        into_b[start + (span,)] = total.astype(BF)

    def active(way, target):
        return target > z if way > 0 else target < z

    def step(way, target, h):
        wait_y(target, h)
        far = z > 0 if way > 0 else z < ns - 1

        @pl.when(jnp.logical_not(far))
        def _():
            add(target, h, acc_a, acc_b, (target,), ())

        @pl.when(far)
        def _():
            wait_line(target, h)
            add(target, h, acc_a, acc_b, (target,), (target,))

        for i in range(2):
            line(i, way, target, h).start()

    def last(h):
        wait_y(z, h)

        @pl.when(z == 0)
        def _():
            wait_line(ns, h)
            add(z, h, own_a, own_b, (), (ns,))

        @pl.when(z == ns - 1)
        def _():
            wait_line(z, h)
            add(z, h, own_a, own_b, (), (z,))

        @pl.when((z > 0) & (z < ns - 1))
        def _():
            wait_line(z, h)
            wait_line(ns, h)
            add(z, h, own_a, own_b, (), (z, ns))

        for i in range(2):
            gather_chip(i, h)

    def slot(at):
        for way, target in steps:
            h = at - z if way > 0 else at - (ns - 1 - z)

            @pl.when(active(way, target) & (h >= 0) & (h < count))
            def _():
                step(way, target, h)

        mine = at - jnp.where(2 * z > ns - 1, z, ns - 1 - z)
        for late, body in ((0, last), (1, lambda h: [move(i, h) for move in (gather_side, gather_y) for i in range(2)]), (2, lambda h: [gather_x(i, h) for i in range(2)])):
            @pl.when((mine >= late) & (mine < count + late))
            def _():
                body(mine - late)

    def finish():
        def ends(h):
            for i in range(2):
                gather_end(i, h)
            for target in range(ns):
                for k in range(1, ny):
                    ya(k, target, h).wait_send()
            for way, target in steps:
                @pl.when(active(way, target))
                def _():
                    for i in range(2):
                        line(i, way, target, h).wait_send()

        each(count, ends)

    return start, slot, count + ns + 1, finish


def reduce_shapes(ga, gb):
    ny, ns, ra, ca = ga.shape
    rb, cb = gb.shape[1:]
    dma = pltpu.SemaphoreType.DMA
    parts = ra // PIECE_ROWS
    outs = [jax.ShapeDtypeStruct((PAIR, ny, 2, ra, ca), BF), jax.ShapeDtypeStruct((PAIR, ny, 2, rb, cb), BF)]
    scratch = [
        pltpu.VMEM((ny - 1, ns, ra, ca), BF),
        pltpu.VMEM((ns, ra, ca), BF),
        pltpu.VMEM((ns + 1, ra, ca), BF),
        pltpu.VMEM((ra, ca), BF),
        pltpu.VMEM((ns, rb, cb), BF),
        pltpu.VMEM((ns + 1, rb, cb), BF),
        pltpu.VMEM((rb, cb), BF),
        dma((ny - 1, ns, parts)), dma((ny - 1, ns, parts)),
        dma((ns, parts)), dma((ns + 1, parts)),
        dma((ns, parts)), dma((ns + 1, parts)),
        dma((2, ny + 1, PAIR, ny, 2, parts)), dma((2, PAIR, ny, 2, parts)),
    ]
    return outs, scratch


def tail_kernel(ga_ref, gb_ref, pa_ref, pb_ref, vec_ref, p_ref, tokens_ref, cot_all, gain_ref,
                all_a, all_b, vec_out, res_ref, *refs, ns, ny):
    flow, (got_p, held, got_x, give, rows_ref, cot_ref, vec_y, vec_h, vec_z, vec_t, ra_s, ra_r, v_s, v_r, rows_s) = refs[:15], refs[15:]
    section, xb, peer, beside = partners()
    z = lax.axis_index("shard")
    yb = lax.axis_index("rep") // PAIR

    def y_peer(k):
        return {"rep": (yb + k) % ny * PAIR + xb}

    def z_peer(k):
        return {"shard": (z + k) % ns}

    greet(peer, beside, *(y_peer(k) for k in range(1, ny)), *(z_peer(k) for k in range(1, ns)))

    def over_y(k):
        return remote(vec_ref, vec_y.at[k - 1], v_s.at[k], v_r.at[k], y_peer(k))

    def over_z(k):
        return remote(vec_h, vec_z.at[k - 1], v_s.at[ny + k], v_r.at[ny + k], z_peer(k))

    to_chip = remote(vec_t.at[1 - section], vec_out.at[section, xb], v_s.at[0], v_r.at[0], peer)

    def to_side(t):
        return remote(vec_out.at[t, xb], vec_out.at[t, xb], v_s.at[ny + ns + t], v_r.at[ny + ns + t], beside)

    for k in range(1, ny):
        over_y(k).start()

    per = p_ref.shape[1] // CHUNK
    rows_copy = pltpu.make_async_copy(tokens_ref.at[0, xb, section], rows_ref, rows_s.at[0])
    cot_copy = pltpu.make_async_copy(cot_all.at[xb * 2 + section], cot_ref, rows_s.at[1])

    def p_peer(x, c):
        span = pl.ds(c * CHUNK, CHUNK)
        return remote(p_ref.at[x * 2 + 1 - section, span], got_p.at[x, c], ra_s.at[0, x, c], ra_r.at[0, x, c], peer)

    def p_beside(c):
        return remote(held.at[1 - xb, c], got_x.at[c], ra_s.at[1, 0, c], ra_r.at[1, 0, c], beside)

    def p_give(c):
        return remote(give.at[c], res_ref.at[1, pl.ds(c * CHUNK, CHUNK)], ra_s.at[1, 1, c], ra_r.at[1, 1, c], peer)

    boards = (all_a, all_b)
    pieces = flow[13:15]
    chip1, side1, y1, x1, end1 = hand_out(1, boards, (pa_ref, pb_ref), *pieces, ny=ny)
    count = ga_ref.shape[2] // PIECE_ROWS
    start, slot, slots, end0 = reduce_flow(0, ga_ref, gb_ref, boards, *flow, ns=ns, ny=ny)

    def both(body):
        each(count, lambda h: [body(i, h) for i in (1, 0)])

    rows_copy.start()
    cot_copy.start()

    def rows_out():
        for c in range(per):
            for x in range(PAIR):
                p_peer(x, c).start()

    def pieces_side():
        both(side1)

    def pieces_y():
        both(y1)

    def rows_beside():
        for c in range(per):
            for x in range(PAIR):
                p_peer(x, c).wait_recv()

                def body(low):
                    span = pl.ds(low, BLOCK)
                    mine = p_ref[x * 2 + section, pl.ds(c * CHUNK + low, BLOCK)].astype(F32)
                    held[x, c, span] = (mine + got_p[x, c, span].astype(F32)).astype(BF)

                by_rows(CHUNK, body)
            p_beside(c).start()

    def sums_z():
        total = vec_ref[...]
        for k in range(1, ny):
            over_y(k).wait()
            total = total + vec_y[k - 1]
        vec_h[...] = total
        for k in range(1, ns):
            over_z(k).start()

    def pieces_x():
        both(x1)

    def sums_chip():
        total = vec_h[...]
        for k in range(1, ns):
            over_z(k).wait()
            total = total + vec_z[k - 1]
        vec_t[...] = total
        to_chip.start()
        vec_out[section, xb] = vec_t[section]

    def rows_end():
        rows_copy.wait()
        cot_copy.wait()
        for c in range(per):
            p_beside(c).wait_recv()

            def body(low):
                span = pl.ds(low, BLOCK)
                there = pl.ds(c * CHUNK + low, BLOCK)
                total = held[xb, c, span].astype(F32) + got_x[c, span].astype(F32)
                rows = rows_ref[there].astype(F32)
                inv = rms(rows)
                hat = rows * inv
                d_hat = total * gain_ref[...]
                d_rows = inv * (d_hat - hat * jnp.mean(d_hat * hat, axis=-1, keepdims=True))
                low_rows = (cot_ref[there].astype(F32) + d_rows).astype(BF)
                give[c, span] = low_rows

                @pl.when(section == 0)
                def _():
                    res_ref[0, there] = low_rows

            by_rows(CHUNK, body)

        @pl.when(section != 0)
        def _():
            for c in range(per):
                p_give(c).start()

    def sums_side():
        to_chip.wait_send()
        remote(vec_t.at[0], vec_out.at[1 - section, xb], v_s.at[0], v_r.at[0], peer).wait_recv()
        for t in range(2):
            to_side(t).start()

    def sums_end():
        for t in range(2):
            to_side(t).wait_send()
            remote(vec_out.at[t, xb], vec_out.at[t, 1 - xb], v_s.at[ny + ns + t], v_r.at[ny + ns + t], beside).wait_recv()

    ahead = min(3, count)
    rows_out()
    both(chip1)
    each(ahead, start)
    between = ((0, pieces_side), (0, rows_beside), (1, sums_z), (3, sums_chip), (4, rows_end), (5, pieces_y), (6, sums_side), (8, sums_end), (10, pieces_x))

    def go(at, _):
        @pl.when(at + ahead < count)
        def _():
            start(at + ahead)

        slot(at)
        for n, body in between:
            @pl.when(at == n)
            def _():
                body()

        return 0

    lax.fori_loop(0, max(slots, between[-1][0] + 1), go, 0)
    both(end1)
    end0()
    for c in range(per):
        for x in range(PAIR):
            p_peer(x, c).wait_send()
        p_beside(c).wait_send()

        @pl.when(section != 0)
        def _():
            p_give(c).wait_send()

        @pl.when(section == 0)
        def _():
            p_give(c).wait_recv()


def run_tail(ga, gb, pa, pb, vec, p, tokens, cot, gain):
    ny, ns = ga.shape[:2]
    seq_len, width = p.shape[1:]
    per = seq_len // CHUNK
    block = (CHUNK, width)
    dma = pltpu.SemaphoreType.DMA
    hbm = pl.BlockSpec(memory_space=pl.ANY)
    outs, scratch = reduce_shapes(ga, gb)
    return pl.pallas_call(
        functools.partial(tail_kernel, ns=ns, ny=ny),
        in_specs=[VM] * 6 + [hbm, hbm, VM],
        out_specs=[VM] * 4,
        out_shape=outs + [jax.ShapeDtypeStruct((2, PAIR) + vec.shape[1:], F32), jax.ShapeDtypeStruct((2, seq_len, width), BF)],
        scratch_shapes=scratch
        + [
            pltpu.VMEM((PAIR, per) + block, BF),
            pltpu.VMEM((PAIR, per) + block, BF),
            pltpu.VMEM((per,) + block, BF),
            pltpu.VMEM((per,) + block, BF),
            pltpu.VMEM((seq_len, width), BF),
            pltpu.VMEM((seq_len, width), BF),
            pltpu.VMEM((ny - 1,) + vec.shape, F32),
            pltpu.VMEM(vec.shape, F32),
            pltpu.VMEM((ns - 1,) + vec.shape, F32),
            pltpu.VMEM(vec.shape, F32),
            dma((2, PAIR, per)), dma((2, PAIR, per)),
            dma((ny + ns + 2,)), dma((ny + ns + 2,)),
            dma((2,)),
        ],
        compiler_params=comm_params(4),
        cost_estimate=pl.CostEstimate(flops=50_000_000, bytes_accessed=300_000_000, transcendentals=0),
        name="tail",
    )(ga, gb, pa, pb, vec, p, tokens, cot, gain)


def place_kernel(a_ref, b_ref, in_ref, out_ref, dt_ref, *, places, dts, ny):
    for col, size, index, off in places:
        in_ref[:, col : col + size] = a_ref[index + (slice(None), slice(off, off + size))].astype(F32)
    for col, size, index, off in dts:
        dt_ref[:, col : col + size] = a_ref[index + (slice(None), slice(off, off + size))].astype(F32)
    part = b_ref.shape[-1]
    for q in range(PAIR):
        for t in range(2):
            for y in range(ny):
                col = (t * ny + y) * part
                out_ref[q, :, col : col + part] = b_ref[q, y, t].astype(F32)


def run_place(pieces, places, dts, columns, heads, block):
    ny = pieces[0].shape[1]
    rows = pieces[0].shape[3]
    lead = (PAIR, ny, 2)
    width = 2 * ny * pieces[1].shape[4]
    return pl.pallas_call(
        functools.partial(place_kernel, places=places, dts=dts, ny=ny),
        grid=(rows // block,),
        in_specs=[pl.BlockSpec(lead + (block, v.shape[4]), lambda i: (0, 0, 0, i, 0)) for v in pieces],
        out_specs=[
            pl.BlockSpec((block, columns), lambda i: (i, 0)),
            pl.BlockSpec((PAIR, block, width), lambda i: (0, i, 0)),
            pl.BlockSpec((block, heads), lambda i: (i, 0)),
        ],
        out_shape=[
            jax.ShapeDtypeStruct((rows, columns), F32),
            jax.ShapeDtypeStruct((PAIR, rows, width), F32),
            jax.ShapeDtypeStruct((rows, heads), F32),
        ],
        compiler_params=PARAMS,
        cost_estimate=pl.CostEstimate(flops=1_000_000, bytes_accessed=25_000_000, transcendentals=0),
        name="place",
    )(*pieces)


def smalls_kernel(z_ref, v_ref, conv_ref, heads_ref, pre_ref, out_ref, full, *, taps, ns, mine_w, states2, heads, width):
    half = ns // 2
    cw = mine_w // half
    unit = heads // ns // PAIR
    gbc, gh = mine_w, mine_w + states2
    spread = head_map(mine_w, 2 * mine_w * PAIR // heads)
    shared = v_ref[0, 0] + v_ref[0, 1] + v_ref[1, 0] + v_ref[1, 1]
    full[:, 2 * PAIR * mine_w :] = shared[:8, gbc : gbc + states2]
    for t in range(2):
        for q in range(PAIR):
            for k in range(half):
                col = ((t * half + k) * PAIR + q) * cw
                full[:, col : col + cw] = v_ref[t, q, :8, k * cw : (k + 1) * cw]
    channels = (2 * PAIR * mine_w + states2) // ns
    inner = 2 * PAIR * mine_w // ns
    part = width // ns
    wide = v_ref.shape[3]
    skips = []
    for t in range(2):
        skips.append([])
        for q in range(PAIR):
            row = v_ref[t, q, taps + 1 : taps + 2, :mine_w]
            high = row.astype(BF)
            rest = row - high.astype(F32)
            mid = rest.astype(BF)
            rows8 = lambda v: jnp.broadcast_to(v, (8, mine_w))
            skips[t].append((mm_t(rows8(high), spread) + mm_t(rows8(mid), spread) + mm_t(rows8(rest - mid.astype(F32)), spread))[0:1])
    heads_ref[...] = jnp.zeros_like(heads_ref)
    for at in range(ns):
        @pl.when(z_ref[0] == at)
        def _():
            conv_ref[...] = full[:, at * channels : (at + 1) * channels]
            out_ref[...] = full[taps + 2 : taps + 3, at * inner : (at + 1) * inner]
            t, k = at // half, at % half
            for q in range(PAIR):
                span = slice(gh + k * unit, gh + (k + 1) * unit)
                put = slice(q * unit, (q + 1) * unit)
                heads_ref[0:1, put] = v_ref[t, q, 0:1, span]
                heads_ref[1:2, put] = v_ref[t, q, 1:2, span]
                heads_ref[2:3, put] = skips[t][q][:, k * unit : (k + 1) * unit]
            for row in range(-(-width // wide)):
                low, high = max(at * part, row * wide), min((at + 1) * part, (row + 1) * wide)
                if low < high:
                    pre_ref[:, low - at * part : high - at * part] = shared[8 + row : 9 + row, low - row * wide : high - row * wide]


def run_smalls(z, v, taps, ns, mine_w, states2, heads, width):
    channels = (2 * PAIR * mine_w + states2) // ns
    whole = lambda *dims: pl.BlockSpec(dims, lambda i, z: (0,) * len(dims))
    return pl.pallas_call(
        functools.partial(smalls_kernel, taps=taps, ns=ns, mine_w=mine_w, states2=states2, heads=heads, width=width),
        grid_spec=pltpu.PrefetchScalarGridSpec(
            num_scalar_prefetch=1,
            grid=(1,),
            in_specs=[whole(*v.shape)],
            out_specs=[whole(8, channels), whole(8, LANES), whole(1, width // ns), whole(1, 2 * PAIR * mine_w // ns)],
            scratch_shapes=[pltpu.VMEM((8, channels * ns), F32)],
        ),
        out_shape=[
            jax.ShapeDtypeStruct((8, channels), F32),
            jax.ShapeDtypeStruct((8, LANES), F32),
            jax.ShapeDtypeStruct((1, width // ns), F32),
            jax.ShapeDtypeStruct((1, 2 * PAIR * mine_w // ns), F32),
        ],
        compiler_params=PARAMS,
        cost_estimate=pl.CostEstimate(flops=1_000_000, bytes_accessed=1_000_000, transcendentals=0),
        name="smalls",
    )(z, v)


def dot(a, b):
    return jnp.dot(a, b, preferred_element_type=F32)


def pick(index, options):
    result = options[-1]
    for place in reversed(range(len(options) - 1)):
        result = jnp.where(index == place, options[place], result)
    return result


def ordered(index, own, other, axis):
    return jnp.stack([pick(index, (own, other)), pick(index, (other, own))], axis=axis)


def joined(index, own, other, axis):
    return jnp.concatenate([pick(index, (own, other)), pick(index, (other, own))], axis=axis)


def on_device(boundary, lengths, in_proj, dt_proj, out_proj, conv_weight, conv_bias, dt_bias, a_log, d_skip, pre_gain, out_gain):
    ns = lax.axis_size("shard")
    nr = lax.axis_size("rep")
    ny = nr // PAIR
    s = lax.axis_index("section")
    z = lax.axis_index("shard")
    rep = lax.axis_index("rep")
    xb = rep % PAIR
    yb = rep // PAIR

    def swap(v):
        return lax.ppermute(v, "section", [(0, 1), (1, 0)])

    def x_swap(v):
        return lax.ppermute(v, "rep", [(i, i ^ 1) for i in range(nr)])

    def y_send(v, k):
        return lax.ppermute(v, "rep", [(i, (i // PAIR + k) % ny * PAIR + i % PAIR) for i in range(nr)])

    micro, seq_len, width = boundary.shape[1], boundary.shape[3], boundary.shape[4]
    inner = out_proj.shape[1] * ns
    heads = dt_bias.shape[1] * ns
    taps, channels = conv_weight.shape[1], conv_weight.shape[2] * ns
    states2 = channels - inner
    cw = inner // ns // PAIR
    half = ns // 2
    mine_w = half * cw
    mine_h = heads // (2 * PAIR)
    part_w = 2 * mine_w // ny

    def column_chunks(v, first):
        out = []
        for t in range(2):
            for shard in range(t * half, (t + 1) * half):
                start = first + shard * PAIR * cw
                out.append(pick(xb, tuple(v[:, start + q * cw : start + (q + 1) * cw] for q in range(PAIR))))
        return [jnp.concatenate(out[:half], axis=1), jnp.concatenate(out[half:], axis=1)]

    own_in = in_proj[0]
    q_own = []
    for a, b in zip(column_chunks(own_in, 0), column_chunks(own_in, inner)):
        if ny == 2:
            q_own += [a, b]
        else:
            q_own += [v[:, k * part_w : (k + 1) * part_w] for v in (a, b) for k in range(ny // 2)]
    q_own = jnp.stack(q_own).reshape(2, ny, width // ns, part_w)
    own_out = out_proj[0]
    o_own = pick(xb, (own_out[:cw], own_out[cw : 2 * cw])).reshape(ny, cw // ny, width)

    flat = lambda v: v.reshape(-1, v.shape[-1])
    smalls_own = tuple(flat(v) for v in (conv_weight, conv_bias, dt_bias, a_log, d_skip, pre_gain, out_gain))
    counts = jnp.broadcast_to(lengths.astype(F32), (micro, LANES))
    tokens, normed0, g_out1, live8, px, pbc, ph, gains, w_bcdt, in0, out0 = run_start(
        boundary[0, :, 0], counts, smalls_own, own_in[:, 2 * inner :], dt_proj[0], q_own, o_own, heads
    )
    smalls = [(px[b], pbc[b], ph[b]) for b in range(2)]
    unit_h = heads // ns // PAIR
    w_in, w_out = [in0.reshape(ny, width, part_w)], [out0.reshape(mine_w, width)]
    seqs = PAIR * micro

    def by_seq(v):
        return v.reshape((seqs, seq_len) + v.shape[1:])

    def of_own(v):
        return pick(xb, (v[0], v[1]))

    chunks = seq_len // CHUNK

    def forward(b, normed, dmix):
        normed = normed.reshape(seqs * seq_len, width)
        proj = [dot(normed, w_in[b][j]).astype(BF) for j in range(ny)]
        if ny > 2:
            proj = [jnp.concatenate(proj[: ny // 2], axis=1), jnp.concatenate(proj[ny // 2 :], axis=1)]
        gate, x = by_seq(proj[0]), by_seq(proj[1])
        bcdt = by_seq(dot(normed, w_bcdt[b]))
        gg, y, state, *sums = run_forward(smalls[b], gate, x, bcdt, dmix, taps, mine_h)
        gg = gg.reshape(seqs * seq_len, mine_w)
        part = by_seq(dot(gg, w_out[b]).astype(BF))
        return part, sums, (normed, gate, x, bcdt, gg, y, state)

    def mixed_back(b, g_out):
        dmix = lax.dot_general(g_out, w_out[b], (((1,), (1,)), ((), ())), preferred_element_type=F32)
        return by_seq(dmix.astype(BF))

    part0, sums, stored0 = forward(0, normed0, None)
    hidden, normed, r0, gained0, in1, out1 = run_onward(
        part0, tokens, sums[0].reshape(seqs * chunks, LANES), live8, gains[1], q_own, o_own, float(inner), ns
    )
    w_in.append(in1.reshape(ny, width, part_w))
    w_out.append(out1.reshape(mine_w, width))
    g_out1 = g_out1.reshape(seqs * seq_len, width)
    dmix1 = mixed_back(1, g_out1)
    part1, sums, stored1 = forward(1, normed, dmix1)
    both_sums = run_sums(jnp.concatenate([v.reshape(seqs * chunks, LANES) for v in sums]), 3)
    r1 = lax.rsqrt(both_sums[: seqs * chunks] / inner + EPSILON)

    def backward(b, dmix, stored, r, coef):
        normed, gate, x, bcdt, _, y, state = stored
        scalars = jnp.concatenate([r.reshape(seqs, chunks, LANES), coef.reshape(seqs, chunks, LANES)], axis=1)
        dgate, dx, dbcdt, gsmall = run_backward(smalls[b], gate, x, bcdt, y, state, dmix, scalars, taps, mine_h)
        flat = lambda v: v.reshape(seqs * seq_len, v.shape[-1])
        dgate, dx, dbcdt = flat(dgate), flat(dx), flat(dbcdt)
        if ny == 2:
            dparts = [dgate, dx]
        else:
            dparts = [v[:, k * part_w : (k + 1) * part_w] for v in (dgate, dx) for k in range(ny // 2)]
        against = lambda a, w: lax.dot_general(a, w, (((1,), (1,)), ((), ())), preferred_element_type=F32)
        d_normed = against(dbcdt, w_bcdt[b])
        for j in range(ny):
            d_normed = d_normed + against(dparts[j], w_in[b][j])
        gpre = jnp.sum(d_normed * normed.astype(F32), axis=0) / gains[b, 0]
        across = lambda a, c: lax.dot_general(a, c, (((0,), (0,)), ((), ())), preferred_element_type=F32)

        dbc = dbcdt[:, :states2]
        cols = [dbc[:, : states2 // 2], dbc[:, states2 // 2 :]]
        total = (pick(s, cols).astype(F32) + swap(pick(s, cols[::-1])).astype(F32)).astype(BF)
        cols = [total[:, : states2 // 4], total[:, states2 // 4 :]]
        total = (pick(xb, cols).astype(F32) + x_swap(pick(xb, cols[::-1])).astype(F32)).astype(BF)
        mine = jnp.concatenate([total, dbcdt[:, states2 : states2 + states2 // 4]], axis=1)
        grad_in = [across(normed, jnp.concatenate([v, mine], axis=1)).astype(BF) for v in dparts]
        grad_in = [v.reshape(ns, width // ns, -1) for v in grad_in]
        wide = gsmall.shape[1]
        gpre = jnp.pad(gpre, (0, 8 * wide - width)).reshape(8, wide)
        return by_seq(d_normed.astype(BF)), grad_in, jnp.concatenate([gsmall, gpre])

    def z_sum(v):
        parts = [v[j] for j in range(ns)]
        total = pick(z, parts).astype(F32)
        for k in range(1, ns):
            send = lax.dynamic_index_in_dim(v, (z + k) % ns, 0, False)
            got = lax.ppermute(send, "shard", [(i, (i + k) % ns) for i in range(ns)])
            total = total + got.astype(F32)
        return total.astype(BF)

    def out_chip(g_out, gg, r):
        g_scaled = (g_out.astype(F32) * r.reshape(-1, 1)).astype(BF)
        across = lambda a, c: lax.dot_general(a, c, (((0,), (0,)), ((), ())), preferred_element_type=F32)
        grad = across(gg, g_scaled).astype(BF)
        cols = [grad[:, : width // 2], grad[:, width // 2 :]]
        send = pick(s, cols[::-1])
        got = swap(send)
        return joined(s, pick(s, cols), got, 0)

    def out_grad(v):
        step = width // 2 // ny
        parts = [v[:, j * step : (j + 1) * step] for j in range(ny)]
        total = pick(yb, parts).astype(F32)
        for k in range(1, ny):
            send = pick((yb + k) % ny, parts)
            got = y_send(send, k)
            total = total + got.astype(F32)
        return total.astype(BF).reshape(ns, cw, -1)

    v1 = out_chip(g_out1, stored1[4], r1)
    gout1 = out_grad(v1)
    d_normed1, gin1, gsmall1 = backward(1, dmix1, stored1, r1, r1 * r1 * r1 * both_sums[seqs * chunks :] / inner)
    piece_b1 = z_sum(gout1)
    d_normed1, *gin1 = lax.optimization_barrier((d_normed1, *gin1))
    total1 = pick(yb, gin1).astype(F32)
    for k in range(1, ny):
        send = pick((yb + k) % ny, gin1)
        got = y_send(send, k)
        total1 = total1 + got.astype(F32)
    total1 = total1.astype(BF)
    cot0, g_out0, dots0 = run_back(d_normed1, hidden, tokens, gained0, live8, gains[1])

    g_out0 = g_out0.reshape(-1, width)
    dmix0 = mixed_back(0, g_out0)
    v0 = out_chip(g_out0, stored0[4], r0)
    dmix0, total1 = lax.optimization_barrier((dmix0, total1))
    gout0 = out_grad(v0)
    piece_a1 = z_sum(total1)

    part1 = part1.reshape(PAIR, micro, seq_len, width)
    mine = pick(s, (part1[:, 0], part1[:, 1])).astype(F32) + swap(pick(s, (part1[:, 1], part1[:, 0]))).astype(F32)
    mine = mine.astype(BF)
    send = of_own(mine[::-1])
    got = x_swap(send)
    mine = of_own(mine).astype(F32) + got.astype(F32)
    own_hidden = of_own(hidden.reshape(PAIR, micro, seq_len, width))
    scale = of_own((live8 * r1).reshape(PAIR, micro, seq_len, 1))
    final = (pick(s, (own_hidden[0], own_hidden[1])).astype(F32) + pick(s, (scale[0], scale[1])) * mine).astype(BF)
    final = ordered(s, final, swap(final), 0)

    d_normed0, gin0, gsmall0 = backward(0, dmix0, stored0, r0, r0 * r0 * dots0 / inner)
    *pieces, vec, res = run_tail(
        jnp.stack(gin0), gout0, piece_a1, piece_b1, jnp.stack([gsmall0, gsmall1]), d_normed0, tokens, cot0, gains[0]
    )
    activations = pick(s, (own_hidden, final))
    input_grads = pick(s, (res, of_own(cot0.reshape(PAIR, micro, seq_len, width))))
    places, dts = [], []
    col = 0
    for plane in range(2):
        for t in range(2):
            for k in range(half):
                for q in range(PAIR):
                    y_at, off = divmod(plane * mine_w + k * cw, part_w)
                    places.append((col, cw, (q, y_at, t), off))
                    col += cw
    quad = states2 // 4
    for t in range(2):
        for q in range(PAIR):
            places.append((col, quad, (q, 0, t), part_w))
            col += quad
    for t in range(2):
        for k in range(half):
            for q in range(PAIR):
                dts.append((((t * half + k) * PAIR + q) * unit_h, unit_h, (q, 0, t), part_w + quad + k * unit_h))
    grad_in, grad_out, grad_dt = run_place(pieces, tuple(places), tuple(dts), col, heads, 64)
    grad_out = grad_out.reshape(PAIR * cw, width)
    g_conv, g_heads, g_pre, g_og = run_smalls(z[None], vec, taps, ns, mine_w, states2, heads, width)
    g_cw, g_cb = g_conv[:taps], g_conv[taps]
    g_dtb, g_alg, g_dsk = (g_heads[i, : heads // ns] for i in range(3))
    g_pre, g_og = g_pre[0], g_og[0]

    return (
        activations[None, :, None],
        input_grads[None, :, None],
        grad_in[None],
        grad_dt[None],
        grad_out[None],
        g_cw[None],
        g_cb[None],
        g_dtb[None],
        g_alg[None],
        g_dsk[None],
        g_pre[None],
        g_og[None],
    )


def solution(mesh):
    shard1 = P("section", "shard")
    shard2 = P("section", "shard", None)
    tokens = P("section", None, ("shard", "rep"), None, None)
    taps = P("section", None, "shard")
    weights = (shard2, shard2, shard2, taps, shard1, shard1, shard1, shard1, shard1, shard1)
    return jax.shard_map(
        on_device,
        mesh=mesh,
        in_specs=(tokens, P(None, ("shard", "rep"))) + weights,
        out_specs=(tokens, tokens) + weights,
        check_vma=False,
    )
```

```python
import functools

import jax
import jax.numpy as jnp
from jax import lax
from jax.experimental import pallas as pl
from jax.experimental.pallas import tpu as pltpu
from jax.sharding import PartitionSpec as P


BF = jnp.bfloat16
F32 = jnp.float32
HIGH = lax.Precision.HIGHEST
EPSILON = 1e-05
CHUNK = 128
LANES = 128
PAIR = 2


def mm(a, b):
    return jnp.dot(a.astype(BF), b.astype(BF), preferred_element_type=F32)


def mm_t(a, b):
    return lax.dot_general(a.astype(BF), b.astype(BF), (((1,), (1,)), ((), ())), preferred_element_type=F32)


def t_mm(a, b):
    return lax.dot_general(a.astype(BF), b.astype(BF), (((0,), (0,)), ((), ())), preferred_element_type=F32)


def rows_of(shape):
    return lax.broadcasted_iota(jnp.int32, shape, 0)


def lanes_of(shape):
    return lax.broadcasted_iota(jnp.int32, shape, 1)


def shift_down(v, steps):
    return jnp.where(rows_of(v.shape) >= steps, pltpu.roll(v, steps, 0), 0.0)


def shift_up(v, steps):
    size = v.shape[0]
    return jnp.where(rows_of(v.shape) < size - steps, pltpu.roll(v, size - steps, 0), 0.0)


def conv(v, taps_ref, taps):
    total = taps_ref[taps : taps + 1, :] + taps_ref[taps - 1 : taps, :] * v
    for k in range(taps - 1):
        total = total + taps_ref[k : k + 1, :] * shift_down(v, taps - 1 - k)
    return total


def conv_back(d_sum, v, taps_ref, taps):
    d_v = taps_ref[taps - 1 : taps, :] * d_sum
    d_taps = []
    for k in range(taps - 1):
        d_v = d_v + taps_ref[k : k + 1, :] * shift_up(d_sum, taps - 1 - k)
        d_taps.append(jnp.sum(d_sum * shift_down(v, taps - 1 - k), axis=0, keepdims=True))
    d_taps.append(jnp.sum(d_sum * v, axis=0, keepdims=True))
    d_taps.append(jnp.sum(d_sum, axis=0, keepdims=True))
    return d_v, d_taps


def head_map(width, head_dim):
    shape = (LANES, width)
    return (rows_of(shape) == lanes_of(shape) // head_dim).astype(BF)


def expand(v, spread):
    high = v.astype(BF)
    low = (v - high.astype(F32)).astype(BF)
    return mm(high, spread) + mm(low, spread)


def step_of(dt, ph_ref):
    pre = dt + ph_ref[0:1, :]
    step = jnp.maximum(pre, 0.0) + jnp.log1p(jnp.exp(-jnp.abs(pre)))
    rate = -jnp.exp(ph_ref[1:2, :])
    return pre, step, rate


def lower_mask():
    shape = (CHUNK, CHUNK)
    return rows_of(shape) >= lanes_of(shape)


def pair_rows(v, first):
    return jnp.concatenate([jnp.where(first, v, 0.0), jnp.where(first, 0.0, v)], axis=0)


def as_row(column):
    return jnp.broadcast_to(column, (CHUNK, LANES)).T[0:1, :]


def as_column(row):
    return jnp.broadcast_to(row, (CHUNK, LANES)).T[:, 0:1]


def forward_kernel(px_ref, pbc_ref, ph_ref, gate_ref, x_ref, bcdt_ref, *refs, taps, heads, with_dots):
    if with_dots:
        dmix_ref, gg_ref, y_ref, st_ref, ss_ref, dot_ref = refs
    else:
        gg_ref, y_ref, st_ref, ss_ref = refs
    width = x_ref.shape[1]
    head_dim = width // heads
    states = pbc_ref.shape[1] // 2
    spread = head_map(width, head_dim)
    bcdt = bcdt_ref[...].astype(F32)
    sums = conv(bcdt[:, : 2 * states], pbc_ref, taps)
    bc = sums * jax.nn.sigmoid(sums)
    _, step, rate = step_of(bcdt[:, 2 * states :], ph_ref)
    decay = rate * step
    sums = conv(x_ref[...].astype(F32), px_ref, taps)
    act = sums * jax.nn.sigmoid(sums)
    xs = act * expand(step, spread)
    lower = lower_mask()
    tri = lower.astype(F32)
    first = lanes_of((CHUNK, 2 * head_dim)) < head_dim
    state = None
    chunks = x_ref.shape[0] // CHUNK
    for c in range(chunks):
        span = slice(c * CHUNK, (c + 1) * CHUNK)
        cum = jnp.dot(tri, decay[span], precision=HIGH, preferred_element_type=F32)
        cum_t = cum.T
        b_c = bc[span, :states].astype(BF)
        c_c = bc[span, states:].astype(BF)
        scores = mm_t(c_c, b_c)
        xs_c = xs[span]
        pieces = []
        for p in range(heads // 2):
            two = slice(p * 2 * head_dim, (p + 1) * 2 * head_dim)
            mixes = []
            for h in (2 * p, 2 * p + 1):
                gap = jnp.minimum(cum[:, h : h + 1] - cum_t[h : h + 1, :], 0.0)
                mixes.append(jnp.where(lower, jnp.exp(gap) * scores, 0.0).astype(BF))
            pieces.append(mm(jnp.concatenate(mixes, axis=1), pair_rows(xs_c[:, two], first)))
        y = jnp.concatenate(pieces, axis=1)
        if c > 0:
            y = y + mm(c_c, state) * expand(jnp.exp(cum), spread)
        if c + 1 < chunks:
            last = cum[CHUNK - 1 : CHUNK, :]
            fresh = t_mm(b_c, xs_c * expand(jnp.exp(last - cum), spread))
            state = fresh if c == 0 else fresh + state * expand(jnp.exp(jnp.broadcast_to(last, (states, LANES))), spread)
            st_ref[c] = state
        y = y + px_ref[taps + 1 : taps + 2, :] * act[span]
        y_low = y.astype(BF)
        y_ref[span, :] = y_low
        y = y_low.astype(F32)
        gate = gate_ref[span, :].astype(F32)
        gated = y * (gate * jax.nn.sigmoid(gate))
        ss_ref[c : c + 1, :] = as_row(jnp.sum(gated * gated, axis=1, keepdims=True))
        gg = gated * px_ref[taps + 2 : taps + 3, :]
        gg_ref[span, :] = gg.astype(BF)
        if with_dots:
            dot_ref[c : c + 1, :] = as_row(jnp.sum(gg * dmix_ref[span, :].astype(F32), axis=1, keepdims=True))


def backward_kernel(
    px_ref, pbc_ref, ph_ref, gate_ref, x_ref, bcdt_ref, y_ref, st_ref, dmix_ref, sc_ref,
    dgate_ref, dx_ref, dbcdt_ref, small_ref, *, taps, heads,
):
    length, width = x_ref.shape
    head_dim = width // heads
    states = pbc_ref.shape[1] // 2
    spread = head_map(width, head_dim)

    @pl.when(pl.program_id(0) == 0)
    def _():
        small_ref[...] = jnp.zeros_like(small_ref)

    gx_ref = small_ref.at[:, :width]
    gbc_ref = small_ref.at[:, width : width + 2 * states]
    gh_ref = small_ref.at[:, width + 2 * states :]

    gate = gate_ref[...].astype(F32)
    y = y_ref[...].astype(F32)
    dmix = dmix_ref[...].astype(F32)
    chunks = length // CHUNK
    r = jnp.concatenate([as_column(sc_ref[c : c + 1, :]) for c in range(chunks)], axis=0)
    coef = jnp.concatenate([as_column(sc_ref[chunks + c : chunks + c + 1, :]) for c in range(chunks)], axis=0)
    sig = jax.nn.sigmoid(gate)
    gated = y * gate * sig
    gx_ref[taps + 2 : taps + 3, :] += jnp.sum(dmix * gated * r, axis=0, keepdims=True)
    dgated = r * px_ref[taps + 2 : taps + 3, :] * dmix - coef * gated
    dgate_ref[...] = (dgated * y * (sig * (1.0 + gate * (1.0 - sig)))).astype(BF)
    dy = dgated * gate * sig

    bcdt = bcdt_ref[...].astype(F32)
    bc_in = bcdt[:, : 2 * states]
    bc_sum = conv(bc_in, pbc_ref, taps)
    bc_sig = jax.nn.sigmoid(bc_sum)
    bc = bc_sum * bc_sig
    pre, step, rate = step_of(bcdt[:, 2 * states :], ph_ref)
    decay = rate * step
    x_in = x_ref[...].astype(F32)
    x_sum = conv(x_in, px_ref, taps)
    x_sig = jax.nn.sigmoid(x_sum)
    act = x_sum * x_sig
    step_wide = expand(step, spread)
    xs = act * step_wide
    gx_ref[taps + 1 : taps + 2, :] += jnp.sum(dy * act, axis=0, keepdims=True)

    lower = lower_mask()
    tri = lower.astype(F32)
    upper = (rows_of((CHUNK, CHUNK)) <= lanes_of((CHUNK, CHUNK))).astype(F32)
    last_row = rows_of((CHUNK, LANES)) == CHUNK - 1
    head_lane = lanes_of((CHUNK, LANES))
    head_row = rows_of((LANES, CHUNK))
    first = lanes_of((CHUNK, 2 * head_dim)) < head_dim
    d_state = None
    d_xs, d_bc, d_decay = [None] * chunks, [None] * chunks, [None] * chunks
    for c in reversed(range(chunks)):
        span = slice(c * CHUNK, (c + 1) * CHUNK)
        cum = jnp.dot(tri, decay[span], precision=HIGH, preferred_element_type=F32)
        cum_t = cum.T
        b_c = bc[span, :states].astype(BF)
        c_c = bc[span, states:].astype(BF)
        xs_c = xs[span]
        dy_c = dy[span]
        scores = mm_t(c_c, b_c)
        d_scores = jnp.zeros((CHUNK, CHUNK), F32)
        by_row = jnp.zeros((CHUNK, LANES), F32)
        by_col = jnp.zeros((LANES, CHUNK), F32)
        pieces = []
        for p in range(heads // 2):
            two = slice(p * 2 * head_dim, (p + 1) * 2 * head_dim)
            dy_two = pair_rows(dy_c[:, two], first).astype(BF)
            d_mix = mm_t(dy_two, xs_c[:, two])
            mixes = []
            for i, h in enumerate((2 * p, 2 * p + 1)):
                gap = jnp.minimum(cum[:, h : h + 1] - cum_t[h : h + 1, :], 0.0)
                fall = jnp.where(lower, jnp.exp(gap), 0.0)
                mixes.append((fall * scores).astype(BF))
                d_fall = d_mix[i * CHUNK : (i + 1) * CHUNK] * fall
                d_scores = d_scores + d_fall
                both = d_fall * scores
                by_row = jnp.where(head_lane == h, jnp.sum(both, axis=1, keepdims=True), by_row)
                by_col = jnp.where(head_row == h, jnp.sum(both, axis=0, keepdims=True), by_col)
            pieces.append(t_mm(jnp.concatenate(mixes, axis=0), dy_two))
        d_xs_c = jnp.concatenate(pieces, axis=1)
        d_c = mm(d_scores, b_c)
        d_b = t_mm(d_scores, c_c)
        d_cum = by_row - by_col.T
        new_state = None
        if c > 0:
            before = st_ref[c - 1]
            grow = expand(jnp.exp(cum), spread)
            d_off = dy_c * grow
            new_state = t_mm(c_c, d_off)
            d_c = d_c + mm_t(d_off, before)
            d_cum = d_cum + mm_t(d_off * mm(c_c, before), spread)
        if c + 1 < chunks:
            last = cum[CHUNK - 1 : CHUNK, :]
            tail = expand(jnp.exp(last - cum), spread)
            tailed = xs_c * tail
            d_tailed = mm(b_c, d_state)
            d_b = d_b + mm_t(tailed, d_state)
            d_xs_c = d_xs_c + d_tailed * tail
            lost = mm_t(d_tailed * tailed, spread)
            d_last = jnp.sum(lost, axis=0, keepdims=True)
            if c > 0:
                whole = expand(jnp.exp(jnp.broadcast_to(last, (states, LANES))), spread)
                d_last = d_last + jnp.sum(mm_t(d_state * before * whole, spread), axis=0, keepdims=True)
                new_state = new_state + d_state * whole
            d_cum = d_cum - lost + jnp.where(last_row, d_last, 0.0)
        d_state = new_state
        d_xs[c] = d_xs_c
        d_bc[c] = jnp.concatenate([d_b, d_c], axis=1)
        d_decay[c] = jnp.dot(upper, d_cum, precision=HIGH, preferred_element_type=F32)
    d_xs = jnp.concatenate(d_xs, axis=0)
    d_bc = jnp.concatenate(d_bc, axis=0)
    d_decay = jnp.concatenate(d_decay, axis=0)

    d_step = mm_t(act * d_xs, spread) + d_decay * rate
    gh_ref[1:2, :] += jnp.sum(d_decay * decay, axis=0, keepdims=True)
    d_dt = d_step * jax.nn.sigmoid(pre)
    gh_ref[0:1, :] += jnp.sum(d_dt, axis=0, keepdims=True)

    d_act = dy * px_ref[taps + 1 : taps + 2, :] + d_xs * step_wide
    d_sum = d_act * (x_sig * (1.0 + x_sum * (1.0 - x_sig)))
    d_x, d_taps = conv_back(d_sum, x_in, px_ref, taps)
    dx_ref[...] = d_x.astype(BF)
    for k, value in enumerate(d_taps):
        gx_ref[k : k + 1, :] += value
    d_sum = d_bc * (bc_sig * (1.0 + bc_sum * (1.0 - bc_sig)))
    d_bc_in, d_taps = conv_back(d_sum, bc_in, pbc_ref, taps)
    for k, value in enumerate(d_taps):
        gbc_ref[k : k + 1, :] += value
    dbcdt_ref[:, : 2 * states] = d_bc_in.astype(BF)
    dbcdt_ref[:, 2 * states :] = d_dt.astype(BF)


def per_seq(*dims):
    return pl.BlockSpec((None,) + dims, lambda i: (i,) + (0,) * len(dims))


def fixed(*dims):
    return pl.BlockSpec(dims, lambda i: (0,) * len(dims))


PARAMS = pltpu.CompilerParams(dimension_semantics=("arbitrary",), vmem_limit_bytes=24 << 20)


def run_forward(small, gate, x, bcdt, dmix, taps, heads):
    px, pbc, ph = small
    seqs, length, width = x.shape
    states = pbc.shape[1] // 2
    chunks = length // CHUNK
    more = [] if dmix is None else [dmix]
    sums = [jax.ShapeDtypeStruct((seqs, chunks, LANES), F32)] * (1 + len(more))
    return pl.pallas_call(
        functools.partial(forward_kernel, taps=taps, heads=heads, with_dots=bool(more)),
        grid=(seqs,),
        in_specs=[fixed(*px.shape), fixed(*pbc.shape), fixed(*ph.shape), per_seq(length, width), per_seq(length, width), per_seq(length, bcdt.shape[2])]
        + [per_seq(length, width)] * len(more),
        out_specs=[per_seq(length, width), per_seq(length, width), per_seq(chunks - 1, states, width)] + [per_seq(chunks, LANES)] * len(sums),
        out_shape=[
            jax.ShapeDtypeStruct((seqs, length, width), BF),
            jax.ShapeDtypeStruct((seqs, length, width), BF),
            jax.ShapeDtypeStruct((seqs, chunks - 1, states, width), F32),
        ]
        + sums,
        compiler_params=PARAMS,
        cost_estimate=pl.CostEstimate(flops=seqs * 400_000_000, bytes_accessed=seqs * 4_000_000, transcendentals=seqs * 2_000_000),
        name="mix_forward",
    )(px, pbc, ph, gate, x, bcdt, *more)


def run_backward(small, gate, x, bcdt, y, state, dmix, scalars, taps, heads):
    px, pbc, ph = small
    seqs, length, width = x.shape
    smalls = px.shape[1] + pbc.shape[1] + ph.shape[1]
    return pl.pallas_call(
        functools.partial(backward_kernel, taps=taps, heads=heads),
        grid=(seqs,),
        in_specs=[
            fixed(*px.shape), fixed(*pbc.shape), fixed(*ph.shape), per_seq(length, width), per_seq(length, width),
            per_seq(length, bcdt.shape[2]), per_seq(length, width), per_seq(*state.shape[1:]), per_seq(length, width), per_seq(*scalars.shape[1:]),
        ],
        out_specs=[per_seq(length, width), per_seq(length, width), per_seq(length, bcdt.shape[2]), fixed(8, smalls)],
        out_shape=[
            jax.ShapeDtypeStruct((seqs, length, width), BF),
            jax.ShapeDtypeStruct((seqs, length, width), BF),
            jax.ShapeDtypeStruct((seqs, length, bcdt.shape[2]), BF),
            jax.ShapeDtypeStruct((8, smalls), F32),
        ],
        compiler_params=PARAMS,
        cost_estimate=pl.CostEstimate(flops=seqs * 1_200_000_000, bytes_accessed=seqs * 6_000_000, transcendentals=seqs * 4_000_000),
        name="mix_backward",
    )(px, pbc, ph, gate, x, bcdt, y, state, dmix, scalars)


MESH = pl.DeviceIdType.MESH
VM = pl.BlockSpec(memory_space=pltpu.VMEM)


def partners():
    section = lax.axis_index("section")
    rep = lax.axis_index("rep")
    xb = rep % PAIR
    return section, xb, {"section": 1 - section}, {"rep": rep + 1 - 2 * xb}


def greet(*devices):
    barrier = pltpu.get_barrier_semaphore()
    for device in devices:
        pl.semaphore_signal(barrier, inc=1, device_id=device, device_id_type=MESH)
    pl.semaphore_wait(barrier, len(devices))


def remote(src, dst, send, recv, device):
    return pltpu.make_async_remote_copy(src_ref=src, dst_ref=dst, send_sem=send, recv_sem=recv, device_id=device, device_id_type=MESH)


def sums_kernel(v_ref, out_ref, got_ref, half_ref, send, recv):
    _, _, peer, beside = partners()
    greet(peer, beside)
    first = remote(v_ref, got_ref.at[0], send.at[0], recv.at[0], peer)
    first.start()
    first.wait()
    half_ref[...] = v_ref[...] + got_ref[0]
    second = remote(half_ref, got_ref.at[1], send.at[1], recv.at[1], beside)
    second.start()
    second.wait()
    out_ref[...] = half_ref[...] + got_ref[1]


def run_sums(v, collective_id):
    return pl.pallas_call(
        sums_kernel,
        in_specs=[VM],
        out_specs=VM,
        out_shape=jax.ShapeDtypeStruct(v.shape, F32),
        scratch_shapes=[pltpu.VMEM((2,) + v.shape, F32), pltpu.VMEM(v.shape, F32), pltpu.SemaphoreType.DMA((2,)), pltpu.SemaphoreType.DMA((2,))],
        compiler_params=pltpu.CompilerParams(collective_id=collective_id, has_side_effects=True),
        cost_estimate=pl.CostEstimate(flops=10_000_000, bytes_accessed=20_000_000, transcendentals=0),
        name="token_sums",
    )(v)


def exchange(part_ref, got_a, held, got_x, send, recv, use):
    section, _, peer, beside = partners()
    per = part_ref.shape[1] // CHUNK
    steps = PAIR * per

    def at(i):
        return i // per, pl.ds(pl.multiple_of(i % per * CHUNK, CHUNK), CHUNK)

    def to_peer(i):
        x, span = at(i)
        return remote(part_ref.at[x * 2 + 1 - section, span], got_a.at[i], send.at[0, i], recv.at[0, i], peer)

    def to_beside(i):
        return remote(held.at[i], got_x.at[i], send.at[1, i], recv.at[1, i], beside)

    def start_peer(i, _):
        to_peer(i).start()
        return 0

    def add(i, _):
        to_peer(i).wait_recv()
        x, span = at(i)
        held[i] = (part_ref[x * 2 + section, span].astype(F32) + got_a[i].astype(F32)).astype(BF)

        @pl.when(i > 0)
        def _():
            to_beside(i - 1).start()

        return 0

    def finish(i):
        to_beside(i).wait_recv()
        x, span = at(i)
        use(i, x, span, held[i].astype(F32) + got_x[i].astype(F32))

    def drain(i, _):
        to_peer(i).wait_send()
        to_beside(i).wait_send()
        return 0

    lax.fori_loop(0, steps, start_peer, 0)
    yield
    lax.fori_loop(0, steps, add, 0)
    yield
    to_beside(steps - 1).start()
    yield
    for i in range(steps):
        finish(i)
        yield
    lax.fori_loop(0, steps, drain, 0)


def weights_flow(b, q_ref, o_ref, w_in, w_out, qs, qr, os_, or_, *, ns, ny, split=False):
    section, xb, peer, _ = partners()
    z = lax.axis_index("shard")
    yb = lax.axis_index("rep") // PAIR
    half = ns // 2
    part = q_ref.shape[2] // PARTS
    home = z // half

    def y_peer(k):
        return {"rep": (yb + k) % ny * PAIR + xb}

    def rows_at(h):
        return pl.ds(h * part, part)

    def there(way):
        return z < ns - 1 if way > 0 else z > 0

    def first(src, way, h):
        return remote(src, w_in.at[yb, z, rows_at(h)], qs.at[0, (way + 1) // 2, h], qr.at[yb, z, h], {"shard": z + way})

    def chip(j, h):
        return remote(q_ref.at[1 - b, j, rows_at(h)], w_in.at[j, z, rows_at(h)], qs.at[1, j, h], qr.at[j, z, h], peer)

    def stay(j, h):
        return pltpu.make_async_copy(q_ref.at[b, j, rows_at(h)], w_in.at[j, z, rows_at(h)], qs.at[2 + ny, j, h])

    def onward(place, way, h):
        block = w_in.at[yb, place, rows_at(h)]
        return remote(block, block, qs.at[2, place, h], qr.at[yb, place, h], {"shard": z + way})

    def across(place, k, h):
        block = w_in.at[yb, place, rows_at(h)]
        return remote(block, block, qs.at[2 + k, place, h], qr.at[yb, place, h], y_peer(k))

    def arrival(j, place, h):
        block = w_in.at[j, place, rows_at(h)]
        return remote(block, block, qs.at[2, place, h], qr.at[j, place, h], peer)

    def o_first(src, way):
        return remote(src, w_out.at[z % half, yb], os_.at[0, (way + 1) // 2], or_.at[z % half, yb], {"shard": z + way})

    def o_chip(j):
        return remote(o_ref.at[j], w_out.at[z % half, j], os_.at[1, j], or_.at[z % half, j], peer)

    def o_stay(j):
        return pltpu.make_async_copy(o_ref.at[j], w_out.at[z % half, j], os_.at[1, j])

    def o_onward(k, way):
        block = w_out.at[k, yb]
        return remote(block, block, os_.at[2, k], or_.at[k, yb], {"shard": z + way})

    def o_across(k, i):
        block = w_out.at[k, yb]
        return remote(block, block, os_.at[2 + i, k], or_.at[k, yb], y_peer(i))

    def o_arrival(k, j):
        block = w_out.at[k, j]
        return remote(block, block, os_.at[2, k], or_.at[k, j], peer)

    def along(copy):
        for way in (1, -1):
            @pl.when(there(way))
            def _():
                copy(way).start()

    def start():
        @pl.when(section == b)
        def _():
            for h in range(PARTS):
                chip(yb, h).start()

            @pl.when(home != b)
            def _():
                o_chip(yb).start()

            for h in range(PARTS):
                along(lambda way: first(q_ref.at[b, yb, rows_at(h)], way, h))

            @pl.when(home == b)
            def _():
                along(lambda way: o_first(o_ref.at[yb], way))

            for k in range(ny):
                j = (yb + k) % ny
                for h in range(PARTS):
                    if k:
                        chip(j, h).start()
                    stay(j, h).start()

                @pl.when(home == b)
                def _():
                    o_stay(j).start()

                if k:
                    @pl.when(home != b)
                    def _():
                        o_chip(j).start()

        @pl.when(section != b)
        def _():
            for h in range(PARTS):
                arrival(yb, z, h).wait_recv()
                along(lambda way: first(w_in.at[yb, z, rows_at(h)], way, h))

            @pl.when(home != b)
            def _():
                o_arrival(z % half, yb).wait_recv()
                along(lambda way: o_first(w_out.at[z % half, yb], way))

    def relay_in(d, h=None):
        for h in range(PARTS) if h is None else (h,):
            for way in (1, -1):
                place = z - way * d

                @pl.when((place >= 0) & (place < ns))
                def _():
                    arrival(yb, place, h).wait_recv()

                    @pl.when(there(way))
                    def _():
                        onward(place, way, h).start()

                    for k in range(1, ny):
                        across(place, k, h).start()

    def relay_out(d):
        for way in (1, -1):
            place = z - way * d
            k = place - section * half

            @pl.when((place >= 0) & (place < ns) & (k >= 0) & (k < half))
            def _():
                o_arrival(k, yb).wait_recv()

                @pl.when(there(way))
                def _():
                    o_onward(k, way).start()

                for i in range(1, ny):
                    o_across(k, i).start()

    def finish_in():
        for place in range(ns):
            @pl.when(place != z)
            def _():
                for h in range(PARTS):
                    for k in range(1, ny):
                        arrival((yb + k) % ny, place, h).wait_recv()
                        across(place, k, h).wait_send()

                    @pl.when(jnp.where(place < z, z < ns - 1, z > 0))
                    def _():
                        onward(place, 1, h).wait_send()

        for way in (1, -1):
            @pl.when(there(way))
            def _():
                for h in range(PARTS):
                    first(w_in.at[yb, z, rows_at(h)], way, h).wait_send()

        @pl.when(section != b)
        def _():
            for k in range(1, ny):
                for h in range(PARTS):
                    arrival((yb + k) % ny, z, h).wait_recv()

        @pl.when(section == b)
        def _():
            for j in range(ny):
                for h in range(PARTS):
                    chip(j, h).wait_send()
                    stay(j, h).wait()

    def finish_out():
        @pl.when((section != b) & (home != b))
        def _():
            for k in range(1, ny):
                o_arrival(z % half, (yb + k) % ny).wait_recv()

        @pl.when(section == home)
        def _():
            for way in (1, -1):
                @pl.when(there(way))
                def _():
                    o_first(w_out.at[z % half, yb], way).wait_send()

        for k in range(half):
            place = section * half + k

            @pl.when(place != z)
            def _():
                for i in range(1, ny):
                    o_arrival(k, (yb + i) % ny).wait_recv()
                    o_across(k, i).wait_send()

                @pl.when(jnp.where(place < z, z < ns - 1, z > 0))
                def _():
                    o_onward(k, 1).wait_send()

        @pl.when(section == b)
        def _():
            for j in range(ny):
                @pl.when(home == b)
                def _():
                    o_stay(j).wait()

                @pl.when(home != b)
                def _():
                    o_chip(j).wait_send()

    def relay(d):
        relay_in(d)
        relay_out(d)

    def finish():
        finish_in()
        finish_out()

    if split:
        return start, relay_in, relay_out, finish
    return start, relay, finish


def weights_shapes(q, o, ns):
    ny = q.shape[1]
    outs = [
        jax.ShapeDtypeStruct((ny, ns) + q.shape[2:], BF),
        jax.ShapeDtypeStruct((ns // 2,) + o.shape, BF),
    ]
    dma = pltpu.SemaphoreType.DMA
    sems = [dma((3 + ny, max(ns, 4), PARTS)), dma((ny, ns, PARTS)), dma((2 + ny, max(ns, 2))), dma((ns // 2, ny))]
    return outs, sems


def greet_line(ns, ny):
    section, xb, peer, beside = partners()
    z = lax.axis_index("shard")
    yb = lax.axis_index("rep") // PAIR
    found = [peer, beside] + [{"rep": (yb + k) % ny * PAIR + xb} for k in range(1, ny)]
    for k in (1, ns - 1):
        found += [{"shard": (z + k) % ns}, {"section": 1 - section, "shard": (z + k) % ns}]
    greet(*found)


def start_kernel(tokens_ref, counts_ref, cw_ref, cb_ref, dtb_ref, alg_ref, dsk_ref, pgn_ref, ogn_ref, bc_ref, dt_ref, q_ref, o_ref,
                 all_tokens, normed_ref, live_out_ref, live_ref, px_ref, pbc_ref, ph_ref, gain_ref, wbc_ref, w_in, w_out,
                 small, all_small, mine, packs, full, row8, all_counts,
                 qs, qr, os_, or_, ts, tr, ss, sr, ps, pr, cs, cr, *, ns, ny, taps, heads):
    section, xb, peer, beside = partners()
    z = lax.axis_index("shard")
    yb = lax.axis_index("rep") // PAIR
    half = ns // 2
    greet_all(ns, ny)
    start, relay, finish = weights_flow(0, q_ref, o_ref, w_in, w_out, qs, qr, os_, or_, ns=ns, ny=ny)

    part = cw_ref.shape[1]
    mine[...] = jnp.zeros_like(mine)
    unit3 = LANES
    mine[0:taps, :part] = cw_ref[...].astype(F32)
    mine[taps : taps + 1, :part] = cb_ref[...].astype(F32)
    for i, ref in enumerate((pgn_ref, ogn_ref)):
        mine[taps + 1 + i : taps + 2 + i, : ref.shape[1]] = ref[...].astype(F32)
    for i, ref in enumerate((dtb_ref, alg_ref, dsk_ref)):
        mine[taps + 3 : taps + 4, i * unit3 : i * unit3 + ref.shape[1]] = ref[...].astype(F32)

    def pack_to(k):
        return remote(mine, packs.at[section, z], ps.at[0, k], pr.at[section, z], {"shard": (z + k) % ns})

    def pack_chip(place):
        return remote(packs.at[section, place], packs.at[section, place], ps.at[1, place], pr.at[section, place], peer)

    def pack_from(t, place):
        return remote(mine, packs.at[t, place], ps.at[0, 0], pr.at[t, place], peer)

    counts = remote(counts_ref, all_counts.at[xb], cs, cr, beside)
    counts.start()
    for k in range(1, ns):
        pack_to(k).start()
    remote(mine, packs.at[section, z], ps.at[0, 0], pr.at[section, z], peer).start()
    packs[section, z] = mine[...]
    all_counts[xb] = counts_ref[...]

    def there(way):
        return z < ns - 1 if way > 0 else z > 0

    lanes = bc_ref.shape[1]
    rows = bc_ref.shape[0] // ny
    for j in range(ny):
        small[j] = jnp.zeros_like(small[j])
        small[j, :, :lanes] = bc_ref[j * rows : (j + 1) * rows]
        small[j, :, lanes : lanes + heads] = dt_ref[j * rows : (j + 1) * rows]

    def first(way):
        return remote(small.at[yb], all_small.at[section, z, yb], ss.at[0, (way + 1) // 2, 0], sr.at[section, z, yb], {"shard": z + way})

    def held(place, j):
        return all_small.at[section, place, j]

    def onward(place, way):
        return remote(held(place, yb), held(place, yb), ss.at[1, place, 0], sr.at[section, place, yb], {"shard": z + way})

    def across(place, k):
        return remote(held(place, yb), held(place, yb), ss.at[1 + k, place, 0], sr.at[section, place, yb], {"rep": (yb + k) % ny * PAIR + xb})

    def chip(place, j):
        return remote(held(place, j), held(place, j), ss.at[1 + ny, place, j], sr.at[section, place, j], peer)

    def arrival(b, place, j):
        return remote(all_small.at[b, place, j], all_small.at[b, place, j], ss.at[1, place, 0], sr.at[b, place, j], peer)

    for way in (1, -1):
        @pl.when(there(way))
        def _():
            first(way).start()

    def tokens_beside(m):
        return remote(tokens_ref.at[m], all_tokens.at[section, xb, m], ts.at[0, m], tr.at[section, xb, m], beside)

    def tokens_chip(x, m):
        if x is None:
            return remote(tokens_ref.at[m], all_tokens.at[section, xb, m], ts.at[1, m], tr.at[section, xb, m], peer)
        place = all_tokens.at[section, x, m]
        return remote(place, place, ts.at[2, m], tr.at[section, x, m], peer)

    def tokens_arrival(b, x, m):
        place = all_tokens.at[b, x, m]
        return remote(place, place, ts.at[0, m], tr.at[b, x, m], peer)

    micro, seq_len, _ = tokens_ref.shape
    start()
    for m in range(micro):
        tokens_beside(m).start()
        tokens_chip(None, m).start()
        all_tokens[section, xb, m] = tokens_ref[m]
    for j in range(ny):
        all_small[section, z, j] = small[j]

    def relay_small(d):
        for way in (1, -1):
            place = z - way * d

            @pl.when((place >= 0) & (place < ns))
            def _():
                arrival(section, place, yb).wait_recv()

                @pl.when(there(way))
                def _():
                    onward(place, way).start()

                for k in range(1, ny):
                    across(place, k).start()
                chip(place, yb).start()

    def unpack():
        channels = part * ns
        inner = ogn_ref.shape[1] * ns
        cw = inner // ns // PAIR
        unit = dtb_ref.shape[1] // PAIR
        mine_w = half * cw
        for place in range(ns):
            pack_from(1 - section, place).wait_recv()
        ph_ref[...] = jnp.zeros_like(ph_ref)
        px_ref[...] = jnp.zeros_like(px_ref)
        pbc_ref[...] = jnp.zeros_like(pbc_ref)
        spread = head_map(mine_w, 2 * PAIR * mine_w // heads)
        for b in range(2):
            for at in range(ns):
                full[0 : taps + 1, at * part : (at + 1) * part] = packs[b, at, 0 : taps + 1, :part]
                size = pgn_ref.shape[1]
                gain_ref[b, :, at * size : (at + 1) * size] = packs[b, at, taps + 1 : taps + 2, :size]
            pbc_ref[b, 0 : taps + 1, :] = full[0 : taps + 1, inner:channels]
            row8[...] = jnp.zeros_like(row8)
            for t in range(2):
                for q in range(PAIR):
                    @pl.when((section == t) & (xb == q))
                    def _():
                        for k in range(half):
                            at = t * half + k
                            col = (at * PAIR + q) * cw
                            put = slice(k * cw, (k + 1) * cw)
                            lane = slice(k * unit, (k + 1) * unit)
                            take = slice(q * unit, (q + 1) * unit)
                            px_ref[b, 0 : taps + 1, put] = full[0 : taps + 1, col : col + cw]
                            px_ref[b, taps + 2 : taps + 3, put] = packs[b, at, taps + 2 : taps + 3, q * cw : (q + 1) * cw]
                            ph_ref[b, 0:1, lane] = packs[b, at, taps + 3 : taps + 4, take]
                            ph_ref[b, 1:2, lane] = packs[b, at, taps + 3 : taps + 4, unit3 + q * unit : unit3 + (q + 1) * unit]
                            row8[0:1, lane] = packs[b, at, taps + 3 : taps + 4, 2 * unit3 + q * unit : 2 * unit3 + (q + 1) * unit]
            px_ref[b, taps + 1 : taps + 2, :] = mm(row8[...], spread)[0:1]

    def shared_columns():
        unit = dtb_ref.shape[1] // PAIR
        shape = (wbc_ref.shape[2] - lanes, LANES)
        source, head = rows_of(shape), lanes_of(shape)
        wanted = ((section * half + head // unit) * PAIR + xb) * unit + head % unit
        chosen = ((source == wanted) & (head < half * unit)).astype(BF)
        for b in range(2):
            for at in range(ns):
                for j in range(ny):
                    low = (at * ny + j) * rows
                    wbc_ref[b, low : low + rows, :lanes] = all_small[b, at, j, :, :lanes]
                    wbc_ref[b, low : low + rows, lanes:] = mm(all_small[b, at, j, :, lanes:], chosen).astype(BF)

    def prepare():
        per = seq_len // CHUNK
        for x in range(PAIR):
            for m in range(micro):
                for c in range(per):
                    row = (x * micro + m) * per + c
                    at = lanes_of((1, LANES)).astype(F32) + float(c * CHUNK)
                    live_ref[row : row + 1, :] = (at < all_counts[x, m : m + 1, :]).astype(F32)

        def step(i, _):
            x, m, c = i // (micro * per), i // per % micro, i % per
            span = pl.ds(pl.multiple_of(c * CHUNK, CHUNK), CHUNK)
            wide = all_tokens[0, x, m, span].astype(F32)
            normed_ref[x * micro + m, span] = (wide * rms(wide) * gain_ref[0]).astype(BF)
            live = as_column(live_ref[pl.ds(i, 1), :])
            live_out_ref[x * micro + m, span] = (all_tokens[1, x, m, span].astype(F32) * live).astype(BF)
            return 0

        lax.fori_loop(0, PAIR * micro * per, step, 0)

    relay_small(1)
    for k in range(1, ns):
        pack_from(section, (z + k) % ns).wait_recv()
        pack_chip((z + k) % ns).start()
    for j in range(ny):
        chip(z, j).start()
    for d in range(1, ns):
        if d == ns - 1:
            unpack()
            for m in range(micro):
                tokens_arrival(section, 1 - xb, m).wait_recv()
                tokens_chip(1 - xb, m).start()
            counts.wait_send()
            remote(counts_ref, all_counts.at[1 - xb], cs, cr, beside).wait_recv()
            for m in range(micro):
                for x in range(PAIR):
                    tokens_arrival(1 - section, x, m).wait_recv()
            prepare()
        relay(d)
        if d + 1 < ns:
            relay_small(d + 1)
    for place in range(ns):
        @pl.when(place != z)
        def _():
            for k in range(1, ny):
                j = (yb + k) % ny
                arrival(section, place, j).wait_recv()
                chip(place, j).start()
    for place in range(ns):
        for j in range(ny):
            arrival(1 - section, place, j).wait_recv()
    shared_columns()
    finish()
    for m in range(micro):
        tokens_beside(m).wait_send()
        tokens_chip(None, m).wait_send()
        tokens_chip(1 - xb, m).wait_send()
    for k in range(1, ns):
        pack_to(k).wait_send()
        pack_chip((z + k) % ns).wait_send()
    pack_from(section, z).wait_send()
    for way in (1, -1):
        @pl.when(there(way))
        def _():
            first(way).wait_send()
    for place in range(ns):
        for j in range(ny):
            chip(place, j).wait_send()

        @pl.when(place != z)
        def _():
            for k in range(1, ny):
                across(place, k).wait_send()

            @pl.when(jnp.where(place < z, z < ns - 1, z > 0))
            def _():
                onward(place, 1).wait_send()


def greet_all(ns, ny):
    section, xb, peer, beside = partners()
    z = lax.axis_index("shard")
    yb = lax.axis_index("rep") // PAIR
    found = [peer, beside] + [{"rep": (yb + k) % ny * PAIR + xb} for k in range(1, ny)]
    for k in range(1, ns):
        found += [{"shard": (z + k) % ns}, {"section": 1 - section, "shard": (z + k) % ns}]
    greet(*found)


def run_start(tokens, counts, smalls, bc, dt, q, o, heads):
    conv_weight, _, dt_bias, _, _, _, out_gain = smalls
    ny = q.shape[1]
    ns = heads // dt_bias.shape[1]
    micro, seq_len, width = tokens.shape
    taps = conv_weight.shape[0]
    inner = out_gain.shape[1] * ns
    mine_w = inner // (2 * PAIR)
    states2 = bc.shape[1]
    seqs = PAIR * micro
    outs, sems = weights_shapes(q, o, ns)
    dma = pltpu.SemaphoreType.DMA
    hbm = pl.BlockSpec(memory_space=pl.ANY)
    shape = jax.ShapeDtypeStruct
    rows = bc.shape[0] // ny
    pack = (8, -(-max(conv_weight.shape[1], out_gain.shape[1]) // LANES) * LANES)
    return pl.pallas_call(
        functools.partial(start_kernel, ns=ns, ny=ny, taps=taps, heads=heads),
        in_specs=[VM] * 13,
        out_specs=[VM] * 9 + [hbm, hbm],
        out_shape=[
            shape((2, PAIR) + tokens.shape, BF),
            shape((seqs, seq_len, width), BF),
            shape((seqs, seq_len, width), BF),
            shape((seqs * seq_len // CHUNK, LANES), F32),
            shape((2, 8, mine_w), F32),
            shape((2, 8, states2), F32),
            shape((2, 8, LANES), F32),
            shape((2, 1, width), F32),
            shape((2, width, states2 + LANES), BF),
        ]
        + outs,
        scratch_shapes=[
            pltpu.VMEM((ny, rows, states2 + LANES), BF),
            pltpu.VMEM((2, ns, ny, rows, states2 + LANES), BF),
            pltpu.VMEM(pack, F32),
            pltpu.VMEM((2, ns) + pack, F32),
            pltpu.VMEM((8, conv_weight.shape[1] * ns), F32),
            pltpu.VMEM((8, LANES), F32),
            pltpu.VMEM((PAIR,) + counts.shape, F32),
        ]
        + sems
        + [
            dma((3, 2)), dma((2, PAIR, 2)), dma((2 + ny, max(ns, 2), ny)), dma((2, ns, ny)),
            dma((2, ns)), dma((2, ns)), dma(()), dma(()),
        ],
        compiler_params=comm_params(5),
        cost_estimate=pl.CostEstimate(flops=50_000_000, bytes_accessed=200_000_000, transcendentals=0),
        name="start",
    )(tokens, counts, *smalls, bc, dt, q, o)


def rms(v):
    return lax.rsqrt(jnp.mean(v * v, axis=-1, keepdims=True) + EPSILON)


def spread_out(out_ref, send, recv, peer, per):
    def copy(i, owner):
        span = pl.ds(pl.multiple_of(i % per * CHUNK, CHUNK), CHUNK)
        place = out_ref.at[i // per * 2 + owner, span]
        return remote(place, place, send.at[2, i], recv.at[2, i], peer)

    return copy


def onward_kernel(part_ref, tokens_ref, sums_ref, live_ref, gain_ref, q_ref, o_ref, hidden_ref, normed_ref, rate_ref, gain_out_ref, w_in, w_out,
                  got_a, held, got_x, got_s, half_s, rows_ref, send, recv, send_s, recv_s, rows_s, qs, qr, os_, or_, *, inner, ns, ny):
    section, _, peer, beside = partners()
    per = part_ref.shape[1] // CHUNK
    steps = PAIR * per
    greet_line(ns, ny)
    start, relay_in, relay_out, finish = weights_flow(1, q_ref, o_ref, w_in, w_out, qs, qr, os_, or_, ns=ns, ny=ny, split=True)

    def rows_at(x):
        return pltpu.make_async_copy(tokens_ref.at[0, x, section], rows_ref.at[x], rows_s.at[x])

    for x in range(PAIR):
        rows_at(x).start()
    first = remote(sums_ref, got_s.at[0], send_s.at[0], recv_s.at[0], peer)
    second = remote(half_s, got_s.at[1], send_s.at[1], recv_s.at[1], beside)
    first.start()
    copy = spread_out(hidden_ref, send, recv, peer, per)

    def use(i, x, span, total):
        seq = x * 2 + section
        scale = as_column(rate_ref[pl.ds(seq * per + i % per, 1), :] * live_ref[pl.ds(seq * per + i % per, 1), :])
        gained = scale * total
        gain_out_ref[i] = gained.astype(BF)
        low = (rows_ref[x, span].astype(F32) + gained).astype(BF)
        hidden_ref[seq, span] = low

        @pl.when(i > 0)
        def _():
            copy(i - 1, section).start()

        wide = low.astype(F32)
        normed_ref[seq, span] = (wide * rms(wide) * gain_ref[...]).astype(BF)

    def other(i, _):
        copy(i, section).wait_recv()
        seq = i // per * 2 + 1 - section
        span = pl.ds(pl.multiple_of(i % per * CHUNK, CHUNK), CHUNK)
        wide = hidden_ref[seq, span].astype(F32)
        normed_ref[seq, span] = (wide * rms(wide) * gain_ref[...]).astype(BF)
        return 0

    def drain(i, _):
        copy(i, section).wait_send()
        return 0

    stages = exchange(part_ref, got_a, held, got_x, send, recv, use)
    next(stages)
    first.wait()
    half_s[...] = sums_ref[...] + got_s[0]
    second.start()
    start()
    next(stages)
    next(stages)
    second.wait()
    rate_ref[...] = lax.rsqrt((half_s[...] + got_s[1]) / inner + EPSILON)
    work = [lambda d=d, h=h: relay_in(d, h) if h < PARTS else relay_out(d) for d in range(1, ns) for h in range(PARTS + 1)]

    def relays(count):
        for _ in range(min(count, len(work))):
            work.pop(0)()

    for x in range(PAIR):
        rows_at(x).wait()
    relays(PARTS + 2)
    for _ in range(steps):
        next(stages)
        relays(1)
    copy(steps - 1, section).start()
    lax.fori_loop(0, steps, other, 0)
    for step in work:
        step()
    finish()
    for _ in stages:
        pass
    lax.fori_loop(0, steps, drain, 0)


def back_kernel(part_ref, hidden_ref, tokens_ref, gained_ref, live_ref, gain_ref, out_ref, live_out_ref, dots_ref,
                got_a, held, got_x, dots_own, dots_got, rows_ref, cot_ref, send, recv, send_s, recv_s, rows_s, cot_s):
    section, _, peer, beside = partners()
    per = part_ref.shape[1] // CHUNK
    steps = PAIR * per
    greet(peer, beside)

    def rows_at(x):
        return pltpu.make_async_copy(hidden_ref.at[x * 2 + section], rows_ref.at[x], rows_s.at[x])

    def cot_at(x):
        return pltpu.make_async_copy(tokens_ref.at[1, x, section], cot_ref.at[x], cot_s.at[x])

    for x in range(PAIR):
        rows_at(x).start()
        cot_at(x).start()
    dots_own[...] = jnp.zeros_like(dots_own)
    copy = spread_out(out_ref, send, recv, peer, per)

    def live_of(seq, i):
        return as_column(live_ref[pl.ds(seq * per + i % per, 1), :])

    def use(i, x, span, total):
        seq = x * 2 + section
        rows = rows_ref[x, span].astype(F32)
        inv = rms(rows)
        hat = rows * inv
        d_hat = total * gain_ref[...]
        d_rows = inv * (d_hat - hat * jnp.mean(d_hat * hat, axis=-1, keepdims=True))
        low = (cot_ref[x, span].astype(F32) + d_rows).astype(BF)
        out_ref[seq, span] = low

        @pl.when(i > 0)
        def _():
            copy(i - 1, section).start()

        live = low.astype(F32) * live_of(seq, i)
        live_out_ref[seq, span] = live.astype(BF)
        dots_own[pl.ds(i, 1), :] = as_row(jnp.sum(live * gained_ref[i].astype(F32), axis=1, keepdims=True))

    def other(i, _):
        copy(i, section).wait_recv()
        seq = i // per * 2 + 1 - section
        span = pl.ds(pl.multiple_of(i % per * CHUNK, CHUNK), CHUNK)
        live_out_ref[seq, span] = (out_ref[seq, span].astype(F32) * live_of(seq, i)).astype(BF)
        return 0

    def drain(i, _):
        copy(i, section).wait_send()
        return 0

    stages = exchange(part_ref, got_a, held, got_x, send, recv, use)
    for _ in range(3):
        next(stages)
    for x in range(PAIR):
        rows_at(x).wait()
        cot_at(x).wait()
    for i in range(steps):
        next(stages)
    copy(steps - 1, section).start()
    dots = remote(dots_own, dots_got, send_s.at[0], recv_s.at[0], peer)
    lax.fori_loop(0, steps, other, 0)
    dots.start()
    for _ in stages:
        pass
    lax.fori_loop(0, steps, drain, 0)
    dots.wait()
    for x in range(PAIR):
        for c in range(per):
            i = x * per + c
            dots_ref[pl.ds((x * 2 + section) * per + c, 1), :] = dots_own[i : i + 1, :]
            dots_ref[pl.ds((x * 2 + 1 - section) * per + c, 1), :] = dots_got[i : i + 1, :]


def exchange_scratch(part):
    steps = PAIR * part.shape[1] // CHUNK
    block = (steps, CHUNK, part.shape[2])
    return [pltpu.VMEM(block, BF)] * 3, [pltpu.SemaphoreType.DMA((3, steps)), pltpu.SemaphoreType.DMA((3, steps))]


def own_rows(part):
    return pltpu.VMEM((PAIR,) + part.shape[1:], BF)


def comm_params(collective_id):
    return pltpu.CompilerParams(collective_id=collective_id, has_side_effects=True, vmem_limit_bytes=60 << 20)


def run_onward(part, rows, sums, live, gain, q, o, inner, ns):
    wide, sems = exchange_scratch(part)
    steps = PAIR * part.shape[1] // CHUNK
    small = pltpu.VMEM(sums.shape, F32)
    ny = q.shape[1]
    outs, more = weights_shapes(q, o, ns)
    return pl.pallas_call(
        functools.partial(onward_kernel, inner=inner, ns=ns, ny=ny),
        in_specs=[VM, pl.BlockSpec(memory_space=pl.ANY)] + [VM] * 5,
        out_specs=[VM] * 4 + [pl.BlockSpec(memory_space=pl.ANY)] * 2,
        out_shape=[
            jax.ShapeDtypeStruct(part.shape, BF),
            jax.ShapeDtypeStruct(part.shape, BF),
            jax.ShapeDtypeStruct(sums.shape, F32),
            jax.ShapeDtypeStruct((steps, CHUNK, part.shape[2]), BF),
        ]
        + outs,
        scratch_shapes=wide + [pltpu.VMEM((2,) + sums.shape, F32), small, own_rows(part)] + sems + [pltpu.SemaphoreType.DMA((2,))] * 3 + more,
        compiler_params=comm_params(1),
        cost_estimate=pl.CostEstimate(flops=50_000_000, bytes_accessed=150_000_000, transcendentals=0),
        name="onward",
    )(part, rows, sums, live, gain, q, o)


def run_back(part, hidden, tokens, gained, live, gain):
    wide, sems = exchange_scratch(part)
    small = pltpu.VMEM((8, LANES), F32)
    hbm = pl.BlockSpec(memory_space=pl.ANY)
    return pl.pallas_call(
        back_kernel,
        in_specs=[VM, hbm, hbm, VM, VM, VM],
        out_specs=[VM] * 3,
        out_shape=[
            jax.ShapeDtypeStruct(part.shape, BF),
            jax.ShapeDtypeStruct(part.shape, BF),
            jax.ShapeDtypeStruct(live.shape, F32),
        ],
        scratch_shapes=wide + [small, small, own_rows(part), own_rows(part)] + sems + [pltpu.SemaphoreType.DMA((2,))] * 4,
        compiler_params=comm_params(2),
        cost_estimate=pl.CostEstimate(flops=50_000_000, bytes_accessed=150_000_000, transcendentals=0),
        name="back",
    )(part, hidden, tokens, gained, live, gain)


PARTS = 2
PIECE_ROWS = 32
BLOCK = 16


def by_rows(count, body):
    def step(i, _):
        body(pl.multiple_of(i * BLOCK, BLOCK))
        return 0

    lax.fori_loop(0, count // BLOCK, step, 0)


def line_steps(n):
    return [step for i in range(n - 1) for step in ((1, n - 1 - i), (-1, i))]


def hand_out(b, boards, owns, pc_s, pc_r, *, ny):
    section, xb, peer, beside = partners()
    yb = lax.axis_index("rep") // PAIR

    def y_peer(k):
        return {"rep": (yb + k) % ny * PAIR + xb}

    def y_from(k):
        return (yb + ny - k) % ny

    def span_of(h):
        return pl.ds(pl.multiple_of(h * PIECE_ROWS, PIECE_ROWS), PIECE_ROWS)

    def piece(i, x, y, t, h, kind, device):
        place = boards[i].at[x, y, t, span_of(h)]
        return remote(place, place, pc_s.at[i, kind, x, y, t, h], pc_r.at[i, x, y, t, h], device)

    def offer(i, h):
        return remote(owns[i].at[span_of(h)], boards[i].at[xb, yb, 1 - b, span_of(h)],
                      pc_s.at[i, 0, xb, yb, 1 - b, h], pc_r.at[i, xb, yb, 1 - b, h], peer)

    def gather_chip(i, h):
        @pl.when(section == b)
        def _():
            boards[i][xb, yb, b, span_of(h)] = owns[i][span_of(h)]

        @pl.when(section != b)
        def _():
            offer(i, h).start()

    def gather_side(i, h):
        @pl.when(section == b)
        def _():
            piece(i, xb, yb, 1 - b, h, 0, peer).wait_recv()
            for t in range(2):
                piece(i, xb, yb, t, h, ny, beside).start()

    def gather_y(i, h):
        @pl.when(section == b)
        def _():
            for t in range(2):
                for k in range(1, ny):
                    piece(i, xb, yb, t, h, k, y_peer(k)).start()

    def gather_x(i, h):
        @pl.when(section == b)
        def _():
            for k in range(1, ny):
                for t in range(2):
                    piece(i, xb, y_from(k), t, h, k, peer).wait_recv()
                    piece(i, xb, y_from(k), t, h, ny, beside).start()

    def gather_end(i, h):
        @pl.when(section == b)
        def _():
            for y in range(ny):
                for t in range(2):
                    piece(i, 1 - xb, y, t, h, ny, beside).wait_recv()
                    piece(i, xb, y, t, h, ny, peer).wait_send()
            for t in range(2):
                for k in range(1, ny):
                    piece(i, xb, yb, t, h, k, peer).wait_send()

        @pl.when(section != b)
        def _():
            offer(i, h).wait_send()

    return gather_chip, gather_side, gather_y, gather_x, gather_end


def each(count, body):
    def step(i, _):
        body(i)
        return 0

    lax.fori_loop(0, count, step, 0)


def reduce_flow(b, ga_ref, gb_ref, gc_ref, boards, got_ya, acc_a, got_za, own_a, acc_b, got_zb, own_b, acc_c, got_zc, own_c,
                ya_s, ya_r, za_s, za_r, zb_s, zb_r, zc_s, zc_r, pc_s, pc_r, *, ns, ny):
    _, xb, peer, _ = partners()
    z = lax.axis_index("shard")
    yb = lax.axis_index("rep") // PAIR
    count = ga_ref.shape[2] // PIECE_ROWS
    steps = line_steps(ns)
    order = []
    for _, target in steps:
        if target not in order:
            order.append(target)
    gather_chip, gather_side, gather_y, gather_x, gather_end = hand_out(b, boards, (own_a, own_b), pc_s, pc_r, ny=ny)
    chip_c, side_c, y_c, x_c, end_c = hand_out(1 - b, boards, (None, own_c), pc_s, pc_r, ny=ny)

    def y_peer(k):
        return {"rep": (yb + k) % ny * PAIR + xb}

    def span_of(h):
        return pl.ds(pl.multiple_of(h * PIECE_ROWS, PIECE_ROWS), PIECE_ROWS)

    def ya(k, target, h):
        return remote(ga_ref.at[(yb + k) % ny, target, span_of(h)], got_ya.at[k - 1, target, span_of(h)],
                      ya_s.at[k - 1, target, h], ya_r.at[k - 1, target, h], y_peer(k))

    def start(h):
        for target in order:
            @pl.when(target != z)
            def _():
                for k in range(1, ny):
                    ya(k, target, h).start()
        for k in range(1, ny):
            ya(k, z, h).start()

    streams = ((acc_a, got_za, za_s, za_r), (acc_b, got_zb, zb_s, zb_r), (acc_c, got_zc, zc_s, zc_r))

    def line(i, way, target, h):
        acc, got, send, recv = streams[i]
        place = jnp.where(target == z - 1, ns, target) if way < 0 else target
        return remote(acc.at[target, span_of(h)], got.at[place, span_of(h)], send.at[target, h], recv.at[place, h], {"shard": z + way})

    def wait_line(place, h):
        for acc, got, send, recv in streams:
            remote(acc.at[0, span_of(h)], got.at[place, span_of(h)], send.at[0, h], recv.at[place, h], peer).wait_recv()

    def wait_y(target, h):
        for k in range(1, ny):
            remote(ga_ref.at[0, target, span_of(h)], got_ya.at[k - 1, target, span_of(h)], ya_s.at[k - 1, target, h],
                   ya_r.at[k - 1, target, h], peer).wait_recv()

    def add(target, h, into_a, into_b, into_c, start, extra):
        span = span_of(h)
        total = ga_ref[yb, target, span].astype(F32)
        for k in range(1, ny):
            total = total + got_ya[k - 1, target, span].astype(F32)
        for place in extra:
            total = total + got_za[place, span].astype(F32)
        into_a[start + (span,)] = total.astype(BF)
        for ref, got, into in ((gb_ref, got_zb, into_b), (gc_ref, got_zc, into_c)):
            total = ref[target, span].astype(F32)
            for place in extra:
                total = total + got[place, span].astype(F32)
            into[start + (span,)] = total.astype(BF)

    def active(way, target):
        return target > z if way > 0 else target < z

    def step(way, target, h):
        wait_y(target, h)
        far = z > 0 if way > 0 else z < ns - 1

        @pl.when(jnp.logical_not(far))
        def _():
            add(target, h, acc_a, acc_b, acc_c, (target,), ())

        @pl.when(far)
        def _():
            wait_line(target, h)
            add(target, h, acc_a, acc_b, acc_c, (target,), (target,))

        for i in range(3):
            line(i, way, target, h).start()

    def last(h):
        wait_y(z, h)

        @pl.when(z == 0)
        def _():
            wait_line(ns, h)
            add(z, h, own_a, own_b, own_c, (), (ns,))

        @pl.when(z == ns - 1)
        def _():
            wait_line(z, h)
            add(z, h, own_a, own_b, own_c, (), (z,))

        @pl.when((z > 0) & (z < ns - 1))
        def _():
            wait_line(z, h)
            wait_line(ns, h)
            add(z, h, own_a, own_b, own_c, (), (z, ns))

        for i in range(2):
            gather_chip(i, h)
        chip_c(1, h)

    def sides(h):
        for i in range(2):
            gather_side(i, h)
        side_c(1, h)
        for i in range(2):
            gather_y(i, h)
        y_c(1, h)

    def crosses(h):
        for i in range(2):
            gather_x(i, h)
        x_c(1, h)

    def slot(at):
        for way, target in steps:
            h = at - z if way > 0 else at - (ns - 1 - z)

            @pl.when(active(way, target) & (h >= 0) & (h < count))
            def _():
                step(way, target, h)

        mine = at - jnp.where(2 * z > ns - 1, z, ns - 1 - z)
        for late, body in ((0, last), (1, sides), (2, crosses)):
            @pl.when((mine >= late) & (mine < count + late))
            def _():
                body(mine - late)

    def finish():
        def ends(h):
            for i in range(2):
                gather_end(i, h)
            end_c(1, h)
            for target in range(ns):
                for k in range(1, ny):
                    ya(k, target, h).wait_send()
            for way, target in steps:
                @pl.when(active(way, target))
                def _():
                    for i in range(3):
                        line(i, way, target, h).wait_send()

        each(count, ends)

    return start, slot, count + ns + 1, finish


def reduce_shapes(ga, gb):
    ny, ns, ra, ca = ga.shape
    rb, cb = gb.shape[1:]
    dma = pltpu.SemaphoreType.DMA
    parts = ra // PIECE_ROWS
    outs = [jax.ShapeDtypeStruct((PAIR, ny, 2, ra, ca), BF), jax.ShapeDtypeStruct((PAIR, ny, 2, rb, cb), BF)]
    scratch = [
        pltpu.VMEM((ny - 1, ns, ra, ca), BF),
        pltpu.VMEM((ns, ra, ca), BF),
        pltpu.VMEM((ns + 1, ra, ca), BF),
        pltpu.VMEM((ra, ca), BF),
        *[pltpu.VMEM((ns, rb, cb), BF), pltpu.VMEM((ns + 1, rb, cb), BF), pltpu.VMEM((rb, cb), BF)] * 2,
        dma((ny - 1, ns, parts)), dma((ny - 1, ns, parts)),
        *[dma((ns, parts)), dma((ns + 1, parts))] * 3,
        dma((2, ny + 1, PAIR, ny, 2, parts)), dma((2, PAIR, ny, 2, parts)),
    ]
    return outs, scratch


def tail_kernel(ga_ref, gb_ref, gc_ref, pa_ref, vec_ref, p_ref, tokens_ref, cot_all, gain_ref,
                all_a, all_b, vec_out, res_ref, *refs, ns, ny):
    flow, (got_p, held, got_x, give, rows_ref, cot_ref, vec_y, vec_h, vec_z, vec_t, ra_s, ra_r, v_s, v_r, rows_s) = refs[:20], refs[20:]
    section, xb, peer, beside = partners()
    z = lax.axis_index("shard")
    yb = lax.axis_index("rep") // PAIR

    def y_peer(k):
        return {"rep": (yb + k) % ny * PAIR + xb}

    def z_peer(k):
        return {"shard": (z + k) % ns}

    greet(peer, beside, *(y_peer(k) for k in range(1, ny)), *(z_peer(k) for k in range(1, ns)))

    def over_y(k):
        return remote(vec_ref, vec_y.at[k - 1], v_s.at[k], v_r.at[k], y_peer(k))

    def over_z(k):
        return remote(vec_h, vec_z.at[k - 1], v_s.at[ny + k], v_r.at[ny + k], z_peer(k))

    to_chip = remote(vec_t.at[1 - section], vec_out.at[section, xb], v_s.at[0], v_r.at[0], peer)

    def to_side(t):
        return remote(vec_out.at[t, xb], vec_out.at[t, xb], v_s.at[ny + ns + t], v_r.at[ny + ns + t], beside)

    for k in range(1, ny):
        over_y(k).start()

    per = p_ref.shape[1] // CHUNK
    rows_copy = pltpu.make_async_copy(tokens_ref.at[0, xb, section], rows_ref, rows_s.at[0])
    cot_copy = pltpu.make_async_copy(cot_all.at[xb * 2 + section], cot_ref, rows_s.at[1])

    def p_peer(x, c):
        span = pl.ds(c * CHUNK, CHUNK)
        return remote(p_ref.at[x * 2 + 1 - section, span], got_p.at[x, c], ra_s.at[0, x, c], ra_r.at[0, x, c], peer)

    def p_beside(c):
        return remote(held.at[1 - xb, c], got_x.at[c], ra_s.at[1, 0, c], ra_r.at[1, 0, c], beside)

    def p_give(c):
        return remote(give.at[c], res_ref.at[1, pl.ds(c * CHUNK, CHUNK)], ra_s.at[1, 1, c], ra_r.at[1, 1, c], peer)

    boards = (all_a, all_b)
    pieces = flow[18:20]
    chip1, side1, y1, x1, end1 = hand_out(1, boards, (pa_ref, None), *pieces, ny=ny)
    count = ga_ref.shape[2] // PIECE_ROWS
    start, slot, slots, end0 = reduce_flow(0, ga_ref, gb_ref, gc_ref, boards, *flow, ns=ns, ny=ny)

    def both(body):
        each(count, lambda h: body(0, h))

    rows_copy.start()
    cot_copy.start()

    def rows_out():
        for c in range(per):
            for x in range(PAIR):
                p_peer(x, c).start()

    def pieces_side():
        both(side1)

    def pieces_y():
        both(y1)

    def rows_beside():
        for c in range(per):
            for x in range(PAIR):
                p_peer(x, c).wait_recv()

                def body(low):
                    span = pl.ds(low, BLOCK)
                    mine = p_ref[x * 2 + section, pl.ds(c * CHUNK + low, BLOCK)].astype(F32)
                    held[x, c, span] = (mine + got_p[x, c, span].astype(F32)).astype(BF)

                by_rows(CHUNK, body)
            p_beside(c).start()

    def sums_z():
        total = vec_ref[...]
        for k in range(1, ny):
            over_y(k).wait()
            total = total + vec_y[k - 1]
        vec_h[...] = total
        for k in range(1, ns):
            over_z(k).start()

    def pieces_x():
        both(x1)

    def sums_chip():
        total = vec_h[...]
        for k in range(1, ns):
            over_z(k).wait()
            total = total + vec_z[k - 1]
        vec_t[...] = total
        to_chip.start()
        vec_out[section, xb] = vec_t[section]

    def rows_end():
        rows_copy.wait()
        cot_copy.wait()
        for c in range(per):
            p_beside(c).wait_recv()

            def body(low):
                span = pl.ds(low, BLOCK)
                there = pl.ds(c * CHUNK + low, BLOCK)
                total = held[xb, c, span].astype(F32) + got_x[c, span].astype(F32)
                rows = rows_ref[there].astype(F32)
                inv = rms(rows)
                hat = rows * inv
                d_hat = total * gain_ref[...]
                d_rows = inv * (d_hat - hat * jnp.mean(d_hat * hat, axis=-1, keepdims=True))
                low_rows = (cot_ref[there].astype(F32) + d_rows).astype(BF)
                give[c, span] = low_rows

                @pl.when(section == 0)
                def _():
                    res_ref[0, there] = low_rows

            by_rows(CHUNK, body)

        @pl.when(section != 0)
        def _():
            for c in range(per):
                p_give(c).start()

    def sums_side():
        to_chip.wait_send()
        remote(vec_t.at[0], vec_out.at[1 - section, xb], v_s.at[0], v_r.at[0], peer).wait_recv()
        for t in range(2):
            to_side(t).start()

    def sums_end():
        for t in range(2):
            to_side(t).wait_send()
            remote(vec_out.at[t, xb], vec_out.at[t, 1 - xb], v_s.at[ny + ns + t], v_r.at[ny + ns + t], beside).wait_recv()

    ahead = min(4, count)
    rows_out()
    both(chip1)
    each(ahead, start)
    between = ((0, pieces_side), (0, rows_beside), (1, sums_z), (4, sums_chip), (6, rows_end), (8, pieces_y), (9, sums_side), (12, sums_end), (15, pieces_x))

    def go(at, _):
        @pl.when(at + ahead < count)
        def _():
            start(at + ahead)

        slot(at)
        for n, body in between:
            @pl.when(at == n)
            def _():
                body()

        return 0

    lax.fori_loop(0, max(slots, between[-1][0] + 1), go, 0)
    both(end1)
    end0()
    for c in range(per):
        for x in range(PAIR):
            p_peer(x, c).wait_send()
        p_beside(c).wait_send()

        @pl.when(section != 0)
        def _():
            p_give(c).wait_send()

        @pl.when(section == 0)
        def _():
            p_give(c).wait_recv()


def run_tail(ga, gb, gc, pa, vec, p, tokens, cot, gain):
    ny, ns = ga.shape[:2]
    seq_len, width = p.shape[1:]
    per = seq_len // CHUNK
    block = (CHUNK, width)
    dma = pltpu.SemaphoreType.DMA
    hbm = pl.BlockSpec(memory_space=pl.ANY)
    outs, scratch = reduce_shapes(ga, gb)
    return pl.pallas_call(
        functools.partial(tail_kernel, ns=ns, ny=ny),
        in_specs=[VM] * 6 + [hbm, hbm, VM],
        out_specs=[VM] * 4,
        out_shape=outs + [jax.ShapeDtypeStruct((2, PAIR) + vec.shape[1:], F32), jax.ShapeDtypeStruct((2, seq_len, width), BF)],
        scratch_shapes=scratch
        + [
            pltpu.VMEM((PAIR, per) + block, BF),
            pltpu.VMEM((PAIR, per) + block, BF),
            pltpu.VMEM((per,) + block, BF),
            pltpu.VMEM((per,) + block, BF),
            pltpu.VMEM((seq_len, width), BF),
            pltpu.VMEM((seq_len, width), BF),
            pltpu.VMEM((ny - 1,) + vec.shape, F32),
            pltpu.VMEM(vec.shape, F32),
            pltpu.VMEM((ns - 1,) + vec.shape, F32),
            pltpu.VMEM(vec.shape, F32),
            dma((2, PAIR, per)), dma((2, PAIR, per)),
            dma((ny + ns + 2,)), dma((ny + ns + 2,)),
            dma((2,)),
        ],
        compiler_params=comm_params(4),
        cost_estimate=pl.CostEstimate(flops=50_000_000, bytes_accessed=300_000_000, transcendentals=0),
        name="tail",
    )(ga, gb, gc, pa, vec, p, tokens, cot, gain)


def place_kernel(a_ref, b_ref, in_ref, out_ref, dt_ref, *, places, dts, ny):
    for col, size, index, off in places:
        in_ref[:, col : col + size] = a_ref[index + (slice(None), slice(off, off + size))].astype(F32)
    for col, size, index, off in dts:
        dt_ref[:, col : col + size] = a_ref[index + (slice(None), slice(off, off + size))].astype(F32)
    part = b_ref.shape[-1]
    for q in range(PAIR):
        for t in range(2):
            for y in range(ny):
                col = (t * ny + y) * part
                out_ref[q, :, col : col + part] = b_ref[q, y, t].astype(F32)


def run_place(pieces, places, dts, columns, heads, block):
    ny = pieces[0].shape[1]
    rows = pieces[0].shape[3]
    lead = (PAIR, ny, 2)
    width = 2 * ny * pieces[1].shape[4]
    return pl.pallas_call(
        functools.partial(place_kernel, places=places, dts=dts, ny=ny),
        grid=(rows // block,),
        in_specs=[pl.BlockSpec(lead + (block, v.shape[4]), lambda i: (0, 0, 0, i, 0)) for v in pieces],
        out_specs=[
            pl.BlockSpec((block, columns), lambda i: (i, 0)),
            pl.BlockSpec((PAIR, block, width), lambda i: (0, i, 0)),
            pl.BlockSpec((block, heads), lambda i: (i, 0)),
        ],
        out_shape=[
            jax.ShapeDtypeStruct((rows, columns), F32),
            jax.ShapeDtypeStruct((PAIR, rows, width), F32),
            jax.ShapeDtypeStruct((rows, heads), F32),
        ],
        compiler_params=PARAMS,
        cost_estimate=pl.CostEstimate(flops=1_000_000, bytes_accessed=25_000_000, transcendentals=0),
        name="place",
    )(*pieces)


def smalls_kernel(z_ref, v_ref, conv_ref, heads_ref, pre_ref, out_ref, full, *, taps, ns, mine_w, states2, heads, width):
    half = ns // 2
    cw = mine_w // half
    unit = heads // ns // PAIR
    gbc, gh = mine_w, mine_w + states2
    spread = head_map(mine_w, 2 * mine_w * PAIR // heads)
    shared = v_ref[0, 0] + v_ref[0, 1] + v_ref[1, 0] + v_ref[1, 1]
    full[:, 2 * PAIR * mine_w :] = shared[:8, gbc : gbc + states2]
    for t in range(2):
        for q in range(PAIR):
            for k in range(half):
                col = ((t * half + k) * PAIR + q) * cw
                full[:, col : col + cw] = v_ref[t, q, :8, k * cw : (k + 1) * cw]
    channels = (2 * PAIR * mine_w + states2) // ns
    inner = 2 * PAIR * mine_w // ns
    part = width // ns
    wide = v_ref.shape[3]
    skips = []
    for t in range(2):
        skips.append([])
        for q in range(PAIR):
            row = v_ref[t, q, taps + 1 : taps + 2, :mine_w]
            high = row.astype(BF)
            rest = row - high.astype(F32)
            mid = rest.astype(BF)
            rows8 = lambda v: jnp.broadcast_to(v, (8, mine_w))
            skips[t].append((mm_t(rows8(high), spread) + mm_t(rows8(mid), spread) + mm_t(rows8(rest - mid.astype(F32)), spread))[0:1])
    heads_ref[...] = jnp.zeros_like(heads_ref)
    for at in range(ns):
        @pl.when(z_ref[0] == at)
        def _():
            conv_ref[...] = full[:, at * channels : (at + 1) * channels]
            out_ref[...] = full[taps + 2 : taps + 3, at * inner : (at + 1) * inner]
            t, k = at // half, at % half
            for q in range(PAIR):
                span = slice(gh + k * unit, gh + (k + 1) * unit)
                put = slice(q * unit, (q + 1) * unit)
                heads_ref[0:1, put] = v_ref[t, q, 0:1, span]
                heads_ref[1:2, put] = v_ref[t, q, 1:2, span]
                heads_ref[2:3, put] = skips[t][q][:, k * unit : (k + 1) * unit]
            for row in range(-(-width // wide)):
                low, high = max(at * part, row * wide), min((at + 1) * part, (row + 1) * wide)
                if low < high:
                    pre_ref[:, low - at * part : high - at * part] = shared[8 + row : 9 + row, low - row * wide : high - row * wide]


def run_smalls(z, v, taps, ns, mine_w, states2, heads, width):
    channels = (2 * PAIR * mine_w + states2) // ns
    whole = lambda *dims: pl.BlockSpec(dims, lambda i, z: (0,) * len(dims))
    return pl.pallas_call(
        functools.partial(smalls_kernel, taps=taps, ns=ns, mine_w=mine_w, states2=states2, heads=heads, width=width),
        grid_spec=pltpu.PrefetchScalarGridSpec(
            num_scalar_prefetch=1,
            grid=(1,),
            in_specs=[whole(*v.shape)],
            out_specs=[whole(8, channels), whole(8, LANES), whole(1, width // ns), whole(1, 2 * PAIR * mine_w // ns)],
            scratch_shapes=[pltpu.VMEM((8, channels * ns), F32)],
        ),
        out_shape=[
            jax.ShapeDtypeStruct((8, channels), F32),
            jax.ShapeDtypeStruct((8, LANES), F32),
            jax.ShapeDtypeStruct((1, width // ns), F32),
            jax.ShapeDtypeStruct((1, 2 * PAIR * mine_w // ns), F32),
        ],
        compiler_params=PARAMS,
        cost_estimate=pl.CostEstimate(flops=1_000_000, bytes_accessed=1_000_000, transcendentals=0),
        name="smalls",
    )(z, v)


def dot(a, b):
    return jnp.dot(a, b, preferred_element_type=F32)


def pick(index, options):
    result = options[-1]
    for place in reversed(range(len(options) - 1)):
        result = jnp.where(index == place, options[place], result)
    return result


def ordered(index, own, other, axis):
    return jnp.stack([pick(index, (own, other)), pick(index, (other, own))], axis=axis)


def joined(index, own, other, axis):
    return jnp.concatenate([pick(index, (own, other)), pick(index, (other, own))], axis=axis)


def on_device(boundary, lengths, in_proj, dt_proj, out_proj, conv_weight, conv_bias, dt_bias, a_log, d_skip, pre_gain, out_gain):
    ns = lax.axis_size("shard")
    nr = lax.axis_size("rep")
    ny = nr // PAIR
    s = lax.axis_index("section")
    z = lax.axis_index("shard")
    rep = lax.axis_index("rep")
    xb = rep % PAIR
    yb = rep // PAIR

    def swap(v):
        return lax.ppermute(v, "section", [(0, 1), (1, 0)])

    def x_swap(v):
        return lax.ppermute(v, "rep", [(i, i ^ 1) for i in range(nr)])

    def y_send(v, k):
        return lax.ppermute(v, "rep", [(i, (i // PAIR + k) % ny * PAIR + i % PAIR) for i in range(nr)])

    micro, seq_len, width = boundary.shape[1], boundary.shape[3], boundary.shape[4]
    inner = out_proj.shape[1] * ns
    heads = dt_bias.shape[1] * ns
    taps, channels = conv_weight.shape[1], conv_weight.shape[2] * ns
    states2 = channels - inner
    cw = inner // ns // PAIR
    half = ns // 2
    mine_w = half * cw
    mine_h = heads // (2 * PAIR)
    part_w = 2 * mine_w // ny

    def column_chunks(v, first):
        out = []
        for t in range(2):
            for shard in range(t * half, (t + 1) * half):
                start = first + shard * PAIR * cw
                out.append(pick(xb, tuple(v[:, start + q * cw : start + (q + 1) * cw] for q in range(PAIR))))
        return [jnp.concatenate(out[:half], axis=1), jnp.concatenate(out[half:], axis=1)]

    own_in = in_proj[0]
    q_own = []
    for a, b in zip(column_chunks(own_in, 0), column_chunks(own_in, inner)):
        if ny == 2:
            q_own += [a, b]
        else:
            q_own += [v[:, k * part_w : (k + 1) * part_w] for v in (a, b) for k in range(ny // 2)]
    q_own = jnp.stack(q_own).reshape(2, ny, width // ns, part_w)
    own_out = out_proj[0]
    o_own = pick(xb, (own_out[:cw], own_out[cw : 2 * cw])).reshape(ny, cw // ny, width)

    flat = lambda v: v.reshape(-1, v.shape[-1])
    smalls_own = tuple(flat(v) for v in (conv_weight, conv_bias, dt_bias, a_log, d_skip, pre_gain, out_gain))
    counts = jnp.broadcast_to(lengths.astype(F32), (micro, LANES))
    tokens, normed0, g_out1, live8, px, pbc, ph, gains, w_bcdt, in0, out0 = run_start(
        boundary[0, :, 0], counts, smalls_own, own_in[:, 2 * inner :], dt_proj[0], q_own, o_own, heads
    )
    smalls = [(px[b], pbc[b], ph[b]) for b in range(2)]
    unit_h = heads // ns // PAIR
    w_in, w_out = [in0.reshape(ny, width, part_w)], [out0.reshape(mine_w, width)]
    seqs = PAIR * micro

    def by_seq(v):
        return v.reshape((seqs, seq_len) + v.shape[1:])

    def of_own(v):
        return pick(xb, (v[0], v[1]))

    chunks = seq_len // CHUNK

    def forward(b, normed, dmix):
        normed = normed.reshape(seqs * seq_len, width)
        proj = [dot(normed, w_in[b][j]).astype(BF) for j in range(ny)]
        if ny > 2:
            proj = [jnp.concatenate(proj[: ny // 2], axis=1), jnp.concatenate(proj[ny // 2 :], axis=1)]
        gate, x = by_seq(proj[0]), by_seq(proj[1])
        bcdt = by_seq(dot(normed, w_bcdt[b]))
        gg, y, state, *sums = run_forward(smalls[b], gate, x, bcdt, dmix, taps, mine_h)
        gg = gg.reshape(seqs * seq_len, mine_w)
        part = by_seq(dot(gg, w_out[b]).astype(BF))
        return part, sums, (normed, gate, x, bcdt, gg, y, state)

    def mixed_back(b, g_out):
        dmix = lax.dot_general(g_out, w_out[b], (((1,), (1,)), ((), ())), preferred_element_type=F32)
        return by_seq(dmix.astype(BF))

    part0, sums, stored0 = forward(0, normed0, None)
    hidden, normed, r0, gained0, in1, out1 = run_onward(
        part0, tokens, sums[0].reshape(seqs * chunks, LANES), live8, gains[1], q_own, o_own, float(inner), ns
    )
    w_in.append(in1.reshape(ny, width, part_w))
    w_out.append(out1.reshape(mine_w, width))
    g_out1 = g_out1.reshape(seqs * seq_len, width)
    dmix1 = mixed_back(1, g_out1)
    part1, sums, stored1 = forward(1, normed, dmix1)
    both_sums = run_sums(jnp.concatenate([v.reshape(seqs * chunks, LANES) for v in sums]), 3)
    r1 = lax.rsqrt(both_sums[: seqs * chunks] / inner + EPSILON)

    def backward(b, dmix, stored, r, coef):
        normed, gate, x, bcdt, _, y, state = stored
        scalars = jnp.concatenate([r.reshape(seqs, chunks, LANES), coef.reshape(seqs, chunks, LANES)], axis=1)
        dgate, dx, dbcdt, gsmall = run_backward(smalls[b], gate, x, bcdt, y, state, dmix, scalars, taps, mine_h)
        flat = lambda v: v.reshape(seqs * seq_len, v.shape[-1])
        dgate, dx, dbcdt = flat(dgate), flat(dx), flat(dbcdt)
        if ny == 2:
            dparts = [dgate, dx]
        else:
            dparts = [v[:, k * part_w : (k + 1) * part_w] for v in (dgate, dx) for k in range(ny // 2)]
        against = lambda a, w: lax.dot_general(a, w, (((1,), (1,)), ((), ())), preferred_element_type=F32)
        d_normed = against(dbcdt, w_bcdt[b])
        for j in range(ny):
            d_normed = d_normed + against(dparts[j], w_in[b][j])
        gpre = jnp.sum(d_normed * normed.astype(F32), axis=0) / gains[b, 0]
        across = lambda a, c: lax.dot_general(a, c, (((0,), (0,)), ((), ())), preferred_element_type=F32)

        dbc = dbcdt[:, :states2]
        cols = [dbc[:, : states2 // 2], dbc[:, states2 // 2 :]]
        total = (pick(s, cols).astype(F32) + swap(pick(s, cols[::-1])).astype(F32)).astype(BF)
        cols = [total[:, : states2 // 4], total[:, states2 // 4 :]]
        send = pick(xb, cols[::-1])
        got = x_swap(send)
        total = (pick(xb, cols).astype(F32) + got.astype(F32)).astype(BF)
        mine = jnp.concatenate([total, dbcdt[:, states2 : states2 + states2 // 4]], axis=1)
        grad_in = [across(normed, jnp.concatenate([v, mine], axis=1)).astype(BF) for v in dparts]
        grad_in = [v.reshape(ns, width // ns, -1) for v in grad_in]
        wide = gsmall.shape[1]
        gpre = jnp.pad(gpre, (0, 8 * wide - width)).reshape(8, wide)
        return by_seq(d_normed.astype(BF)), grad_in, jnp.concatenate([gsmall, gpre])

    def z_sum(v):
        parts = [v[j] for j in range(ns)]
        total = pick(z, parts).astype(F32)
        for k in range(1, ns):
            send = lax.dynamic_index_in_dim(v, (z + k) % ns, 0, False)
            got = lax.ppermute(send, "shard", [(i, (i + k) % ns) for i in range(ns)])
            total = total + got.astype(F32)
        return total.astype(BF)

    def out_chip(g_out, gg, r):
        g_scaled = (g_out.astype(F32) * r.reshape(-1, 1)).astype(BF)
        across = lambda a, c: lax.dot_general(a, c, (((0,), (0,)), ((), ())), preferred_element_type=F32)
        grad = across(gg, g_scaled).astype(BF)
        cols = [grad[:, : width // 2], grad[:, width // 2 :]]
        send = pick(s, cols[::-1])
        got = swap(send)
        return joined(s, pick(s, cols), got, 0)

    def out_grad(v):
        step = width // 2 // ny
        parts = [v[:, j * step : (j + 1) * step] for j in range(ny)]
        total = pick(yb, parts).astype(F32)
        for k in range(1, ny):
            send = pick((yb + k) % ny, parts)
            got = y_send(send, k)
            total = total + got.astype(F32)
        return total.astype(BF).reshape(ns, cw, -1)

    v1 = out_chip(g_out1, stored1[4], r1)
    gout1 = out_grad(v1)
    d_normed1, gin1, gsmall1 = backward(1, dmix1, stored1, r1, r1 * r1 * r1 * both_sums[seqs * chunks :] / inner)
    d_normed1, *gin1 = lax.optimization_barrier((d_normed1, *gin1))
    total1 = pick(yb, gin1).astype(F32)
    for k in range(1, ny):
        send = pick((yb + k) % ny, gin1)
        got = y_send(send, k)
        total1 = total1 + got.astype(F32)
    total1 = total1.astype(BF)
    cot0, g_out0, dots0 = run_back(d_normed1, hidden, tokens, gained0, live8, gains[1])

    g_out0 = g_out0.reshape(-1, width)
    dmix0 = mixed_back(0, g_out0)
    v0 = out_chip(g_out0, stored0[4], r0)
    dmix0, total1 = lax.optimization_barrier((dmix0, total1))
    gout0 = out_grad(v0)
    piece_a1 = z_sum(total1)

    part1 = part1.reshape(PAIR, micro, seq_len, width)
    mine = pick(s, (part1[:, 0], part1[:, 1])).astype(F32) + swap(pick(s, (part1[:, 1], part1[:, 0]))).astype(F32)
    mine = mine.astype(BF)
    send = of_own(mine[::-1])
    got = x_swap(send)
    mine = of_own(mine).astype(F32) + got.astype(F32)
    own_hidden = of_own(hidden.reshape(PAIR, micro, seq_len, width))
    scale = of_own((live8 * r1).reshape(PAIR, micro, seq_len, 1))
    final = (pick(s, (own_hidden[0], own_hidden[1])).astype(F32) + pick(s, (scale[0], scale[1])) * mine).astype(BF)
    final = ordered(s, final, swap(final), 0)

    d_normed0, gin0, gsmall0 = backward(0, dmix0, stored0, r0, r0 * r0 * dots0 / inner)
    *pieces, vec, res = run_tail(
        jnp.stack(gin0), gout0, gout1, piece_a1, jnp.stack([gsmall0, gsmall1]), d_normed0, tokens, cot0, gains[0]
    )
    activations = pick(s, (own_hidden, final))
    input_grads = pick(s, (res, of_own(cot0.reshape(PAIR, micro, seq_len, width))))
    places, dts = [], []
    col = 0
    for plane in range(2):
        for t in range(2):
            for k in range(half):
                for q in range(PAIR):
                    y_at, off = divmod(plane * mine_w + k * cw, part_w)
                    places.append((col, cw, (q, y_at, t), off))
                    col += cw
    quad = states2 // 4
    for t in range(2):
        for q in range(PAIR):
            places.append((col, quad, (q, 0, t), part_w))
            col += quad
    for t in range(2):
        for k in range(half):
            for q in range(PAIR):
                dts.append((((t * half + k) * PAIR + q) * unit_h, unit_h, (q, 0, t), part_w + quad + k * unit_h))
    grad_in, grad_out, grad_dt = run_place(pieces, tuple(places), tuple(dts), col, heads, 64)
    grad_out = grad_out.reshape(PAIR * cw, width)
    g_conv, g_heads, g_pre, g_og = run_smalls(z[None], vec, taps, ns, mine_w, states2, heads, width)
    g_cw, g_cb = g_conv[:taps], g_conv[taps]
    g_dtb, g_alg, g_dsk = (g_heads[i, : heads // ns] for i in range(3))
    g_pre, g_og = g_pre[0], g_og[0]

    return (
        activations[None, :, None],
        input_grads[None, :, None],
        grad_in[None],
        grad_dt[None],
        grad_out[None],
        g_cw[None],
        g_cb[None],
        g_dtb[None],
        g_alg[None],
        g_dsk[None],
        g_pre[None],
        g_og[None],
    )


def solution(mesh):
    shard1 = P("section", "shard")
    shard2 = P("section", "shard", None)
    tokens = P("section", None, ("shard", "rep"), None, None)
    taps = P("section", None, "shard")
    weights = (shard2, shard2, shard2, taps, shard1, shard1, shard1, shard1, shard1, shard1)
    return jax.shard_map(
        on_device,
        mesh=mesh,
        in_specs=(tokens, P(None, ("shard", "rep"))) + weights,
        out_specs=(tokens, tokens) + weights,
        check_vma=False,
    )
```

```python
import functools

import jax
import jax.numpy as jnp
from jax import lax
from jax.experimental import pallas as pl
from jax.experimental.pallas import tpu as pltpu
from jax.sharding import PartitionSpec as P


BF = jnp.bfloat16
F32 = jnp.float32
HIGH = lax.Precision.HIGHEST
EPSILON = 1e-05
CHUNK = 128
LANES = 128
PAIR = 2


def mm(a, b):
    return jnp.dot(a.astype(BF), b.astype(BF), preferred_element_type=F32)


def mm_t(a, b):
    return lax.dot_general(a.astype(BF), b.astype(BF), (((1,), (1,)), ((), ())), preferred_element_type=F32)


def t_mm(a, b):
    return lax.dot_general(a.astype(BF), b.astype(BF), (((0,), (0,)), ((), ())), preferred_element_type=F32)


def rows_of(shape):
    return lax.broadcasted_iota(jnp.int32, shape, 0)


def lanes_of(shape):
    return lax.broadcasted_iota(jnp.int32, shape, 1)


def shift_down(v, steps):
    return jnp.where(rows_of(v.shape) >= steps, pltpu.roll(v, steps, 0), 0.0)


def shift_up(v, steps):
    size = v.shape[0]
    return jnp.where(rows_of(v.shape) < size - steps, pltpu.roll(v, size - steps, 0), 0.0)


def conv(v, taps_ref, taps):
    total = taps_ref[taps : taps + 1, :] + taps_ref[taps - 1 : taps, :] * v
    for k in range(taps - 1):
        total = total + taps_ref[k : k + 1, :] * shift_down(v, taps - 1 - k)
    return total


def conv_back(d_sum, v, taps_ref, taps):
    d_v = taps_ref[taps - 1 : taps, :] * d_sum
    d_taps = []
    for k in range(taps - 1):
        d_v = d_v + taps_ref[k : k + 1, :] * shift_up(d_sum, taps - 1 - k)
        d_taps.append(jnp.sum(d_sum * shift_down(v, taps - 1 - k), axis=0, keepdims=True))
    d_taps.append(jnp.sum(d_sum * v, axis=0, keepdims=True))
    d_taps.append(jnp.sum(d_sum, axis=0, keepdims=True))
    return d_v, d_taps


def head_map(width, head_dim):
    shape = (LANES, width)
    return (rows_of(shape) == lanes_of(shape) // head_dim).astype(BF)


def expand(v, spread):
    high = v.astype(BF)
    low = (v - high.astype(F32)).astype(BF)
    return mm(high, spread) + mm(low, spread)


def step_of(dt, ph_ref):
    pre = dt + ph_ref[0:1, :]
    step = jnp.maximum(pre, 0.0) + jnp.log1p(jnp.exp(-jnp.abs(pre)))
    rate = -jnp.exp(ph_ref[1:2, :])
    return pre, step, rate


def lower_mask():
    shape = (CHUNK, CHUNK)
    return rows_of(shape) >= lanes_of(shape)


def pair_rows(v, first):
    return jnp.concatenate([jnp.where(first, v, 0.0), jnp.where(first, 0.0, v)], axis=0)


def as_row(column):
    return jnp.broadcast_to(column, (CHUNK, LANES)).T[0:1, :]


def as_column(row):
    return jnp.broadcast_to(row, (CHUNK, LANES)).T[:, 0:1]


def forward_kernel(px_ref, pbc_ref, ph_ref, gate_ref, x_ref, bcdt_ref, *refs, taps, heads, with_dots):
    if with_dots:
        dmix_ref, gg_ref, y_ref, st_ref, ss_ref, dot_ref = refs
    else:
        gg_ref, y_ref, st_ref, ss_ref = refs
    width = x_ref.shape[1]
    head_dim = width // heads
    states = pbc_ref.shape[1] // 2
    spread = head_map(width, head_dim)
    bcdt = bcdt_ref[...].astype(F32)
    sums = conv(bcdt[:, : 2 * states], pbc_ref, taps)
    bc = sums * jax.nn.sigmoid(sums)
    _, step, rate = step_of(bcdt[:, 2 * states :], ph_ref)
    decay = rate * step
    sums = conv(x_ref[...].astype(F32), px_ref, taps)
    act = sums * jax.nn.sigmoid(sums)
    xs = act * expand(step, spread)
    lower = lower_mask()
    tri = lower.astype(F32)
    first = lanes_of((CHUNK, 2 * head_dim)) < head_dim
    state = None
    chunks = x_ref.shape[0] // CHUNK
    for c in range(chunks):
        span = slice(c * CHUNK, (c + 1) * CHUNK)
        cum = jnp.dot(tri, decay[span], precision=HIGH, preferred_element_type=F32)
        cum_t = cum.T
        b_c = bc[span, :states].astype(BF)
        c_c = bc[span, states:].astype(BF)
        scores = mm_t(c_c, b_c)
        xs_c = xs[span]
        pieces = []
        for p in range(heads // 2):
            two = slice(p * 2 * head_dim, (p + 1) * 2 * head_dim)
            mixes = []
            for h in (2 * p, 2 * p + 1):
                gap = jnp.minimum(cum[:, h : h + 1] - cum_t[h : h + 1, :], 0.0)
                mixes.append(jnp.where(lower, jnp.exp(gap) * scores, 0.0).astype(BF))
            pieces.append(mm(jnp.concatenate(mixes, axis=1), pair_rows(xs_c[:, two], first)))
        y = jnp.concatenate(pieces, axis=1)
        if c > 0:
            y = y + mm(c_c, state) * expand(jnp.exp(cum), spread)
        if c + 1 < chunks:
            last = cum[CHUNK - 1 : CHUNK, :]
            fresh = t_mm(b_c, xs_c * expand(jnp.exp(last - cum), spread))
            state = fresh if c == 0 else fresh + state * expand(jnp.exp(jnp.broadcast_to(last, (states, LANES))), spread)
            st_ref[c] = state
        y = y + px_ref[taps + 1 : taps + 2, :] * act[span]
        y_low = y.astype(BF)
        y_ref[span, :] = y_low
        y = y_low.astype(F32)
        gate = gate_ref[span, :].astype(F32)
        gated = y * (gate * jax.nn.sigmoid(gate))
        ss_ref[c : c + 1, :] = as_row(jnp.sum(gated * gated, axis=1, keepdims=True))
        gg = gated * px_ref[taps + 2 : taps + 3, :]
        gg_ref[span, :] = gg.astype(BF)
        if with_dots:
            dot_ref[c : c + 1, :] = as_row(jnp.sum(gg * dmix_ref[span, :].astype(F32), axis=1, keepdims=True))


def backward_kernel(
    px_ref, pbc_ref, ph_ref, gate_ref, x_ref, bcdt_ref, y_ref, st_ref, dmix_ref, sc_ref,
    dgate_ref, dx_ref, dbcdt_ref, small_ref, *, taps, heads,
):
    length, width = x_ref.shape
    head_dim = width // heads
    states = pbc_ref.shape[1] // 2
    spread = head_map(width, head_dim)

    @pl.when(pl.program_id(0) == 0)
    def _():
        small_ref[...] = jnp.zeros_like(small_ref)

    gx_ref = small_ref.at[:, :width]
    gbc_ref = small_ref.at[:, width : width + 2 * states]
    gh_ref = small_ref.at[:, width + 2 * states :]

    gate = gate_ref[...].astype(F32)
    y = y_ref[...].astype(F32)
    dmix = dmix_ref[...].astype(F32)
    chunks = length // CHUNK
    r = jnp.concatenate([as_column(sc_ref[c : c + 1, :]) for c in range(chunks)], axis=0)
    coef = jnp.concatenate([as_column(sc_ref[chunks + c : chunks + c + 1, :]) for c in range(chunks)], axis=0)
    sig = jax.nn.sigmoid(gate)
    gated = y * gate * sig
    gx_ref[taps + 2 : taps + 3, :] += jnp.sum(dmix * gated * r, axis=0, keepdims=True)
    dgated = r * px_ref[taps + 2 : taps + 3, :] * dmix - coef * gated
    dgate_ref[...] = (dgated * y * (sig * (1.0 + gate * (1.0 - sig)))).astype(BF)
    dy = dgated * gate * sig

    bcdt = bcdt_ref[...].astype(F32)
    bc_in = bcdt[:, : 2 * states]
    bc_sum = conv(bc_in, pbc_ref, taps)
    bc_sig = jax.nn.sigmoid(bc_sum)
    bc = bc_sum * bc_sig
    pre, step, rate = step_of(bcdt[:, 2 * states :], ph_ref)
    decay = rate * step
    x_in = x_ref[...].astype(F32)
    x_sum = conv(x_in, px_ref, taps)
    x_sig = jax.nn.sigmoid(x_sum)
    act = x_sum * x_sig
    step_wide = expand(step, spread)
    xs = act * step_wide
    gx_ref[taps + 1 : taps + 2, :] += jnp.sum(dy * act, axis=0, keepdims=True)

    lower = lower_mask()
    tri = lower.astype(F32)
    upper = (rows_of((CHUNK, CHUNK)) <= lanes_of((CHUNK, CHUNK))).astype(F32)
    last_row = rows_of((CHUNK, LANES)) == CHUNK - 1
    head_lane = lanes_of((CHUNK, LANES))
    head_row = rows_of((LANES, CHUNK))
    first = lanes_of((CHUNK, 2 * head_dim)) < head_dim
    d_state = None
    d_xs, d_bc, d_decay = [None] * chunks, [None] * chunks, [None] * chunks
    for c in reversed(range(chunks)):
        span = slice(c * CHUNK, (c + 1) * CHUNK)
        cum = jnp.dot(tri, decay[span], precision=HIGH, preferred_element_type=F32)
        cum_t = cum.T
        b_c = bc[span, :states].astype(BF)
        c_c = bc[span, states:].astype(BF)
        xs_c = xs[span]
        dy_c = dy[span]
        scores = mm_t(c_c, b_c)
        d_scores = jnp.zeros((CHUNK, CHUNK), F32)
        by_row = jnp.zeros((CHUNK, LANES), F32)
        by_col = jnp.zeros((LANES, CHUNK), F32)
        pieces = []
        for p in range(heads // 2):
            two = slice(p * 2 * head_dim, (p + 1) * 2 * head_dim)
            dy_two = pair_rows(dy_c[:, two], first).astype(BF)
            d_mix = mm_t(dy_two, xs_c[:, two])
            mixes = []
            for i, h in enumerate((2 * p, 2 * p + 1)):
                gap = jnp.minimum(cum[:, h : h + 1] - cum_t[h : h + 1, :], 0.0)
                fall = jnp.where(lower, jnp.exp(gap), 0.0)
                mixes.append((fall * scores).astype(BF))
                d_fall = d_mix[i * CHUNK : (i + 1) * CHUNK] * fall
                d_scores = d_scores + d_fall
                both = d_fall * scores
                by_row = jnp.where(head_lane == h, jnp.sum(both, axis=1, keepdims=True), by_row)
                by_col = jnp.where(head_row == h, jnp.sum(both, axis=0, keepdims=True), by_col)
            pieces.append(t_mm(jnp.concatenate(mixes, axis=0), dy_two))
        d_xs_c = jnp.concatenate(pieces, axis=1)
        d_c = mm(d_scores, b_c)
        d_b = t_mm(d_scores, c_c)
        d_cum = by_row - by_col.T
        new_state = None
        if c > 0:
            before = st_ref[c - 1]
            grow = expand(jnp.exp(cum), spread)
            d_off = dy_c * grow
            new_state = t_mm(c_c, d_off)
            d_c = d_c + mm_t(d_off, before)
            d_cum = d_cum + mm_t(d_off * mm(c_c, before), spread)
        if c + 1 < chunks:
            last = cum[CHUNK - 1 : CHUNK, :]
            tail = expand(jnp.exp(last - cum), spread)
            tailed = xs_c * tail
            d_tailed = mm(b_c, d_state)
            d_b = d_b + mm_t(tailed, d_state)
            d_xs_c = d_xs_c + d_tailed * tail
            lost = mm_t(d_tailed * tailed, spread)
            d_last = jnp.sum(lost, axis=0, keepdims=True)
            if c > 0:
                whole = expand(jnp.exp(jnp.broadcast_to(last, (states, LANES))), spread)
                d_last = d_last + jnp.sum(mm_t(d_state * before * whole, spread), axis=0, keepdims=True)
                new_state = new_state + d_state * whole
            d_cum = d_cum - lost + jnp.where(last_row, d_last, 0.0)
        d_state = new_state
        d_xs[c] = d_xs_c
        d_bc[c] = jnp.concatenate([d_b, d_c], axis=1)
        d_decay[c] = jnp.dot(upper, d_cum, precision=HIGH, preferred_element_type=F32)
    d_xs = jnp.concatenate(d_xs, axis=0)
    d_bc = jnp.concatenate(d_bc, axis=0)
    d_decay = jnp.concatenate(d_decay, axis=0)

    d_step = mm_t(act * d_xs, spread) + d_decay * rate
    gh_ref[1:2, :] += jnp.sum(d_decay * decay, axis=0, keepdims=True)
    d_dt = d_step * jax.nn.sigmoid(pre)
    gh_ref[0:1, :] += jnp.sum(d_dt, axis=0, keepdims=True)

    d_act = dy * px_ref[taps + 1 : taps + 2, :] + d_xs * step_wide
    d_sum = d_act * (x_sig * (1.0 + x_sum * (1.0 - x_sig)))
    d_x, d_taps = conv_back(d_sum, x_in, px_ref, taps)
    dx_ref[...] = d_x.astype(BF)
    for k, value in enumerate(d_taps):
        gx_ref[k : k + 1, :] += value
    d_sum = d_bc * (bc_sig * (1.0 + bc_sum * (1.0 - bc_sig)))
    d_bc_in, d_taps = conv_back(d_sum, bc_in, pbc_ref, taps)
    for k, value in enumerate(d_taps):
        gbc_ref[k : k + 1, :] += value
    dbcdt_ref[:, : 2 * states] = d_bc_in.astype(BF)
    dbcdt_ref[:, 2 * states :] = d_dt.astype(BF)


def per_seq(*dims):
    return pl.BlockSpec((None,) + dims, lambda i: (i,) + (0,) * len(dims))


def fixed(*dims):
    return pl.BlockSpec(dims, lambda i: (0,) * len(dims))


PARAMS = pltpu.CompilerParams(dimension_semantics=("arbitrary",), vmem_limit_bytes=18 << 20)


def run_forward(small, gate, x, bcdt, dmix, taps, heads):
    px, pbc, ph = small
    seqs, length, width = x.shape
    states = pbc.shape[1] // 2
    chunks = length // CHUNK
    more = [] if dmix is None else [dmix]
    sums = [jax.ShapeDtypeStruct((seqs, chunks, LANES), F32)] * (1 + len(more))
    return pl.pallas_call(
        functools.partial(forward_kernel, taps=taps, heads=heads, with_dots=bool(more)),
        grid=(seqs,),
        in_specs=[fixed(*px.shape), fixed(*pbc.shape), fixed(*ph.shape), per_seq(length, width), per_seq(length, width), per_seq(length, bcdt.shape[2])]
        + [per_seq(length, width)] * len(more),
        out_specs=[per_seq(length, width), per_seq(length, width), per_seq(chunks - 1, states, width)] + [per_seq(chunks, LANES)] * len(sums),
        out_shape=[
            jax.ShapeDtypeStruct((seqs, length, width), BF),
            jax.ShapeDtypeStruct((seqs, length, width), BF),
            jax.ShapeDtypeStruct((seqs, chunks - 1, states, width), F32),
        ]
        + sums,
        compiler_params=PARAMS,
        cost_estimate=pl.CostEstimate(flops=seqs * 400_000_000, bytes_accessed=seqs * 4_000_000, transcendentals=seqs * 2_000_000),
        name="mix_forward",
    )(px, pbc, ph, gate, x, bcdt, *more)


def run_backward(small, gate, x, bcdt, y, state, dmix, scalars, taps, heads):
    px, pbc, ph = small
    seqs, length, width = x.shape
    smalls = px.shape[1] + pbc.shape[1] + ph.shape[1]
    return pl.pallas_call(
        functools.partial(backward_kernel, taps=taps, heads=heads),
        grid=(seqs,),
        in_specs=[
            fixed(*px.shape), fixed(*pbc.shape), fixed(*ph.shape), per_seq(length, width), per_seq(length, width),
            per_seq(length, bcdt.shape[2]), per_seq(length, width), per_seq(*state.shape[1:]), per_seq(length, width), per_seq(*scalars.shape[1:]),
        ],
        out_specs=[per_seq(length, width), per_seq(length, width), per_seq(length, bcdt.shape[2]), fixed(8, smalls)],
        out_shape=[
            jax.ShapeDtypeStruct((seqs, length, width), BF),
            jax.ShapeDtypeStruct((seqs, length, width), BF),
            jax.ShapeDtypeStruct((seqs, length, bcdt.shape[2]), BF),
            jax.ShapeDtypeStruct((8, smalls), F32),
        ],
        compiler_params=PARAMS,
        cost_estimate=pl.CostEstimate(flops=seqs * 1_200_000_000, bytes_accessed=seqs * 6_000_000, transcendentals=seqs * 4_000_000),
        name="mix_backward",
    )(px, pbc, ph, gate, x, bcdt, y, state, dmix, scalars)


MESH = pl.DeviceIdType.MESH
VM = pl.BlockSpec(memory_space=pltpu.VMEM)


def partners():
    section = lax.axis_index("section")
    rep = lax.axis_index("rep")
    xb = rep % PAIR
    return section, xb, {"section": 1 - section}, {"rep": rep + 1 - 2 * xb}


def greet(*devices):
    barrier = pltpu.get_barrier_semaphore()
    for device in devices:
        pl.semaphore_signal(barrier, inc=1, device_id=device, device_id_type=MESH)
    pl.semaphore_wait(barrier, len(devices))


def remote(src, dst, send, recv, device):
    return pltpu.make_async_remote_copy(src_ref=src, dst_ref=dst, send_sem=send, recv_sem=recv, device_id=device, device_id_type=MESH)


def sums_kernel(v_ref, out_ref, got_ref, half_ref, send, recv):
    _, _, peer, beside = partners()
    greet(peer, beside)
    first = remote(v_ref, got_ref.at[0], send.at[0], recv.at[0], peer)
    first.start()
    first.wait()
    half_ref[...] = v_ref[...] + got_ref[0]
    second = remote(half_ref, got_ref.at[1], send.at[1], recv.at[1], beside)
    second.start()
    second.wait()
    out_ref[...] = half_ref[...] + got_ref[1]


def run_sums(v, collective_id):
    return pl.pallas_call(
        sums_kernel,
        in_specs=[VM],
        out_specs=VM,
        out_shape=jax.ShapeDtypeStruct(v.shape, F32),
        scratch_shapes=[pltpu.VMEM((2,) + v.shape, F32), pltpu.VMEM(v.shape, F32), pltpu.SemaphoreType.DMA((2,)), pltpu.SemaphoreType.DMA((2,))],
        compiler_params=comm_params(collective_id, 8),
        cost_estimate=pl.CostEstimate(flops=10_000_000, bytes_accessed=20_000_000, transcendentals=0),
        name="token_sums",
    )(v)


def exchange(part_ref, got_a, held, got_x, send, recv, use):
    section, _, peer, beside = partners()
    per = part_ref.shape[1] // CHUNK
    steps = PAIR * per

    def at(i):
        return i // per, pl.ds(pl.multiple_of(i % per * CHUNK, CHUNK), CHUNK)

    def to_peer(i):
        x, span = at(i)
        return remote(part_ref.at[x * 2 + 1 - section, span], got_a.at[i], send.at[0, i], recv.at[0, i], peer)

    def to_beside(i):
        return remote(held.at[i], got_x.at[i], send.at[1, i], recv.at[1, i], beside)

    def start_peer(i, _):
        to_peer(i).start()
        return 0

    def add(i, _):
        to_peer(i).wait_recv()
        x, span = at(i)
        held[i] = (part_ref[x * 2 + section, span].astype(F32) + got_a[i].astype(F32)).astype(BF)

        @pl.when(i > 0)
        def _():
            to_beside(i - 1).start()

        return 0

    def finish(i):
        to_beside(i).wait_recv()
        x, span = at(i)
        use(i, x, span, held[i].astype(F32) + got_x[i].astype(F32))

    def drain(i, _):
        to_peer(i).wait_send()
        to_beside(i).wait_send()
        return 0

    lax.fori_loop(0, steps, start_peer, 0)
    yield
    lax.fori_loop(0, steps, add, 0)
    yield
    to_beside(steps - 1).start()
    yield
    for i in range(steps):
        finish(i)
        yield
    lax.fori_loop(0, steps, drain, 0)


def weights_flow(b, q_ref, o_ref, w_in, w_out, qs, qr, os_, or_, *, ns, ny, split=False):
    section, xb, peer, _ = partners()
    z = lax.axis_index("shard")
    yb = lax.axis_index("rep") // PAIR
    half = ns // 2
    part = q_ref.shape[2] // PARTS
    home = z // half

    def y_peer(k):
        return {"rep": (yb + k) % ny * PAIR + xb}

    def rows_at(h):
        return pl.ds(h * part, part)

    def there(way):
        return z < ns - 1 if way > 0 else z > 0

    def first(src, way, h):
        return remote(src, w_in.at[yb, z, rows_at(h)], qs.at[0, (way + 1) // 2, h], qr.at[yb, z, h], {"shard": z + way})

    def chip(j, h):
        return remote(q_ref.at[1 - b, j, rows_at(h)], w_in.at[j, z, rows_at(h)], qs.at[1, j, h], qr.at[j, z, h], peer)

    def stay(j, h):
        return pltpu.make_async_copy(q_ref.at[b, j, rows_at(h)], w_in.at[j, z, rows_at(h)], qs.at[2 + ny, j, h])

    def onward(place, way, h):
        block = w_in.at[yb, place, rows_at(h)]
        return remote(block, block, qs.at[2, place, h], qr.at[yb, place, h], {"shard": z + way})

    def across(place, k, h):
        block = w_in.at[yb, place, rows_at(h)]
        return remote(block, block, qs.at[2 + k, place, h], qr.at[yb, place, h], y_peer(k))

    def arrival(j, place, h):
        block = w_in.at[j, place, rows_at(h)]
        return remote(block, block, qs.at[2, place, h], qr.at[j, place, h], peer)

    def o_first(src, way):
        return remote(src, w_out.at[z % half, yb], os_.at[0, (way + 1) // 2], or_.at[z % half, yb], {"shard": z + way})

    def o_chip(j):
        return remote(o_ref.at[j], w_out.at[z % half, j], os_.at[1, j], or_.at[z % half, j], peer)

    def o_stay(j):
        return pltpu.make_async_copy(o_ref.at[j], w_out.at[z % half, j], os_.at[1, j])

    def o_onward(k, way):
        block = w_out.at[k, yb]
        return remote(block, block, os_.at[2, k], or_.at[k, yb], {"shard": z + way})

    def o_across(k, i):
        block = w_out.at[k, yb]
        return remote(block, block, os_.at[2 + i, k], or_.at[k, yb], y_peer(i))

    def o_arrival(k, j):
        block = w_out.at[k, j]
        return remote(block, block, os_.at[2, k], or_.at[k, j], peer)

    def along(copy):
        for way in (1, -1):
            @pl.when(there(way))
            def _():
                copy(way).start()

    def start():
        @pl.when(section == b)
        def _():
            for h in range(PARTS):
                chip(yb, h).start()

            @pl.when(home != b)
            def _():
                o_chip(yb).start()

            for h in range(PARTS):
                along(lambda way: first(q_ref.at[b, yb, rows_at(h)], way, h))

            @pl.when(home == b)
            def _():
                along(lambda way: o_first(o_ref.at[yb], way))

            for k in range(ny):
                j = (yb + k) % ny
                for h in range(PARTS):
                    if k:
                        chip(j, h).start()
                    stay(j, h).start()

                @pl.when(home == b)
                def _():
                    o_stay(j).start()

                if k:
                    @pl.when(home != b)
                    def _():
                        o_chip(j).start()

        @pl.when(section != b)
        def _():
            for h in range(PARTS):
                arrival(yb, z, h).wait_recv()
                along(lambda way: first(w_in.at[yb, z, rows_at(h)], way, h))

            @pl.when(home != b)
            def _():
                o_arrival(z % half, yb).wait_recv()
                along(lambda way: o_first(w_out.at[z % half, yb], way))

    def relay_in(d, h=None):
        for h in range(PARTS) if h is None else (h,):
            for way in (1, -1):
                place = z - way * d

                @pl.when((place >= 0) & (place < ns))
                def _():
                    arrival(yb, place, h).wait_recv()

                    @pl.when(there(way))
                    def _():
                        onward(place, way, h).start()

                    for k in range(1, ny):
                        across(place, k, h).start()

    def relay_out(d):
        for way in (1, -1):
            place = z - way * d
            k = place - section * half

            @pl.when((place >= 0) & (place < ns) & (k >= 0) & (k < half))
            def _():
                o_arrival(k, yb).wait_recv()

                @pl.when(there(way))
                def _():
                    o_onward(k, way).start()

                for i in range(1, ny):
                    o_across(k, i).start()

    def finish_in():
        for place in range(ns):
            @pl.when(place != z)
            def _():
                for h in range(PARTS):
                    for k in range(1, ny):
                        arrival((yb + k) % ny, place, h).wait_recv()
                        across(place, k, h).wait_send()

                    @pl.when(jnp.where(place < z, z < ns - 1, z > 0))
                    def _():
                        onward(place, 1, h).wait_send()

        for way in (1, -1):
            @pl.when(there(way))
            def _():
                for h in range(PARTS):
                    first(w_in.at[yb, z, rows_at(h)], way, h).wait_send()

        @pl.when(section != b)
        def _():
            for k in range(1, ny):
                for h in range(PARTS):
                    arrival((yb + k) % ny, z, h).wait_recv()

        @pl.when(section == b)
        def _():
            for j in range(ny):
                for h in range(PARTS):
                    chip(j, h).wait_send()
                    stay(j, h).wait()

    def finish_out():
        @pl.when((section != b) & (home != b))
        def _():
            for k in range(1, ny):
                o_arrival(z % half, (yb + k) % ny).wait_recv()

        @pl.when(section == home)
        def _():
            for way in (1, -1):
                @pl.when(there(way))
                def _():
                    o_first(w_out.at[z % half, yb], way).wait_send()

        for k in range(half):
            place = section * half + k

            @pl.when(place != z)
            def _():
                for i in range(1, ny):
                    o_arrival(k, (yb + i) % ny).wait_recv()
                    o_across(k, i).wait_send()

                @pl.when(jnp.where(place < z, z < ns - 1, z > 0))
                def _():
                    o_onward(k, 1).wait_send()

        @pl.when(section == b)
        def _():
            for j in range(ny):
                @pl.when(home == b)
                def _():
                    o_stay(j).wait()

                @pl.when(home != b)
                def _():
                    o_chip(j).wait_send()

    def relay(d):
        relay_in(d)
        relay_out(d)

    def finish():
        finish_in()
        finish_out()

    if split:
        return start, relay_in, relay_out, finish
    return start, relay, finish


def weights_shapes(q, o, ns):
    ny = q.shape[1]
    outs = [
        jax.ShapeDtypeStruct((ny, ns) + q.shape[2:], BF),
        jax.ShapeDtypeStruct((ns // 2,) + o.shape, BF),
    ]
    dma = pltpu.SemaphoreType.DMA
    sems = [dma((3 + ny, max(ns, 4), PARTS)), dma((ny, ns, PARTS)), dma((2 + ny, max(ns, 2))), dma((ns // 2, ny))]
    return outs, sems


def greet_line(ns, ny):
    section, xb, peer, beside = partners()
    z = lax.axis_index("shard")
    yb = lax.axis_index("rep") // PAIR
    found = [peer, beside] + [{"rep": (yb + k) % ny * PAIR + xb} for k in range(1, ny)]
    for k in (1, ns - 1):
        found += [{"shard": (z + k) % ns}, {"section": 1 - section, "shard": (z + k) % ns}]
    greet(*found)


def start_kernel(tokens_ref, counts_ref, cw_ref, cb_ref, dtb_ref, alg_ref, dsk_ref, pgn_ref, ogn_ref, bc_ref, dt_ref, q_ref, o_ref,
                 all_tokens, normed_ref, live_out_ref, live_ref, px_ref, pbc_ref, ph_ref, gain_ref, wbc_ref, w_in, w_out,
                 small, all_small, mine, packs, full, row8, all_counts,
                 qs, qr, os_, or_, ts, tr, ss, sr, ps, pr, cs, cr, *, ns, ny, taps, heads):
    section, xb, peer, beside = partners()
    z = lax.axis_index("shard")
    yb = lax.axis_index("rep") // PAIR
    half = ns // 2
    greet_all(ns, ny)
    start, relay, finish = weights_flow(0, q_ref, o_ref, w_in, w_out, qs, qr, os_, or_, ns=ns, ny=ny)

    part = cw_ref.shape[1]
    mine[...] = jnp.zeros_like(mine)
    unit3 = LANES
    mine[0:taps, :part] = cw_ref[...].astype(F32)
    mine[taps : taps + 1, :part] = cb_ref[...].astype(F32)
    for i, ref in enumerate((pgn_ref, ogn_ref)):
        mine[taps + 1 + i : taps + 2 + i, : ref.shape[1]] = ref[...].astype(F32)
    for i, ref in enumerate((dtb_ref, alg_ref, dsk_ref)):
        mine[taps + 3 : taps + 4, i * unit3 : i * unit3 + ref.shape[1]] = ref[...].astype(F32)

    def pack_to(k):
        return remote(mine, packs.at[section, z], ps.at[0, k], pr.at[section, z], {"shard": (z + k) % ns})

    def pack_chip(place):
        return remote(packs.at[section, place], packs.at[section, place], ps.at[1, place], pr.at[section, place], peer)

    def pack_from(t, place):
        return remote(mine, packs.at[t, place], ps.at[0, 0], pr.at[t, place], peer)

    counts = remote(counts_ref, all_counts.at[xb], cs, cr, beside)
    counts.start()
    for k in range(1, ns):
        pack_to(k).start()
    remote(mine, packs.at[section, z], ps.at[0, 0], pr.at[section, z], peer).start()
    packs[section, z] = mine[...]
    all_counts[xb] = counts_ref[...]

    def there(way):
        return z < ns - 1 if way > 0 else z > 0

    lanes = bc_ref.shape[1]
    rows = bc_ref.shape[0] // ny
    for j in range(ny):
        small[j] = jnp.zeros_like(small[j])
        small[j, :, :lanes] = bc_ref[j * rows : (j + 1) * rows]
        small[j, :, lanes : lanes + heads] = dt_ref[j * rows : (j + 1) * rows]

    def first(way):
        return remote(small.at[yb], all_small.at[section, z, yb], ss.at[0, (way + 1) // 2, 0], sr.at[section, z, yb], {"shard": z + way})

    def held(place, j):
        return all_small.at[section, place, j]

    def onward(place, way):
        return remote(held(place, yb), held(place, yb), ss.at[1, place, 0], sr.at[section, place, yb], {"shard": z + way})

    def across(place, k):
        return remote(held(place, yb), held(place, yb), ss.at[1 + k, place, 0], sr.at[section, place, yb], {"rep": (yb + k) % ny * PAIR + xb})

    def chip(place, j):
        return remote(held(place, j), held(place, j), ss.at[1 + ny, place, j], sr.at[section, place, j], peer)

    def arrival(b, place, j):
        return remote(all_small.at[b, place, j], all_small.at[b, place, j], ss.at[1, place, 0], sr.at[b, place, j], peer)

    for way in (1, -1):
        @pl.when(there(way))
        def _():
            first(way).start()

    def tokens_beside(m):
        return remote(tokens_ref.at[m], all_tokens.at[section, xb, m], ts.at[0, m], tr.at[section, xb, m], beside)

    def tokens_chip(x, m):
        if x is None:
            return remote(tokens_ref.at[m], all_tokens.at[section, xb, m], ts.at[1, m], tr.at[section, xb, m], peer)
        place = all_tokens.at[section, x, m]
        return remote(place, place, ts.at[2, m], tr.at[section, x, m], peer)

    def tokens_arrival(b, x, m):
        place = all_tokens.at[b, x, m]
        return remote(place, place, ts.at[0, m], tr.at[b, x, m], peer)

    micro, seq_len, _ = tokens_ref.shape
    start()
    for m in range(micro):
        tokens_beside(m).start()
        tokens_chip(None, m).start()
        all_tokens[section, xb, m] = tokens_ref[m]
    for j in range(ny):
        all_small[section, z, j] = small[j]

    def relay_small(d):
        for way in (1, -1):
            place = z - way * d

            @pl.when((place >= 0) & (place < ns))
            def _():
                arrival(section, place, yb).wait_recv()

                @pl.when(there(way))
                def _():
                    onward(place, way).start()

                for k in range(1, ny):
                    across(place, k).start()
                chip(place, yb).start()

    def unpack():
        channels = part * ns
        inner = ogn_ref.shape[1] * ns
        cw = inner // ns // PAIR
        unit = dtb_ref.shape[1] // PAIR
        mine_w = half * cw
        for place in range(ns):
            pack_from(1 - section, place).wait_recv()
        ph_ref[...] = jnp.zeros_like(ph_ref)
        px_ref[...] = jnp.zeros_like(px_ref)
        pbc_ref[...] = jnp.zeros_like(pbc_ref)
        spread = head_map(mine_w, 2 * PAIR * mine_w // heads)
        for b in range(2):
            for at in range(ns):
                full[0 : taps + 1, at * part : (at + 1) * part] = packs[b, at, 0 : taps + 1, :part]
                size = pgn_ref.shape[1]
                gain_ref[b, :, at * size : (at + 1) * size] = packs[b, at, taps + 1 : taps + 2, :size]
            pbc_ref[b, 0 : taps + 1, :] = full[0 : taps + 1, inner:channels]
            row8[...] = jnp.zeros_like(row8)
            for t in range(2):
                for q in range(PAIR):
                    @pl.when((section == t) & (xb == q))
                    def _():
                        for k in range(half):
                            at = t * half + k
                            col = (at * PAIR + q) * cw
                            put = slice(k * cw, (k + 1) * cw)
                            lane = slice(k * unit, (k + 1) * unit)
                            take = slice(q * unit, (q + 1) * unit)
                            px_ref[b, 0 : taps + 1, put] = full[0 : taps + 1, col : col + cw]
                            px_ref[b, taps + 2 : taps + 3, put] = packs[b, at, taps + 2 : taps + 3, q * cw : (q + 1) * cw]
                            ph_ref[b, 0:1, lane] = packs[b, at, taps + 3 : taps + 4, take]
                            ph_ref[b, 1:2, lane] = packs[b, at, taps + 3 : taps + 4, unit3 + q * unit : unit3 + (q + 1) * unit]
                            row8[0:1, lane] = packs[b, at, taps + 3 : taps + 4, 2 * unit3 + q * unit : 2 * unit3 + (q + 1) * unit]
            px_ref[b, taps + 1 : taps + 2, :] = mm(row8[...], spread)[0:1]

    def shared_columns():
        unit = dtb_ref.shape[1] // PAIR
        shape = (wbc_ref.shape[2] - lanes, LANES)
        source, head = rows_of(shape), lanes_of(shape)
        wanted = ((section * half + head // unit) * PAIR + xb) * unit + head % unit
        chosen = ((source == wanted) & (head < half * unit)).astype(BF)
        for b in range(2):
            for at in range(ns):
                for j in range(ny):
                    low = (at * ny + j) * rows
                    wbc_ref[b, low : low + rows, :lanes] = all_small[b, at, j, :, :lanes]
                    wbc_ref[b, low : low + rows, lanes:] = mm(all_small[b, at, j, :, lanes:], chosen).astype(BF)

    def prepare():
        per = seq_len // CHUNK
        for x in range(PAIR):
            for m in range(micro):
                for c in range(per):
                    row = (x * micro + m) * per + c
                    at = lanes_of((1, LANES)).astype(F32) + float(c * CHUNK)
                    live_ref[row : row + 1, :] = (at < all_counts[x, m : m + 1, :]).astype(F32)

        def step(i, _):
            x, m, c = i // (micro * per), i // per % micro, i % per
            span = pl.ds(pl.multiple_of(c * CHUNK, CHUNK), CHUNK)
            wide = all_tokens[0, x, m, span].astype(F32)
            normed_ref[x * micro + m, span] = (wide * rms(wide) * gain_ref[0]).astype(BF)
            live = as_column(live_ref[pl.ds(i, 1), :])
            live_out_ref[x * micro + m, span] = (all_tokens[1, x, m, span].astype(F32) * live).astype(BF)
            return 0

        lax.fori_loop(0, PAIR * micro * per, step, 0)

    relay_small(1)
    for k in range(1, ns):
        pack_from(section, (z + k) % ns).wait_recv()
        pack_chip((z + k) % ns).start()
    for j in range(ny):
        chip(z, j).start()
    for d in range(1, ns):
        if d == ns - 1:
            unpack()
            for m in range(micro):
                tokens_arrival(section, 1 - xb, m).wait_recv()
                tokens_chip(1 - xb, m).start()
            counts.wait_send()
            remote(counts_ref, all_counts.at[1 - xb], cs, cr, beside).wait_recv()
            for m in range(micro):
                for x in range(PAIR):
                    tokens_arrival(1 - section, x, m).wait_recv()
            prepare()
        relay(d)
        if d + 1 < ns:
            relay_small(d + 1)
    for place in range(ns):
        @pl.when(place != z)
        def _():
            for k in range(1, ny):
                j = (yb + k) % ny
                arrival(section, place, j).wait_recv()
                chip(place, j).start()
    for place in range(ns):
        for j in range(ny):
            arrival(1 - section, place, j).wait_recv()
    shared_columns()
    finish()
    for m in range(micro):
        tokens_beside(m).wait_send()
        tokens_chip(None, m).wait_send()
        tokens_chip(1 - xb, m).wait_send()
    for k in range(1, ns):
        pack_to(k).wait_send()
        pack_chip((z + k) % ns).wait_send()
    pack_from(section, z).wait_send()
    for way in (1, -1):
        @pl.when(there(way))
        def _():
            first(way).wait_send()
    for place in range(ns):
        for j in range(ny):
            chip(place, j).wait_send()

        @pl.when(place != z)
        def _():
            for k in range(1, ny):
                across(place, k).wait_send()

            @pl.when(jnp.where(place < z, z < ns - 1, z > 0))
            def _():
                onward(place, 1).wait_send()


def greet_all(ns, ny):
    section, xb, peer, beside = partners()
    z = lax.axis_index("shard")
    yb = lax.axis_index("rep") // PAIR
    found = [peer, beside] + [{"rep": (yb + k) % ny * PAIR + xb} for k in range(1, ny)]
    for k in range(1, ns):
        found += [{"shard": (z + k) % ns}, {"section": 1 - section, "shard": (z + k) % ns}]
    greet(*found)


def run_start(tokens, counts, smalls, bc, dt, q, o, heads):
    conv_weight, _, dt_bias, _, _, _, out_gain = smalls
    ny = q.shape[1]
    ns = heads // dt_bias.shape[1]
    micro, seq_len, width = tokens.shape
    taps = conv_weight.shape[0]
    inner = out_gain.shape[1] * ns
    mine_w = inner // (2 * PAIR)
    states2 = bc.shape[1]
    seqs = PAIR * micro
    outs, sems = weights_shapes(q, o, ns)
    dma = pltpu.SemaphoreType.DMA
    hbm = pl.BlockSpec(memory_space=pl.ANY)
    shape = jax.ShapeDtypeStruct
    rows = bc.shape[0] // ny
    pack = (8, -(-max(conv_weight.shape[1], out_gain.shape[1]) // LANES) * LANES)
    return pl.pallas_call(
        functools.partial(start_kernel, ns=ns, ny=ny, taps=taps, heads=heads),
        in_specs=[VM] * 13,
        out_specs=[VM] * 9 + [hbm, hbm],
        out_shape=[
            shape((2, PAIR) + tokens.shape, BF),
            shape((seqs, seq_len, width), BF),
            shape((seqs, seq_len, width), BF),
            shape((seqs * seq_len // CHUNK, LANES), F32),
            shape((2, 8, mine_w), F32),
            shape((2, 8, states2), F32),
            shape((2, 8, LANES), F32),
            shape((2, 1, width), F32),
            shape((2, width, states2 + LANES), BF),
        ]
        + outs,
        scratch_shapes=[
            pltpu.VMEM((ny, rows, states2 + LANES), BF),
            pltpu.VMEM((2, ns, ny, rows, states2 + LANES), BF),
            pltpu.VMEM(pack, F32),
            pltpu.VMEM((2, ns) + pack, F32),
            pltpu.VMEM((8, conv_weight.shape[1] * ns), F32),
            pltpu.VMEM((8, LANES), F32),
            pltpu.VMEM((PAIR,) + counts.shape, F32),
        ]
        + sems
        + [
            dma((3, 2)), dma((2, PAIR, 2)), dma((2 + ny, max(ns, 2), ny)), dma((2, ns, ny)),
            dma((2, ns)), dma((2, ns)), dma(()), dma(()),
        ],
        compiler_params=comm_params(5, 34),
        cost_estimate=pl.CostEstimate(flops=50_000_000, bytes_accessed=200_000_000, transcendentals=0),
        name="start",
    )(tokens, counts, *smalls, bc, dt, q, o)


def rms(v):
    return lax.rsqrt(jnp.mean(v * v, axis=-1, keepdims=True) + EPSILON)


def spread_out(out_ref, send, recv, peer, per):
    def copy(i, owner):
        span = pl.ds(pl.multiple_of(i % per * CHUNK, CHUNK), CHUNK)
        place = out_ref.at[i // per * 2 + owner, span]
        return remote(place, place, send.at[2, i], recv.at[2, i], peer)

    return copy


def onward_kernel(part_ref, tokens_ref, sums_ref, live_ref, gain_ref, q_ref, o_ref, hidden_ref, normed_ref, rate_ref, gain_out_ref, w_in, w_out,
                  got_a, held, got_x, got_s, half_s, rows_ref, send, recv, send_s, recv_s, rows_s, qs, qr, os_, or_, *, inner, ns, ny):
    section, _, peer, beside = partners()
    per = part_ref.shape[1] // CHUNK
    steps = PAIR * per
    greet_line(ns, ny)
    start, relay_in, relay_out, finish = weights_flow(1, q_ref, o_ref, w_in, w_out, qs, qr, os_, or_, ns=ns, ny=ny, split=True)

    def rows_at(x):
        return pltpu.make_async_copy(tokens_ref.at[0, x, section], rows_ref.at[x], rows_s.at[x])

    for x in range(PAIR):
        rows_at(x).start()
    first = remote(sums_ref, got_s.at[0], send_s.at[0], recv_s.at[0], peer)
    second = remote(half_s, got_s.at[1], send_s.at[1], recv_s.at[1], beside)
    first.start()
    copy = spread_out(hidden_ref, send, recv, peer, per)

    def use(i, x, span, total):
        seq = x * 2 + section
        scale = as_column(rate_ref[pl.ds(seq * per + i % per, 1), :] * live_ref[pl.ds(seq * per + i % per, 1), :])
        gained = scale * total
        gain_out_ref[i] = gained.astype(BF)
        low = (rows_ref[x, span].astype(F32) + gained).astype(BF)
        hidden_ref[seq, span] = low

        @pl.when(i > 0)
        def _():
            copy(i - 1, section).start()

        wide = low.astype(F32)
        normed_ref[seq, span] = (wide * rms(wide) * gain_ref[...]).astype(BF)

    def other(i, _):
        copy(i, section).wait_recv()
        seq = i // per * 2 + 1 - section
        span = pl.ds(pl.multiple_of(i % per * CHUNK, CHUNK), CHUNK)
        wide = hidden_ref[seq, span].astype(F32)
        normed_ref[seq, span] = (wide * rms(wide) * gain_ref[...]).astype(BF)
        return 0

    def drain(i, _):
        copy(i, section).wait_send()
        return 0

    stages = exchange(part_ref, got_a, held, got_x, send, recv, use)
    next(stages)
    first.wait()
    half_s[...] = sums_ref[...] + got_s[0]
    second.start()
    start()
    next(stages)
    next(stages)
    second.wait()
    rate_ref[...] = lax.rsqrt((half_s[...] + got_s[1]) / inner + EPSILON)
    work = [lambda d=d, h=h: relay_in(d, h) if h < PARTS else relay_out(d) for d in range(1, ns) for h in range(PARTS + 1)]

    def relays(count):
        for _ in range(min(count, len(work))):
            work.pop(0)()

    for x in range(PAIR):
        rows_at(x).wait()
    relays(PARTS + 2)
    for _ in range(steps):
        next(stages)
        relays(1)
    copy(steps - 1, section).start()
    lax.fori_loop(0, steps, other, 0)
    for step in work:
        step()
    finish()
    for _ in stages:
        pass
    lax.fori_loop(0, steps, drain, 0)


def back_kernel(part_ref, hidden_ref, tokens_ref, gained_ref, live_ref, gain_ref, out_ref, live_out_ref, dots_ref,
                got_a, held, got_x, dots_own, dots_got, rows_ref, cot_ref, send, recv, send_s, recv_s, rows_s, cot_s):
    section, _, peer, beside = partners()
    per = part_ref.shape[1] // CHUNK
    steps = PAIR * per
    greet(peer, beside)

    def rows_at(x):
        return pltpu.make_async_copy(hidden_ref.at[x * 2 + section], rows_ref.at[x], rows_s.at[x])

    def cot_at(x):
        return pltpu.make_async_copy(tokens_ref.at[1, x, section], cot_ref.at[x], cot_s.at[x])

    for x in range(PAIR):
        rows_at(x).start()
        cot_at(x).start()
    dots_own[...] = jnp.zeros_like(dots_own)
    copy = spread_out(out_ref, send, recv, peer, per)

    def live_of(seq, i):
        return as_column(live_ref[pl.ds(seq * per + i % per, 1), :])

    def use(i, x, span, total):
        seq = x * 2 + section
        rows = rows_ref[x, span].astype(F32)
        inv = rms(rows)
        hat = rows * inv
        d_hat = total * gain_ref[...]
        d_rows = inv * (d_hat - hat * jnp.mean(d_hat * hat, axis=-1, keepdims=True))
        low = (cot_ref[x, span].astype(F32) + d_rows).astype(BF)
        out_ref[seq, span] = low

        @pl.when(i > 0)
        def _():
            copy(i - 1, section).start()

        live = low.astype(F32) * live_of(seq, i)
        live_out_ref[seq, span] = live.astype(BF)
        dots_own[pl.ds(i, 1), :] = as_row(jnp.sum(live * gained_ref[i].astype(F32), axis=1, keepdims=True))

    def other(i, _):
        copy(i, section).wait_recv()
        seq = i // per * 2 + 1 - section
        span = pl.ds(pl.multiple_of(i % per * CHUNK, CHUNK), CHUNK)
        live_out_ref[seq, span] = (out_ref[seq, span].astype(F32) * live_of(seq, i)).astype(BF)
        return 0

    def drain(i, _):
        copy(i, section).wait_send()
        return 0

    stages = exchange(part_ref, got_a, held, got_x, send, recv, use)
    for _ in range(3):
        next(stages)
    for x in range(PAIR):
        rows_at(x).wait()
        cot_at(x).wait()
    for i in range(steps):
        next(stages)
    copy(steps - 1, section).start()
    dots = remote(dots_own, dots_got, send_s.at[0], recv_s.at[0], peer)
    lax.fori_loop(0, steps, other, 0)
    dots.start()
    for _ in stages:
        pass
    lax.fori_loop(0, steps, drain, 0)
    dots.wait()
    for x in range(PAIR):
        for c in range(per):
            i = x * per + c
            dots_ref[pl.ds((x * 2 + section) * per + c, 1), :] = dots_own[i : i + 1, :]
            dots_ref[pl.ds((x * 2 + 1 - section) * per + c, 1), :] = dots_got[i : i + 1, :]


def exchange_scratch(part):
    steps = PAIR * part.shape[1] // CHUNK
    block = (steps, CHUNK, part.shape[2])
    return [pltpu.VMEM(block, BF)] * 3, [pltpu.SemaphoreType.DMA((3, steps)), pltpu.SemaphoreType.DMA((3, steps))]


def own_rows(part):
    return pltpu.VMEM((PAIR,) + part.shape[1:], BF)


def comm_params(collective_id, mib=60):
    return pltpu.CompilerParams(collective_id=collective_id, has_side_effects=True, vmem_limit_bytes=mib << 20)


def run_onward(part, rows, sums, live, gain, q, o, inner, ns):
    wide, sems = exchange_scratch(part)
    steps = PAIR * part.shape[1] // CHUNK
    small = pltpu.VMEM(sums.shape, F32)
    ny = q.shape[1]
    outs, more = weights_shapes(q, o, ns)
    return pl.pallas_call(
        functools.partial(onward_kernel, inner=inner, ns=ns, ny=ny),
        in_specs=[VM, pl.BlockSpec(memory_space=pl.ANY)] + [VM] * 5,
        out_specs=[VM] * 4 + [pl.BlockSpec(memory_space=pl.ANY)] * 2,
        out_shape=[
            jax.ShapeDtypeStruct(part.shape, BF),
            jax.ShapeDtypeStruct(part.shape, BF),
            jax.ShapeDtypeStruct(sums.shape, F32),
            jax.ShapeDtypeStruct((steps, CHUNK, part.shape[2]), BF),
        ]
        + outs,
        scratch_shapes=wide + [pltpu.VMEM((2,) + sums.shape, F32), small, own_rows(part)] + sems + [pltpu.SemaphoreType.DMA((2,))] * 3 + more,
        compiler_params=comm_params(1, 32),
        cost_estimate=pl.CostEstimate(flops=50_000_000, bytes_accessed=150_000_000, transcendentals=0),
        name="onward",
    )(part, rows, sums, live, gain, q, o)


def run_back(part, hidden, tokens, gained, live, gain):
    wide, sems = exchange_scratch(part)
    small = pltpu.VMEM((8, LANES), F32)
    hbm = pl.BlockSpec(memory_space=pl.ANY)
    return pl.pallas_call(
        back_kernel,
        in_specs=[VM, hbm, hbm, VM, VM, VM],
        out_specs=[VM] * 3,
        out_shape=[
            jax.ShapeDtypeStruct(part.shape, BF),
            jax.ShapeDtypeStruct(part.shape, BF),
            jax.ShapeDtypeStruct(live.shape, F32),
        ],
        scratch_shapes=wide + [small, small, own_rows(part), own_rows(part)] + sems + [pltpu.SemaphoreType.DMA((2,))] * 4,
        compiler_params=comm_params(2, 28),
        cost_estimate=pl.CostEstimate(flops=50_000_000, bytes_accessed=150_000_000, transcendentals=0),
        name="back",
    )(part, hidden, tokens, gained, live, gain)


PARTS = 2
PIECE_ROWS = 32
BLOCK = 16


def by_rows(count, body):
    def step(i, _):
        body(pl.multiple_of(i * BLOCK, BLOCK))
        return 0

    lax.fori_loop(0, count // BLOCK, step, 0)


def line_steps(n):
    return [step for i in range(n - 1) for step in ((1, n - 1 - i), (-1, i))]


def hand_out(b, boards, owns, pc_s, pc_r, *, ny):
    section, xb, peer, beside = partners()
    yb = lax.axis_index("rep") // PAIR

    def y_peer(k):
        return {"rep": (yb + k) % ny * PAIR + xb}

    def y_from(k):
        return (yb + ny - k) % ny

    def span_of(h):
        return pl.ds(pl.multiple_of(h * PIECE_ROWS, PIECE_ROWS), PIECE_ROWS)

    def piece(i, x, y, t, h, kind, device):
        place = boards[i].at[x, y, t, span_of(h)]
        return remote(place, place, pc_s.at[i, kind, x, y, t, h], pc_r.at[i, x, y, t, h], device)

    def offer(i, h):
        return remote(owns[i].at[span_of(h)], boards[i].at[xb, yb, 1 - b, span_of(h)],
                      pc_s.at[i, 0, xb, yb, 1 - b, h], pc_r.at[i, xb, yb, 1 - b, h], peer)

    def gather_chip(i, h):
        @pl.when(section == b)
        def _():
            boards[i][xb, yb, b, span_of(h)] = owns[i][span_of(h)]

        @pl.when(section != b)
        def _():
            offer(i, h).start()

    def gather_side(i, h):
        @pl.when(section == b)
        def _():
            piece(i, xb, yb, 1 - b, h, 0, peer).wait_recv()
            for t in range(2):
                piece(i, xb, yb, t, h, ny, beside).start()

    def gather_y(i, h):
        @pl.when(section == b)
        def _():
            for t in range(2):
                for k in range(1, ny):
                    piece(i, xb, yb, t, h, k, y_peer(k)).start()

    def gather_x(i, h):
        @pl.when(section == b)
        def _():
            for k in range(1, ny):
                for t in range(2):
                    piece(i, xb, y_from(k), t, h, k, peer).wait_recv()
                    piece(i, xb, y_from(k), t, h, ny, beside).start()

    def gather_end(i, h):
        @pl.when(section == b)
        def _():
            for y in range(ny):
                for t in range(2):
                    piece(i, 1 - xb, y, t, h, ny, beside).wait_recv()
                    piece(i, xb, y, t, h, ny, peer).wait_send()
            for t in range(2):
                for k in range(1, ny):
                    piece(i, xb, yb, t, h, k, peer).wait_send()

        @pl.when(section != b)
        def _():
            offer(i, h).wait_send()

    return gather_chip, gather_side, gather_y, gather_x, gather_end


def each(count, body):
    def step(i, _):
        body(i)
        return 0

    lax.fori_loop(0, count, step, 0)


def reduce_flow(b, ga_ref, gb_ref, gc_ref, boards, got_ya, acc_a, got_za, own_a, acc_b, got_zb, own_b, acc_c, got_zc, own_c,
                ya_s, ya_r, za_s, za_r, zb_s, zb_r, zc_s, zc_r, pc_s, pc_r, *, ns, ny):
    _, xb, peer, _ = partners()
    z = lax.axis_index("shard")
    yb = lax.axis_index("rep") // PAIR
    count = ga_ref.shape[2] // PIECE_ROWS
    steps = line_steps(ns)
    order = []
    for _, target in steps:
        if target not in order:
            order.append(target)
    gather_chip, gather_side, gather_y, gather_x, gather_end = hand_out(b, boards, (own_a, own_b), pc_s, pc_r, ny=ny)
    chip_c, side_c, y_c, x_c, end_c = hand_out(1 - b, boards, (None, own_c), pc_s, pc_r, ny=ny)

    def y_peer(k):
        return {"rep": (yb + k) % ny * PAIR + xb}

    def span_of(h):
        return pl.ds(pl.multiple_of(h * PIECE_ROWS, PIECE_ROWS), PIECE_ROWS)

    def ya(k, target, h):
        return remote(ga_ref.at[(yb + k) % ny, target, span_of(h)], got_ya.at[k - 1, target, span_of(h)],
                      ya_s.at[k - 1, target, h], ya_r.at[k - 1, target, h], y_peer(k))

    def start(h):
        for target in order:
            @pl.when(target != z)
            def _():
                for k in range(1, ny):
                    ya(k, target, h).start()
        for k in range(1, ny):
            ya(k, z, h).start()

    streams = ((acc_a, got_za, za_s, za_r), (acc_b, got_zb, zb_s, zb_r), (acc_c, got_zc, zc_s, zc_r))

    def line(i, way, target, h):
        acc, got, send, recv = streams[i]
        place = jnp.where(target == z - 1, ns, target) if way < 0 else target
        return remote(acc.at[target, span_of(h)], got.at[place, span_of(h)], send.at[target, h], recv.at[place, h], {"shard": z + way})

    def wait_line(place, h):
        for acc, got, send, recv in streams:
            remote(acc.at[0, span_of(h)], got.at[place, span_of(h)], send.at[0, h], recv.at[place, h], peer).wait_recv()

    def wait_y(target, h):
        for k in range(1, ny):
            remote(ga_ref.at[0, target, span_of(h)], got_ya.at[k - 1, target, span_of(h)], ya_s.at[k - 1, target, h],
                   ya_r.at[k - 1, target, h], peer).wait_recv()

    def add(target, h, into_a, into_b, into_c, start, extra):
        span = span_of(h)
        total = ga_ref[yb, target, span].astype(F32)
        for k in range(1, ny):
            total = total + got_ya[k - 1, target, span].astype(F32)
        for place in extra:
            total = total + got_za[place, span].astype(F32)
        into_a[start + (span,)] = total.astype(BF)
        for ref, got, into in ((gb_ref, got_zb, into_b), (gc_ref, got_zc, into_c)):
            total = ref[target, span].astype(F32)
            for place in extra:
                total = total + got[place, span].astype(F32)
            into[start + (span,)] = total.astype(BF)

    def active(way, target):
        return target > z if way > 0 else target < z

    def step(way, target, h):
        wait_y(target, h)
        far = z > 0 if way > 0 else z < ns - 1

        @pl.when(jnp.logical_not(far))
        def _():
            add(target, h, acc_a, acc_b, acc_c, (target,), ())

        @pl.when(far)
        def _():
            wait_line(target, h)
            add(target, h, acc_a, acc_b, acc_c, (target,), (target,))

        for i in range(3):
            line(i, way, target, h).start()

    def last(h):
        wait_y(z, h)

        @pl.when(z == 0)
        def _():
            wait_line(ns, h)
            add(z, h, own_a, own_b, own_c, (), (ns,))

        @pl.when(z == ns - 1)
        def _():
            wait_line(z, h)
            add(z, h, own_a, own_b, own_c, (), (z,))

        @pl.when((z > 0) & (z < ns - 1))
        def _():
            wait_line(z, h)
            wait_line(ns, h)
            add(z, h, own_a, own_b, own_c, (), (z, ns))

        for i in range(2):
            gather_chip(i, h)
        chip_c(1, h)

    def sides(h):
        for i in range(2):
            gather_side(i, h)
        side_c(1, h)
        for i in range(2):
            gather_y(i, h)
        y_c(1, h)

    def crosses(h):
        for i in range(2):
            gather_x(i, h)
        x_c(1, h)

    def slot(at):
        for way, target in steps:
            h = at - z if way > 0 else at - (ns - 1 - z)

            @pl.when(active(way, target) & (h >= 0) & (h < count))
            def _():
                step(way, target, h)

        mine = at - jnp.where(2 * z > ns - 1, z, ns - 1 - z)
        for late, body in ((0, last), (1, sides), (2, crosses)):
            @pl.when((mine >= late) & (mine < count + late))
            def _():
                body(mine - late)

    def finish():
        def ends(h):
            for i in range(2):
                gather_end(i, h)
            end_c(1, h)
            for target in range(ns):
                for k in range(1, ny):
                    ya(k, target, h).wait_send()
            for way, target in steps:
                @pl.when(active(way, target))
                def _():
                    for i in range(3):
                        line(i, way, target, h).wait_send()

        each(count, ends)

    return start, slot, count + ns + 1, finish


def reduce_shapes(ga, gb):
    ny, ns, ra, ca = ga.shape
    rb, cb = gb.shape[1:]
    dma = pltpu.SemaphoreType.DMA
    parts = ra // PIECE_ROWS
    outs = [jax.ShapeDtypeStruct((PAIR, ny, 2, ra, ca), BF), jax.ShapeDtypeStruct((PAIR, ny, 2, rb, cb), BF)]
    scratch = [
        pltpu.VMEM((ny - 1, ns, ra, ca), BF),
        pltpu.VMEM((ns, ra, ca), BF),
        pltpu.VMEM((ns + 1, ra, ca), BF),
        pltpu.VMEM((ra, ca), BF),
        *[pltpu.VMEM((ns, rb, cb), BF), pltpu.VMEM((ns + 1, rb, cb), BF), pltpu.VMEM((rb, cb), BF)] * 2,
        dma((ny - 1, ns, parts)), dma((ny - 1, ns, parts)),
        *[dma((ns, parts)), dma((ns + 1, parts))] * 3,
        dma((2, ny + 1, PAIR, ny, 2, parts)), dma((2, PAIR, ny, 2, parts)),
    ]
    return outs, scratch


def tail_kernel(ga_ref, gb_ref, gc_ref, pa_ref, vec_ref, p_ref, tokens_ref, cot_all, gain_ref,
                all_a, all_b, vec_out, res_ref, *refs, ns, ny):
    flow, (got_p, held, got_x, give, rows_ref, cot_ref, vec_y, vec_h, vec_z, vec_t, ra_s, ra_r, v_s, v_r, rows_s) = refs[:20], refs[20:]
    section, xb, peer, beside = partners()
    z = lax.axis_index("shard")
    yb = lax.axis_index("rep") // PAIR

    def y_peer(k):
        return {"rep": (yb + k) % ny * PAIR + xb}

    def z_peer(k):
        return {"shard": (z + k) % ns}

    greet(peer, beside, *(y_peer(k) for k in range(1, ny)), *(z_peer(k) for k in range(1, ns)))

    def over_y(k):
        return remote(vec_ref, vec_y.at[k - 1], v_s.at[k], v_r.at[k], y_peer(k))

    def over_z(k):
        return remote(vec_h, vec_z.at[k - 1], v_s.at[ny + k], v_r.at[ny + k], z_peer(k))

    to_chip = remote(vec_t.at[1 - section], vec_out.at[section, xb], v_s.at[0], v_r.at[0], peer)

    def to_side(t):
        return remote(vec_out.at[t, xb], vec_out.at[t, xb], v_s.at[ny + ns + t], v_r.at[ny + ns + t], beside)

    for k in range(1, ny):
        over_y(k).start()

    per = p_ref.shape[1] // CHUNK
    rows_copy = pltpu.make_async_copy(tokens_ref.at[0, xb, section], rows_ref, rows_s.at[0])
    cot_copy = pltpu.make_async_copy(cot_all.at[xb * 2 + section], cot_ref, rows_s.at[1])

    def p_peer(x, c):
        span = pl.ds(c * CHUNK, CHUNK)
        return remote(p_ref.at[x * 2 + 1 - section, span], got_p.at[x, c], ra_s.at[0, x, c], ra_r.at[0, x, c], peer)

    def p_beside(c):
        return remote(held.at[1 - xb, c], got_x.at[c], ra_s.at[1, 0, c], ra_r.at[1, 0, c], beside)

    def p_give(c):
        return remote(give.at[c], res_ref.at[1, pl.ds(c * CHUNK, CHUNK)], ra_s.at[1, 1, c], ra_r.at[1, 1, c], peer)

    boards = (all_a, all_b)
    pieces = flow[18:20]
    chip1, side1, y1, x1, end1 = hand_out(1, boards, (pa_ref, None), *pieces, ny=ny)
    count = ga_ref.shape[2] // PIECE_ROWS
    start, slot, slots, end0 = reduce_flow(0, ga_ref, gb_ref, gc_ref, boards, *flow, ns=ns, ny=ny)

    def both(body):
        each(count, lambda h: body(0, h))

    rows_copy.start()
    cot_copy.start()

    def rows_out():
        for c in range(per):
            for x in range(PAIR):
                p_peer(x, c).start()

    def pieces_side():
        both(side1)

    def pieces_y():
        both(y1)

    def rows_beside():
        for c in range(per):
            for x in range(PAIR):
                p_peer(x, c).wait_recv()

                def body(low):
                    span = pl.ds(low, BLOCK)
                    mine = p_ref[x * 2 + section, pl.ds(c * CHUNK + low, BLOCK)].astype(F32)
                    held[x, c, span] = (mine + got_p[x, c, span].astype(F32)).astype(BF)

                by_rows(CHUNK, body)
            p_beside(c).start()

    def sums_z():
        total = vec_ref[...]
        for k in range(1, ny):
            over_y(k).wait()
            total = total + vec_y[k - 1]
        vec_h[...] = total
        for k in range(1, ns):
            over_z(k).start()

    def pieces_x():
        both(x1)

    def sums_chip():
        total = vec_h[...]
        for k in range(1, ns):
            over_z(k).wait()
            total = total + vec_z[k - 1]
        vec_t[...] = total
        to_chip.start()
        vec_out[section, xb] = vec_t[section]

    def rows_end():
        rows_copy.wait()
        cot_copy.wait()
        for c in range(per):
            p_beside(c).wait_recv()

            def body(low):
                span = pl.ds(low, BLOCK)
                there = pl.ds(c * CHUNK + low, BLOCK)
                total = held[xb, c, span].astype(F32) + got_x[c, span].astype(F32)
                rows = rows_ref[there].astype(F32)
                inv = rms(rows)
                hat = rows * inv
                d_hat = total * gain_ref[...]
                d_rows = inv * (d_hat - hat * jnp.mean(d_hat * hat, axis=-1, keepdims=True))
                low_rows = (cot_ref[there].astype(F32) + d_rows).astype(BF)
                give[c, span] = low_rows

                @pl.when(section == 0)
                def _():
                    res_ref[0, there] = low_rows

            by_rows(CHUNK, body)

        @pl.when(section != 0)
        def _():
            for c in range(per):
                p_give(c).start()

    def sums_side():
        to_chip.wait_send()
        remote(vec_t.at[0], vec_out.at[1 - section, xb], v_s.at[0], v_r.at[0], peer).wait_recv()
        for t in range(2):
            to_side(t).start()

    def sums_end():
        for t in range(2):
            to_side(t).wait_send()
            remote(vec_out.at[t, xb], vec_out.at[t, 1 - xb], v_s.at[ny + ns + t], v_r.at[ny + ns + t], beside).wait_recv()

    ahead = min(4, count)
    rows_out()
    both(chip1)
    each(ahead, start)
    between = ((0, pieces_side), (0, rows_beside), (1, sums_z), (4, sums_chip), (6, rows_end), (8, pieces_y), (9, sums_side), (12, sums_end), (15, pieces_x))

    def go(at, _):
        @pl.when(at + ahead < count)
        def _():
            start(at + ahead)

        slot(at)
        for n, body in between:
            @pl.when(at == n)
            def _():
                body()

        return 0

    lax.fori_loop(0, max(slots, between[-1][0] + 1), go, 0)
    both(end1)
    end0()
    for c in range(per):
        for x in range(PAIR):
            p_peer(x, c).wait_send()
        p_beside(c).wait_send()

        @pl.when(section != 0)
        def _():
            p_give(c).wait_send()

        @pl.when(section == 0)
        def _():
            p_give(c).wait_recv()


def run_tail(ga, gb, gc, pa, vec, p, tokens, cot, gain):
    ny, ns = ga.shape[:2]
    seq_len, width = p.shape[1:]
    per = seq_len // CHUNK
    block = (CHUNK, width)
    dma = pltpu.SemaphoreType.DMA
    hbm = pl.BlockSpec(memory_space=pl.ANY)
    outs, scratch = reduce_shapes(ga, gb)
    return pl.pallas_call(
        functools.partial(tail_kernel, ns=ns, ny=ny),
        in_specs=[VM] * 6 + [hbm, hbm, VM],
        out_specs=[VM] * 4,
        out_shape=outs + [jax.ShapeDtypeStruct((2, PAIR) + vec.shape[1:], F32), jax.ShapeDtypeStruct((2, seq_len, width), BF)],
        scratch_shapes=scratch
        + [
            pltpu.VMEM((PAIR, per) + block, BF),
            pltpu.VMEM((PAIR, per) + block, BF),
            pltpu.VMEM((per,) + block, BF),
            pltpu.VMEM((per,) + block, BF),
            pltpu.VMEM((seq_len, width), BF),
            pltpu.VMEM((seq_len, width), BF),
            pltpu.VMEM((ny - 1,) + vec.shape, F32),
            pltpu.VMEM(vec.shape, F32),
            pltpu.VMEM((ns - 1,) + vec.shape, F32),
            pltpu.VMEM(vec.shape, F32),
            dma((2, PAIR, per)), dma((2, PAIR, per)),
            dma((ny + ns + 2,)), dma((ny + ns + 2,)),
            dma((2,)),
        ],
        compiler_params=comm_params(4, 58),
        cost_estimate=pl.CostEstimate(flops=50_000_000, bytes_accessed=300_000_000, transcendentals=0),
        name="tail",
    )(ga, gb, gc, pa, vec, p, tokens, cot, gain)


def place_kernel(a_ref, b_ref, in_ref, out_ref, dt_ref, *, places, dts, ny):
    for col, size, index, off in places:
        in_ref[:, col : col + size] = a_ref[index + (slice(None), slice(off, off + size))].astype(F32)
    for col, size, index, off in dts:
        dt_ref[:, col : col + size] = a_ref[index + (slice(None), slice(off, off + size))].astype(F32)
    part = b_ref.shape[-1]
    for q in range(PAIR):
        for t in range(2):
            for y in range(ny):
                col = (t * ny + y) * part
                out_ref[q, :, col : col + part] = b_ref[q, y, t].astype(F32)


def run_place(pieces, places, dts, columns, heads, block):
    ny = pieces[0].shape[1]
    rows = pieces[0].shape[3]
    lead = (PAIR, ny, 2)
    width = 2 * ny * pieces[1].shape[4]
    return pl.pallas_call(
        functools.partial(place_kernel, places=places, dts=dts, ny=ny),
        grid=(rows // block,),
        in_specs=[pl.BlockSpec(lead + (block, v.shape[4]), lambda i: (0, 0, 0, i, 0)) for v in pieces],
        out_specs=[
            pl.BlockSpec((block, columns), lambda i: (i, 0)),
            pl.BlockSpec((PAIR, block, width), lambda i: (0, i, 0)),
            pl.BlockSpec((block, heads), lambda i: (i, 0)),
        ],
        out_shape=[
            jax.ShapeDtypeStruct((rows, columns), F32),
            jax.ShapeDtypeStruct((PAIR, rows, width), F32),
            jax.ShapeDtypeStruct((rows, heads), F32),
        ],
        compiler_params=PARAMS,
        cost_estimate=pl.CostEstimate(flops=1_000_000, bytes_accessed=25_000_000, transcendentals=0),
        name="place",
    )(*pieces)


def smalls_kernel(z_ref, v_ref, conv_ref, heads_ref, pre_ref, out_ref, full, *, taps, ns, mine_w, states2, heads, width):
    half = ns // 2
    cw = mine_w // half
    unit = heads // ns // PAIR
    gbc, gh = mine_w, mine_w + states2
    spread = head_map(mine_w, 2 * mine_w * PAIR // heads)
    shared = v_ref[0, 0] + v_ref[0, 1] + v_ref[1, 0] + v_ref[1, 1]
    full[:, 2 * PAIR * mine_w :] = shared[:8, gbc : gbc + states2]
    for t in range(2):
        for q in range(PAIR):
            for k in range(half):
                col = ((t * half + k) * PAIR + q) * cw
                full[:, col : col + cw] = v_ref[t, q, :8, k * cw : (k + 1) * cw]
    channels = (2 * PAIR * mine_w + states2) // ns
    inner = 2 * PAIR * mine_w // ns
    part = width // ns
    wide = v_ref.shape[3]
    skips = []
    for t in range(2):
        skips.append([])
        for q in range(PAIR):
            row = v_ref[t, q, taps + 1 : taps + 2, :mine_w]
            high = row.astype(BF)
            rest = row - high.astype(F32)
            mid = rest.astype(BF)
            rows8 = lambda v: jnp.broadcast_to(v, (8, mine_w))
            skips[t].append((mm_t(rows8(high), spread) + mm_t(rows8(mid), spread) + mm_t(rows8(rest - mid.astype(F32)), spread))[0:1])
    heads_ref[...] = jnp.zeros_like(heads_ref)
    for at in range(ns):
        @pl.when(z_ref[0] == at)
        def _():
            conv_ref[...] = full[:, at * channels : (at + 1) * channels]
            out_ref[...] = full[taps + 2 : taps + 3, at * inner : (at + 1) * inner]
            t, k = at // half, at % half
            for q in range(PAIR):
                span = slice(gh + k * unit, gh + (k + 1) * unit)
                put = slice(q * unit, (q + 1) * unit)
                heads_ref[0:1, put] = v_ref[t, q, 0:1, span]
                heads_ref[1:2, put] = v_ref[t, q, 1:2, span]
                heads_ref[2:3, put] = skips[t][q][:, k * unit : (k + 1) * unit]
            for row in range(-(-width // wide)):
                low, high = max(at * part, row * wide), min((at + 1) * part, (row + 1) * wide)
                if low < high:
                    pre_ref[:, low - at * part : high - at * part] = shared[8 + row : 9 + row, low - row * wide : high - row * wide]


def run_smalls(z, v, taps, ns, mine_w, states2, heads, width):
    channels = (2 * PAIR * mine_w + states2) // ns
    whole = lambda *dims: pl.BlockSpec(dims, lambda i, z: (0,) * len(dims))
    return pl.pallas_call(
        functools.partial(smalls_kernel, taps=taps, ns=ns, mine_w=mine_w, states2=states2, heads=heads, width=width),
        grid_spec=pltpu.PrefetchScalarGridSpec(
            num_scalar_prefetch=1,
            grid=(1,),
            in_specs=[whole(*v.shape)],
            out_specs=[whole(8, channels), whole(8, LANES), whole(1, width // ns), whole(1, 2 * PAIR * mine_w // ns)],
            scratch_shapes=[pltpu.VMEM((8, channels * ns), F32)],
        ),
        out_shape=[
            jax.ShapeDtypeStruct((8, channels), F32),
            jax.ShapeDtypeStruct((8, LANES), F32),
            jax.ShapeDtypeStruct((1, width // ns), F32),
            jax.ShapeDtypeStruct((1, 2 * PAIR * mine_w // ns), F32),
        ],
        compiler_params=PARAMS,
        cost_estimate=pl.CostEstimate(flops=1_000_000, bytes_accessed=1_000_000, transcendentals=0),
        name="smalls",
    )(z, v)


def dot(a, b):
    return jnp.dot(a, b, preferred_element_type=F32)


def pick(index, options):
    result = options[-1]
    for place in reversed(range(len(options) - 1)):
        result = jnp.where(index == place, options[place], result)
    return result


def ordered(index, own, other, axis):
    return jnp.stack([pick(index, (own, other)), pick(index, (other, own))], axis=axis)


def joined(index, own, other, axis):
    return jnp.concatenate([pick(index, (own, other)), pick(index, (other, own))], axis=axis)


def on_device(boundary, lengths, in_proj, dt_proj, out_proj, conv_weight, conv_bias, dt_bias, a_log, d_skip, pre_gain, out_gain):
    ns = lax.axis_size("shard")
    nr = lax.axis_size("rep")
    ny = nr // PAIR
    s = lax.axis_index("section")
    z = lax.axis_index("shard")
    rep = lax.axis_index("rep")
    xb = rep % PAIR
    yb = rep // PAIR

    def swap(v):
        return lax.ppermute(v, "section", [(0, 1), (1, 0)])

    def x_swap(v):
        return lax.ppermute(v, "rep", [(i, i ^ 1) for i in range(nr)])

    def y_send(v, k):
        return lax.ppermute(v, "rep", [(i, (i // PAIR + k) % ny * PAIR + i % PAIR) for i in range(nr)])

    micro, seq_len, width = boundary.shape[1], boundary.shape[3], boundary.shape[4]
    inner = out_proj.shape[1] * ns
    heads = dt_bias.shape[1] * ns
    taps, channels = conv_weight.shape[1], conv_weight.shape[2] * ns
    states2 = channels - inner
    cw = inner // ns // PAIR
    half = ns // 2
    mine_w = half * cw
    mine_h = heads // (2 * PAIR)
    part_w = 2 * mine_w // ny

    def column_chunks(v, first):
        out = []
        for t in range(2):
            for shard in range(t * half, (t + 1) * half):
                start = first + shard * PAIR * cw
                out.append(pick(xb, tuple(v[:, start + q * cw : start + (q + 1) * cw] for q in range(PAIR))))
        return [jnp.concatenate(out[:half], axis=1), jnp.concatenate(out[half:], axis=1)]

    own_in = in_proj[0]
    q_own = []
    for a, b in zip(column_chunks(own_in, 0), column_chunks(own_in, inner)):
        if ny == 2:
            q_own += [a, b]
        else:
            q_own += [v[:, k * part_w : (k + 1) * part_w] for v in (a, b) for k in range(ny // 2)]
    q_own = jnp.stack(q_own).reshape(2, ny, width // ns, part_w)
    own_out = out_proj[0]
    o_own = pick(xb, (own_out[:cw], own_out[cw : 2 * cw])).reshape(ny, cw // ny, width)

    flat = lambda v: v.reshape(-1, v.shape[-1])
    smalls_own = tuple(flat(v) for v in (conv_weight, conv_bias, dt_bias, a_log, d_skip, pre_gain, out_gain))
    counts = jnp.broadcast_to(lengths.astype(F32), (micro, LANES))
    tokens, normed0, g_out1, live8, px, pbc, ph, gains, w_bcdt, in0, out0 = run_start(
        boundary[0, :, 0], counts, smalls_own, own_in[:, 2 * inner :], dt_proj[0], q_own, o_own, heads
    )
    smalls = [(px[b], pbc[b], ph[b]) for b in range(2)]
    unit_h = heads // ns // PAIR
    w_in, w_out = [in0.reshape(ny, width, part_w)], [out0.reshape(mine_w, width)]
    seqs = PAIR * micro

    def by_seq(v):
        return v.reshape((seqs, seq_len) + v.shape[1:])

    def of_own(v):
        return pick(xb, (v[0], v[1]))

    chunks = seq_len // CHUNK

    def forward(b, normed, dmix):
        normed = normed.reshape(seqs * seq_len, width)
        proj = [dot(normed, w_in[b][j]).astype(BF) for j in range(ny)]
        if ny > 2:
            proj = [jnp.concatenate(proj[: ny // 2], axis=1), jnp.concatenate(proj[ny // 2 :], axis=1)]
        gate, x = by_seq(proj[0]), by_seq(proj[1])
        bcdt = by_seq(dot(normed, w_bcdt[b]))
        gg, y, state, *sums = run_forward(smalls[b], gate, x, bcdt, dmix, taps, mine_h)
        gg = gg.reshape(seqs * seq_len, mine_w)
        part = by_seq(dot(gg, w_out[b]).astype(BF))
        return part, sums, (normed, gate, x, bcdt, gg, y, state)

    def mixed_back(b, g_out):
        dmix = lax.dot_general(g_out, w_out[b], (((1,), (1,)), ((), ())), preferred_element_type=F32)
        return by_seq(dmix.astype(BF))

    part0, sums, stored0 = forward(0, normed0, None)
    hidden, normed, r0, gained0, in1, out1 = run_onward(
        part0, tokens, sums[0].reshape(seqs * chunks, LANES), live8, gains[1], q_own, o_own, float(inner), ns
    )
    w_in.append(in1.reshape(ny, width, part_w))
    w_out.append(out1.reshape(mine_w, width))
    g_out1 = g_out1.reshape(seqs * seq_len, width)
    dmix1 = mixed_back(1, g_out1)
    part1, sums, stored1 = forward(1, normed, dmix1)
    both_sums = run_sums(jnp.concatenate([v.reshape(seqs * chunks, LANES) for v in sums]), 3)
    r1 = lax.rsqrt(both_sums[: seqs * chunks] / inner + EPSILON)

    def backward(b, dmix, stored, r, coef):
        normed, gate, x, bcdt, _, y, state = stored
        scalars = jnp.concatenate([r.reshape(seqs, chunks, LANES), coef.reshape(seqs, chunks, LANES)], axis=1)
        dgate, dx, dbcdt, gsmall = run_backward(smalls[b], gate, x, bcdt, y, state, dmix, scalars, taps, mine_h)
        flat = lambda v: v.reshape(seqs * seq_len, v.shape[-1])
        dgate, dx, dbcdt = flat(dgate), flat(dx), flat(dbcdt)
        if ny == 2:
            dparts = [dgate, dx]
        else:
            dparts = [v[:, k * part_w : (k + 1) * part_w] for v in (dgate, dx) for k in range(ny // 2)]
        against = lambda a, w: lax.dot_general(a, w, (((1,), (1,)), ((), ())), preferred_element_type=F32)
        d_normed = against(dbcdt, w_bcdt[b])
        for j in range(ny):
            d_normed = d_normed + against(dparts[j], w_in[b][j])
        gpre = jnp.sum(d_normed * normed.astype(F32), axis=0) / gains[b, 0]
        across = lambda a, c: lax.dot_general(a, c, (((0,), (0,)), ((), ())), preferred_element_type=F32)

        dbc = dbcdt[:, :states2]
        cols = [dbc[:, : states2 // 2], dbc[:, states2 // 2 :]]
        total = (pick(s, cols).astype(F32) + swap(pick(s, cols[::-1])).astype(F32)).astype(BF)
        cols = [total[:, : states2 // 4], total[:, states2 // 4 :]]
        send = pick(xb, cols[::-1])
        got = x_swap(send)
        total = (pick(xb, cols).astype(F32) + got.astype(F32)).astype(BF)
        mine = jnp.concatenate([total, dbcdt[:, states2 : states2 + states2 // 4]], axis=1)
        grad_in = [across(normed, jnp.concatenate([v, mine], axis=1)).astype(BF) for v in dparts]
        grad_in = [v.reshape(ns, width // ns, -1) for v in grad_in]
        wide = gsmall.shape[1]
        gpre = jnp.pad(gpre, (0, 8 * wide - width)).reshape(8, wide)
        return by_seq(d_normed.astype(BF)), grad_in, jnp.concatenate([gsmall, gpre])

    def z_sum(v):
        parts = [v[j] for j in range(ns)]
        total = pick(z, parts).astype(F32)
        for k in range(1, ns):
            send = lax.dynamic_index_in_dim(v, (z + k) % ns, 0, False)
            got = lax.ppermute(send, "shard", [(i, (i + k) % ns) for i in range(ns)])
            total = total + got.astype(F32)
        return total.astype(BF)

    def out_chip(g_out, gg, r):
        g_scaled = (g_out.astype(F32) * r.reshape(-1, 1)).astype(BF)
        across = lambda a, c: lax.dot_general(a, c, (((0,), (0,)), ((), ())), preferred_element_type=F32)
        grad = across(gg, g_scaled).astype(BF)
        cols = [grad[:, : width // 2], grad[:, width // 2 :]]
        send = pick(s, cols[::-1])
        got = swap(send)
        return joined(s, pick(s, cols), got, 0)

    def out_grad(v):
        step = width // 2 // ny
        parts = [v[:, j * step : (j + 1) * step] for j in range(ny)]
        total = pick(yb, parts).astype(F32)
        for k in range(1, ny):
            send = pick((yb + k) % ny, parts)
            got = y_send(send, k)
            total = total + got.astype(F32)
        return total.astype(BF).reshape(ns, cw, -1)

    v1 = out_chip(g_out1, stored1[4], r1)
    gout1 = out_grad(v1)
    d_normed1, gin1, gsmall1 = backward(1, dmix1, stored1, r1, r1 * r1 * r1 * both_sums[seqs * chunks :] / inner)
    d_normed1, *gin1 = lax.optimization_barrier((d_normed1, *gin1))
    total1 = pick(yb, gin1).astype(F32)
    for k in range(1, ny):
        send = pick((yb + k) % ny, gin1)
        got = y_send(send, k)
        total1 = total1 + got.astype(F32)
    total1 = total1.astype(BF)
    cot0, g_out0, dots0 = run_back(d_normed1, hidden, tokens, gained0, live8, gains[1])

    g_out0 = g_out0.reshape(-1, width)
    dmix0 = mixed_back(0, g_out0)
    v0 = out_chip(g_out0, stored0[4], r0)
    dmix0, total1 = lax.optimization_barrier((dmix0, total1))
    gout0 = out_grad(v0)
    piece_a1 = z_sum(total1)

    part1 = part1.reshape(PAIR, micro, seq_len, width)
    mine = pick(s, (part1[:, 0], part1[:, 1])).astype(F32) + swap(pick(s, (part1[:, 1], part1[:, 0]))).astype(F32)
    mine = mine.astype(BF)
    send = of_own(mine[::-1])
    got = x_swap(send)
    mine = of_own(mine).astype(F32) + got.astype(F32)
    own_hidden = of_own(hidden.reshape(PAIR, micro, seq_len, width))
    scale = of_own((live8 * r1).reshape(PAIR, micro, seq_len, 1))
    final = (pick(s, (own_hidden[0], own_hidden[1])).astype(F32) + pick(s, (scale[0], scale[1])) * mine).astype(BF)
    final = ordered(s, final, swap(final), 0)

    d_normed0, gin0, gsmall0 = backward(0, dmix0, stored0, r0, r0 * r0 * dots0 / inner)
    *pieces, vec, res = run_tail(
        jnp.stack(gin0), gout0, gout1, piece_a1, jnp.stack([gsmall0, gsmall1]), d_normed0, tokens, cot0, gains[0]
    )
    activations = pick(s, (own_hidden, final))
    input_grads = pick(s, (res, of_own(cot0.reshape(PAIR, micro, seq_len, width))))
    places, dts = [], []
    col = 0
    for plane in range(2):
        for t in range(2):
            for k in range(half):
                for q in range(PAIR):
                    y_at, off = divmod(plane * mine_w + k * cw, part_w)
                    places.append((col, cw, (q, y_at, t), off))
                    col += cw
    quad = states2 // 4
    for t in range(2):
        for q in range(PAIR):
            places.append((col, quad, (q, 0, t), part_w))
            col += quad
    for t in range(2):
        for k in range(half):
            for q in range(PAIR):
                dts.append((((t * half + k) * PAIR + q) * unit_h, unit_h, (q, 0, t), part_w + quad + k * unit_h))
    grad_in, grad_out, grad_dt = run_place(pieces, tuple(places), tuple(dts), col, heads, 64)
    grad_out = grad_out.reshape(PAIR * cw, width)
    g_conv, g_heads, g_pre, g_og = run_smalls(z[None], vec, taps, ns, mine_w, states2, heads, width)
    g_cw, g_cb = g_conv[:taps], g_conv[taps]
    g_dtb, g_alg, g_dsk = (g_heads[i, : heads // ns] for i in range(3))
    g_pre, g_og = g_pre[0], g_og[0]

    return (
        activations[None, :, None],
        input_grads[None, :, None],
        grad_in[None],
        grad_dt[None],
        grad_out[None],
        g_cw[None],
        g_cb[None],
        g_dtb[None],
        g_alg[None],
        g_dsk[None],
        g_pre[None],
        g_og[None],
    )


def solution(mesh):
    shard1 = P("section", "shard")
    shard2 = P("section", "shard", None)
    tokens = P("section", None, ("shard", "rep"), None, None)
    taps = P("section", None, "shard")
    weights = (shard2, shard2, shard2, taps, shard1, shard1, shard1, shard1, shard1, shard1)
    return jax.shard_map(
        on_device,
        mesh=mesh,
        in_specs=(tokens, P(None, ("shard", "rep"))) + weights,
        out_specs=(tokens, tokens) + weights,
        check_vma=False,
    )
```
